32 devices in a mesh: dp: 2 (over x), sp: 16 (over z, y, core).
Axes of the slice: x: 2, y: 2, z: 4, core: 2. Of those that a mesh axis runs over, the one named last changes fastest.
Arguments:
- x_in: bfloat16 [4, 2048, 2048], P('dp', 'sp'), parts along dimension 0
- grad_y: bfloat16 [4, 2048, 2048], P('dp', 'sp'), parts along dimension 0
- positions: int32 [4, 2048], P('dp', 'sp'), parts along dimension 0
- g_norm: bfloat16 [2048], replicated
- w_query: bfloat16 [2048, 2048], replicated
- w_key: bfloat16 [2048, 2048], replicated
- w_value: bfloat16 [2048, 2048], replicated
- w_out: bfloat16 [2048, 2048], replicated
- g_query: bfloat16 [2048], replicated
- g_key: bfloat16 [2048], replicated
Outputs:
- output 1: bfloat16 [4, 2048, 2048], P('dp', 'sp'), parts along dimension 0
- output 2: bfloat16 [4, 2048, 2048], P('dp', 'sp'), parts along dimension 0
- output 3: float32 [4096], P(('dp', 'sp')), parts along dimension 0
- output 4: float32 [4096, 2048], P(('dp', 'sp')), parts along dimension 0
- output 5: float32 [4096, 2048], P(('dp', 'sp')), parts along dimension 0
- output 6: float32 [4096, 2048], P(('dp', 'sp')), parts along dimension 0
- output 7: float32 [4096, 2048], P(('dp', 'sp')), parts along dimension 0
- output 8: float32 [4096], P(('dp', 'sp')), parts along dimension 0
- output 9: float32 [4096], P(('dp', 'sp')), parts along dimension 0
There are 2 independent parts. The reference program is written for one: setup_inputs(seed, part) draws one part's arguments, and reference() takes and returns one part's arrays. A program takes and returns all parts, laid end to end along the dimension named above; an argument that names none is the same for every part.
All inputs are finite; a program needn't handle non-finite values.
Results may differ from the reference program's by a relative error of at most 0.01132.
Values are sent between devices in bfloat16 or wider.
A program may use at most 1 GiB of HBM per device.

```python
import jax
import jax.numpy as jnp
from jax import lax

N_BATCH = 2
SEQ_LEN = 2048
D_MODEL = 2048
N_HEADS = 16
HEAD_DIM = 128
QUERY_BLOCK = min(128, SEQ_LEN)
NORM_EPS = 1e-5
ROPE_BASE = 10000.0
NEG_BIG = -1e30


def setup_inputs(seed: int = 0, part: int = 0) -> dict:
    part_key = jax.random.fold_in(jax.random.key(seed), part)
    key_x, key_dy, key_pos = jax.random.split(part_key, 3)
    weight_keys = jax.random.split(jax.random.key(seed + 1), 9)
    act_shape = (N_BATCH, SEQ_LEN, D_MODEL)
    x_in = jax.random.normal(key_x, act_shape, jnp.float32).astype(jnp.bfloat16)
    grad_y = jax.random.normal(key_dy, act_shape, jnp.float32).astype(jnp.bfloat16)
    tok_idx = jnp.arange(SEQ_LEN, dtype=jnp.int32)
    restart = jax.random.randint(key_pos, (N_BATCH, SEQ_LEN), 0, 256) == 0
    doc_start = lax.cummax(jnp.where(restart, tok_idx[None, :], 0), axis=1)
    positions = (tok_idx[None, :] - doc_start).astype(jnp.int32)
    fan_scale = D_MODEL ** -0.5
    head_q = jnp.repeat(jax.random.uniform(weight_keys[0], (N_HEADS,), jnp.float32, 0.5, 1.5), HEAD_DIM)
    head_k = jnp.repeat(jax.random.uniform(weight_keys[1], (N_HEADS,), jnp.float32, 0.5, 1.5), HEAD_DIM)
    w_shape = (D_MODEL, D_MODEL)
    w_query = (jax.random.normal(weight_keys[2], w_shape, jnp.float32) * fan_scale * head_q[None, :]).astype(jnp.bfloat16)
    w_key = (jax.random.normal(weight_keys[3], w_shape, jnp.float32) * fan_scale * head_k[None, :]).astype(jnp.bfloat16)
    w_value = (jax.random.normal(weight_keys[4], w_shape, jnp.float32) * fan_scale).astype(jnp.bfloat16)
    w_out = (jax.random.normal(weight_keys[5], w_shape, jnp.float32) * fan_scale).astype(jnp.bfloat16)
    g_norm = (1.0 + 0.3 * jax.random.normal(weight_keys[6], (D_MODEL,), jnp.float32)).astype(jnp.bfloat16)
    g_query = (1.7 + 0.4 * jax.random.normal(weight_keys[7], (D_MODEL,), jnp.float32)).astype(jnp.bfloat16)
    g_key = (1.7 + 0.4 * jax.random.normal(weight_keys[8], (D_MODEL,), jnp.float32)).astype(jnp.bfloat16)
    return {'x_in': x_in, 'grad_y': grad_y, 'positions': positions, 'g_norm': g_norm, 'w_query': w_query, 'w_key': w_key, 'w_value': w_value, 'w_out': w_out, 'g_query': g_query, 'g_key': g_key}


def rms_scale(values, gain_vec):
    inv_rms = lax.rsqrt(jnp.mean(values * values, axis=-1, keepdims=True) + NORM_EPS)
    return values * inv_rms * gain_vec


def rope_tables(positions):
    half_dim = HEAD_DIM // 2
    inv_freq = ROPE_BASE ** (-jnp.arange(half_dim, dtype=jnp.float32) * (2.0 / HEAD_DIM))
    angles = positions.astype(jnp.float32)[..., None] * inv_freq
    return jnp.cos(angles)[:, :, None, :], jnp.sin(angles)[:, :, None, :]


def rope_apply(values, cos_t, sin_t):
    half_dim = values.shape[-1] // 2
    first_half = values[..., :half_dim]
    second_half = values[..., half_dim:]
    return jnp.concatenate([first_half * cos_t - second_half * sin_t, second_half * cos_t + first_half * sin_t], axis=-1)


def mat_f32(left_op, right_op):
    return jnp.dot(left_op, right_op, precision=lax.Precision.HIGHEST)


def causal_attention(q_bf, k_bf, v_bf):
    q_f = q_bf.astype(jnp.float32)
    k_f = k_bf.astype(jnp.float32)
    v_f = v_bf.astype(jnp.float32)
    key_pos = jnp.arange(SEQ_LEN)
    qk_scale = HEAD_DIM ** -0.5

    def one_block(q_start):
        q_blk = lax.dynamic_slice_in_dim(q_f, q_start, QUERY_BLOCK, axis=1)
        scores = jnp.einsum('bqhd,bkhd->bhqk', q_blk, k_f, precision=lax.Precision.HIGHEST) * qk_scale
        q_pos = q_start + jnp.arange(QUERY_BLOCK)
        scores = jnp.where(q_pos[:, None] >= key_pos[None, :], scores, NEG_BIG)
        prob_f = jax.nn.softmax(scores, axis=-1)
        return jnp.einsum('bhqk,bkhd->bqhd', prob_f, v_f, precision=lax.Precision.HIGHEST)

    starts = jnp.arange(SEQ_LEN // QUERY_BLOCK) * QUERY_BLOCK
    blocks = lax.map(jax.checkpoint(one_block), starts)
    merged = jnp.moveaxis(blocks, 0, 1).reshape(q_bf.shape)
    return merged.astype(jnp.bfloat16)


def reference(x_in, grad_y, positions, g_norm, w_query, w_key, w_value, w_out, g_query, g_key):
    cos_t, sin_t = rope_tables(positions)
    head_shape = (N_BATCH, SEQ_LEN, N_HEADS, HEAD_DIM)
    flat_shape = (N_BATCH, SEQ_LEN, D_MODEL)

    def forward(x_f, gain_n, wq_f, wk_f, wv_f, wo_f, gain_q, gain_k):
        hidden = rms_scale(x_f, gain_n).astype(jnp.bfloat16).astype(jnp.float32)
        q_raw = mat_f32(hidden, wq_f)
        k_raw = mat_f32(hidden, wk_f)
        v_val = mat_f32(hidden, wv_f).astype(jnp.bfloat16)
        q_rot = rope_apply(rms_scale(q_raw, gain_q).reshape(head_shape), cos_t, sin_t).astype(jnp.bfloat16)
        k_rot = rope_apply(rms_scale(k_raw, gain_k).reshape(head_shape), cos_t, sin_t).astype(jnp.bfloat16)
        attended = causal_attention(q_rot, k_rot, v_val.reshape(head_shape))
        o_proj = mat_f32(attended.reshape(flat_shape).astype(jnp.float32), wo_f)
        return (x_f + o_proj).astype(jnp.bfloat16)

    y_out, pullback = jax.vjp(forward, x_in.astype(jnp.float32), g_norm.astype(jnp.float32), w_query.astype(jnp.float32), w_key.astype(jnp.float32), w_value.astype(jnp.float32), w_out.astype(jnp.float32), g_query.astype(jnp.float32), g_key.astype(jnp.float32))
    cotangents = pullback(grad_y)
    return (y_out, cotangents[0].astype(jnp.bfloat16), cotangents[1], cotangents[2], cotangents[3], cotangents[4], cotangents[5], cotangents[6], cotangents[7])
```

```python
import functools
import jax
import jax.numpy as jnp
from jax import lax
from jax.experimental import pallas as pl
from jax.experimental.pallas import tpu as pltpu
from jax.sharding import PartitionSpec as P

HEAD_DIM = 128
NORM_EPS = 1e-5
ROPE_BASE = 10000.0
NEG_BIG = -1e30
LOG2E = 1.4426950408889634
FWD_BLOCK = 1024
BWD_BLOCK = 512
F32, BF = jnp.float32, jnp.bfloat16
NT = (((1,), (1,)), ((), ()))


def rope_tables(positions):
    half = HEAD_DIM // 2
    inv_freq = ROPE_BASE ** (-jnp.arange(half, dtype=F32) * (2.0 / HEAD_DIM))
    angles = positions.astype(F32)[:, None] * inv_freq
    cos_t, sin_t = jnp.cos(angles), jnp.sin(angles)
    return jnp.concatenate([cos_t, cos_t], 1), jnp.concatenate([-sin_t, sin_t], 1)


def column(row):
    return jnp.broadcast_to(row, (HEAD_DIM, row.shape[1])).T


def as_row(col):
    return jnp.broadcast_to(col, (col.shape[0], HEAD_DIM)).T[0:1, :]


def half_roll(u):
    return pltpu.roll(u, HEAD_DIM // 2, 1)


def proj_kernel(h_ref, w_ref, st_ref, c_ref, s_ref, g_ref, q_ref, k_ref, v_ref, qh_ref, kh_ref):
    h = h_ref[0]
    cols = q_ref.shape[1]
    for idx, (out, hat_out) in enumerate(((q_ref, qh_ref), (k_ref, kh_ref))):
        raw = mm32(h, w_ref[:, idx * cols:(idx + 1) * cols])
        inv = column(st_ref[0, idx:idx + 1, :])
        for lo in range(0, cols, HEAD_DIM):
            hs = slice(lo, lo + HEAD_DIM)
            hat = raw[:, hs] * inv
            hat_out[:, hs] = hat
            u = hat * g_ref[idx:idx + 1, hs]
            out[:, hs] = (u * c_ref[...] + half_roll(u) * s_ref[...]).astype(BF)
    v_ref[...] = mm32(h, w_ref[:, 2 * cols:]).astype(BF)


def tok_kernel(dq_ref, dk_ref, qr_ref, kr_ref, st_ref, c_ref, s_ref, g_ref, qo_ref, ko_ref, row_ref, nrm_ref):
    n_chip, rows, cols = dq_ref.shape
    dim = n_chip * cols
    for idx, (d_ref, raw_ref, out) in enumerate(((dq_ref, qr_ref, qo_ref), (dk_ref, kr_ref, ko_ref))):
        inv = column(st_ref[idx:idx + 1, :])
        acc = jnp.zeros((rows, HEAD_DIM), F32)
        for lo in range(0, dim, HEAD_DIM):
            hs = slice(lo, lo + HEAD_DIM)
            d = d_ref[lo // cols, :, lo % cols:lo % cols + HEAD_DIM].astype(F32)
            nrm = (d * c_ref[...] - half_roll(d) * s_ref[...]) * g_ref[idx:idx + 1, hs]
            nrm_ref[:, hs] = nrm
            acc += nrm * (raw_ref[:, hs] * inv)
        row = jnp.sum(acc, axis=1, keepdims=True) / dim
        row_ref[idx:idx + 1, :] = as_row(row)
        for lo in range(0, dim, HEAD_DIM):
            hs = slice(lo, lo + HEAD_DIM)
            out[:, hs] = (inv * (nrm_ref[:, hs] - raw_ref[:, hs] * inv * row)).astype(BF)


def dw_qk_kernel(d_ref, hat_ref, st_ref, row_ref, c_ref, s_ref, g_ref, h_ref, out_ref, dg_ref, dt_ref, *, idx):
    n_chip, rows = st_ref.shape[0], st_ref.shape[2]
    cols = d_ref.shape[1]

    @pl.when(pl.program_id(0) == 0)
    def _():
        dg_ref[...] = jnp.zeros_like(dg_ref)
        for p in range(n_chip):
            ts = slice(p * rows, (p + 1) * rows)
            inv = column(st_ref[p, idx:idx + 1, :])
            row = column(row_ref[p, idx:idx + 1, :])
            for lo in range(0, cols, HEAD_DIM):
                hs = slice(lo, lo + HEAD_DIM)
                d = d_ref[ts, hs].astype(F32)
                rot = d * c_ref[ts, :] - half_roll(d) * s_ref[ts, :]
                hat = hat_ref[ts, hs]
                raw = inv * (rot * g_ref[idx:idx + 1, hs] - hat * row)
                dt_ref[hs, ts] = raw.astype(BF).T
                dg_ref[0:1, hs] += jnp.sum(rot * hat, axis=0, keepdims=True)

    dw_block(dt_ref, h_ref, out_ref)


def dw_v_kernel(d_ref, h_ref, out_ref, dt_ref):
    @pl.when(pl.program_id(0) == 0)
    def _():
        dt_ref[...] = d_ref[...].T

    dw_block(dt_ref, h_ref, out_ref)


def dw_block(dt_ref, h_ref, out_ref):
    dw = mm32(dt_ref[...], h_ref[...]).T
    half = out_ref.shape[2]
    out_ref[0, 0] = dw[:half]
    out_ref[0, 1] = dw[half:]


def attn_fwd_kernel(q_ref,k_ref,v_ref,o_ref,ot_ref,lse_ref,vt_ref,*,blk,heads):
    n=q_ref.shape[0]; nb=n//blk
    c=HEAD_DIM**-0.5*LOG2E
    for h in range(heads):
        vt_ref[h*HEAD_DIM:(h+1)*HEAD_DIM,:]=v_ref[:,h*HEAD_DIM:(h+1)*HEAD_DIM].T
    causal=(lax.broadcasted_iota(jnp.int32,(blk,blk),0)<=lax.broadcasted_iota(jnp.int32,(blk,blk),1))
    def qstep(j,_):
        qs=pl.ds(pl.multiple_of(j*blk,blk),blk)
        qb=[q_ref[qs,h*HEAD_DIM:(h+1)*HEAD_DIM] for h in range(heads)]
        def tile(i,carry,diag):
            ks=pl.ds(pl.multiple_of(i*blk,blk),blk)
            out=[]
            for h in range(heads):
                m,l,acc=carry[h]
                s=mm32_nt(k_ref[ks,h*HEAD_DIM:(h+1)*HEAD_DIM],qb[h])
                if diag: s=jnp.where(causal,s,NEG_BIG)
                mn=jnp.maximum(m,jnp.max(s,axis=0,keepdims=True))
                al=jnp.exp2((m-mn)*c)
                p=jnp.exp2((s-mn)*c)
                l=al*l+jnp.sum(p,axis=0,keepdims=True)
                acc=al*acc+mm32(vt_ref[h*HEAD_DIM:(h+1)*HEAD_DIM,ks],p.astype(BF))
                out.append((mn,l,acc))
            return tuple(out)
        init=tuple((jnp.full((1,blk),NEG_BIG,F32),jnp.zeros((1,blk),F32),jnp.zeros((HEAD_DIM,blk),F32)) for _ in range(heads))
        st=lax.fori_loop(0,j,lambda i,cr:tile(i,cr,False),init)
        st=tile(j,st,True)
        for h in range(heads):
            m,l,acc=st[h]
            ot=acc/l
            ot_ref[h*HEAD_DIM:(h+1)*HEAD_DIM,qs]=ot
            o_ref[qs,h*HEAD_DIM:(h+1)*HEAD_DIM]=ot.T.astype(BF)
            lse_ref[h:h+1,qs]=m*c+jnp.log2(l)
        return 0
    lax.fori_loop(0,nb,qstep,0)

def attn_bwd_kernel(q_ref,k_ref,v_ref,do_ref,ot_ref,lse_ref,dq_ref,dk_ref,dv_ref,kt_ref,dka_ref,dva_ref,*,blk,heads):
    n=q_ref.shape[0]; nb=n//blk
    sc=HEAD_DIM**-0.5; c=sc*LOG2E
    for h in range(heads):
        kt_ref[h*HEAD_DIM:(h+1)*HEAD_DIM,:]=k_ref[:,h*HEAD_DIM:(h+1)*HEAD_DIM].T
    dka_ref[...]=jnp.zeros_like(dka_ref); dva_ref[...]=jnp.zeros_like(dva_ref)
    causal=(lax.broadcasted_iota(jnp.int32,(blk,blk),0)<=lax.broadcasted_iota(jnp.int32,(blk,blk),1))
    def qstep(j,_):
        qs=pl.ds(pl.multiple_of(j*blk,blk),blk)
        hs=[slice(h*HEAD_DIM,(h+1)*HEAD_DIM) for h in range(heads)]
        qb=[q_ref[qs,s] for s in hs]; dob=[do_ref[qs,s] for s in hs]
        lse=[lse_ref[h:h+1,qs] for h in range(heads)]
        dl=[jnp.sum(ot_ref[hs[h],qs]*dob[h].astype(F32).T,axis=0,keepdims=True) for h in range(heads)]
        def tile(i,carry,diag):
            ks=pl.ds(pl.multiple_of(i*blk,blk),blk)
            out=[]
            for h in range(heads):
                s=mm32_nt(k_ref[ks,hs[h]],qb[h])
                dp=mm32_nt(v_ref[ks,hs[h]],dob[h])
                p=jnp.exp2(s*c-lse[h])
                if diag: p=jnp.where(causal,p,0.0)
                ds=(p*(dp-dl[h])).astype(BF)
                dva_ref[ks,hs[h]]+=mm32(p.astype(BF),dob[h])
                dka_ref[ks,hs[h]]+=mm32(ds,qb[h])
                out.append(carry[h]+mm32(kt_ref[hs[h],ks],ds))
            return tuple(out)
        st=tuple(jnp.zeros((HEAD_DIM,blk),F32) for _ in range(heads))
        st=lax.fori_loop(0,j,lambda i,cr:tile(i,cr,False),st)
        st=tile(j,st,True)
        for h in range(heads):
            dq_ref[qs,hs[h]]=(st[h]*sc).T.astype(BF)
        return 0
    lax.fori_loop(0,nb,qstep,0)
    dk_ref[...]=(dka_ref[...]*sc).astype(BF)
    dv_ref[...]=dva_ref[...].astype(BF)


VM = pl.BlockSpec(memory_space=pltpu.VMEM)


def attn_fwd(q, k, v):
    n, d = q.shape
    heads = d // HEAD_DIM
    return pl.pallas_call(
        functools.partial(attn_fwd_kernel, blk=FWD_BLOCK, heads=heads),
        out_shape=(jax.ShapeDtypeStruct((n, d), BF), jax.ShapeDtypeStruct((d, n), F32), jax.ShapeDtypeStruct((heads, n), F32)),
        in_specs=[VM] * 3, out_specs=(VM,) * 3, scratch_shapes=[pltpu.VMEM((d, n), BF)], name='attn_fwd',
        cost_estimate=pl.CostEstimate(flops=8 * n * n * d, bytes_accessed=12 * n * d, transcendentals=n * n * heads // 2),
    )(q, k, v)


def attn_bwd(q, k, v, do, ot, lse):
    n, d = q.shape
    heads = d // HEAD_DIM
    return pl.pallas_call(
        functools.partial(attn_bwd_kernel, blk=BWD_BLOCK, heads=heads),
        out_shape=(jax.ShapeDtypeStruct((n, d), BF),) * 3,
        in_specs=[VM] * 6, out_specs=(VM,) * 3,
        scratch_shapes=[pltpu.VMEM((d, n), BF), pltpu.VMEM((n, d), F32), pltpu.VMEM((n, d), F32)], name='attn_bwd',
        cost_estimate=pl.CostEstimate(flops=12 * n * n * d, bytes_accessed=20 * n * d, transcendentals=n * n * heads // 2),
    )(q, k, v, do, ot, lse)


def mm32(a, b):
    return jnp.dot(a, b, preferred_element_type=F32)


def mm32_nt(a, b):
    return lax.dot_general(a, b, NT, preferred_element_type=F32)


def whole(shape):
    return pl.BlockSpec(shape, lambda p: (0,) * len(shape))


def project_heads(hid, w_cat, stats, cos_a, sin_a, gains):
    n_chip, rows, dim = hid.shape
    cols = w_cat.shape[1] // 3
    n = n_chip * rows
    block = pl.BlockSpec((rows, cols), lambda p: (p, 0))
    table = pl.BlockSpec((rows, HEAD_DIM), lambda p: (p, 0))
    return pl.pallas_call(
        proj_kernel, grid=(n_chip,), name='proj',
        out_shape=(jax.ShapeDtypeStruct((n, cols), BF),) * 3 + (jax.ShapeDtypeStruct((n, cols), F32),) * 2,
        in_specs=[pl.BlockSpec((1, rows, dim), lambda p: (p, 0, 0)), whole(w_cat.shape), pl.BlockSpec((1,) + stats.shape[1:], lambda p: (p, 0, 0)), table, table, whole(gains.shape)],
        out_specs=(block,) * 5,
        cost_estimate=pl.CostEstimate(flops=6 * n * dim * cols, bytes_accessed=2 * n * dim + 20 * n * cols, transcendentals=0),
    )(hid, w_cat, stats, cos_a, sin_a, gains)


def token_back(dq, dk, q_raw, k_raw, st, cos_t, sin_t, gains):
    rows, dim = q_raw.shape
    return pl.pallas_call(
        tok_kernel, name='tok_back', in_specs=[VM] * 8, out_specs=(VM,) * 3,
        out_shape=(jax.ShapeDtypeStruct((rows, dim), BF),) * 2 + (jax.ShapeDtypeStruct((2, rows), F32),),
        scratch_shapes=[pltpu.VMEM((rows, dim), F32)],
        cost_estimate=pl.CostEstimate(flops=200 * rows * dim, bytes_accessed=16 * rows * dim, transcendentals=0),
    )(dq, dk, q_raw, k_raw, st, cos_t, sin_t, gains)


def weight_back(d, hid, extra=None, idx=0):
    n, cols = d.shape
    dim = hid.shape[1]
    n_chip = dim // cols
    out_shape = jax.ShapeDtypeStruct((n_chip, 2, cols // 2, cols), F32)
    out_spec = pl.BlockSpec((1, 2, cols // 2, cols), lambda p: (p, 0, 0, 0))
    h_spec = pl.BlockSpec((n, cols), lambda p: (0, p))
    scratch = [pltpu.VMEM((cols, n), BF)]
    cost = pl.CostEstimate(flops=2 * n * cols * dim, bytes_accessed=2 * n * dim + 4 * cols * dim, transcendentals=0)
    if extra is None:
        return pl.pallas_call(dw_v_kernel, grid=(n_chip,), name='dw_v', out_shape=out_shape, in_specs=[whole(d.shape), h_spec], out_specs=out_spec, scratch_shapes=scratch, cost_estimate=cost)(d, hid)
    return pl.pallas_call(
        functools.partial(dw_qk_kernel, idx=idx), grid=(n_chip,), name='dw_qk',
        out_shape=(out_shape, jax.ShapeDtypeStruct((8, cols), F32)),
        in_specs=[whole(d.shape)] + [whole(e.shape) for e in extra] + [h_spec],
        out_specs=(out_spec, whole((8, cols))), scratch_shapes=scratch, cost_estimate=cost,
    )(d, *extra, hid)


def solution(mesh):
    n_sp = mesh.shape['sp']
    n_chip = n_sp // 2
    same_core = [[2 * p + c for p in range(n_chip)] for c in range(2)]
    pairs = [(i, i ^ 1) for i in range(n_sp)]

    def swap(t):
        return lax.ppermute(t, 'sp', pairs)

    def gather(t):
        return lax.all_gather(t, 'sp', axis=0, axis_index_groups=same_core)

    def exchange(t):
        return lax.all_to_all(t, 'sp', split_axis=0, concat_axis=0, axis_index_groups=same_core)

    def device_step(x_loc, gy_loc, positions, g_norm, w_query, w_key, w_value, w_out, g_query, g_key):
        me = lax.axis_index('sp')
        chip, core = me // 2, me % 2
        first = core == 0
        loc, dim = x_loc.shape[1], x_loc.shape[2]
        rows = 2 * loc
        cols = dim // n_chip

        def pick(t, idx):
            return lax.dynamic_index_in_dim(t, idx, 0, keepdims=False)

        def join(mine, other):
            return jnp.where(first, jnp.concatenate([mine, other], 0), jnp.concatenate([other, mine], 0))

        def to_core(t):
            return join(pick(t, core), swap(pick(t, 1 - core)))

        def from_core(t):
            halves = t.reshape(2, loc, dim)
            mine, other = pick(halves, core), swap(pick(halves, 1 - core))
            return jnp.where(first, jnp.stack([mine, other]), jnp.stack([other, mine]))

        def my_cols(w):
            return lax.dynamic_slice_in_dim(w, chip * cols, cols, axis=1)

        def inv_of(raw):
            return lax.rsqrt(jnp.mean(raw * raw, axis=-1, keepdims=True) + NORM_EPS)

        def spread(t):
            return exchange(jnp.broadcast_to(t[None], (n_chip,) + t.shape))

        x_f = to_core(x_loc).astype(F32)
        gy = to_core(gy_loc)
        pos = to_core(positions)
        x_inv = inv_of(x_f)
        x_hat = x_f * x_inv
        hidden = (x_hat * g_norm.astype(F32)).astype(BF)
        hid_all = gather(hidden)
        gy_tied, _ = lax.optimization_barrier((gy, hidden))
        gy_all = gather(gy_tied).reshape(n_chip * rows, dim)
        q_raw, k_raw = mm32(hidden, w_query), mm32(hidden, w_key)
        st = jnp.stack([inv_of(q_raw)[:, 0], inv_of(k_raw)[:, 0], pos.astype(F32)])
        cos_t, sin_t = rope_tables(pos)
        stats = spread(st)

        cos_a, sin_a = rope_tables(stats[:, 2].reshape(n_chip * rows))
        gains = jnp.stack([g_query, g_key]).astype(F32)
        gains_h = lax.dynamic_slice_in_dim(gains, chip * cols, cols, axis=1)
        w_cat = jnp.concatenate([my_cols(w_query), my_cols(w_key), my_cols(w_value)], 1)
        q, k, v, qh_hat, kh_hat = project_heads(hid_all, w_cat, stats, cos_a, sin_a, gains_h)
        hid_all = hid_all.reshape(n_chip * rows, dim)
        att, att_t, lse = attn_fwd(q, k, v)

        def to_tokens(t):
            return exchange(t.reshape(n_chip, rows, cols))

        def flat(t):
            return jnp.moveaxis(t, 0, 1).reshape(rows, dim)

        att_tok = to_tokens(att)
        att_tok, gy_all = lax.optimization_barrier((att_tok, gy_all))
        y = (x_f + mm32(flat(att_tok), w_out)).astype(BF)
        w_rows = lax.dynamic_slice_in_dim(w_out, chip * cols, cols, axis=0)
        d_att = mm32_nt(gy_all, w_rows).astype(BF)
        dq, dk, dv = attn_bwd(q, k, v, d_att, att_t, lse)
        dq_tok, dk_tok, dv_tok = to_tokens(dq), to_tokens(dk), to_tokens(dv)

        dwo = mm32(att_t.astype(BF), gy_all).reshape(2, loc, dim)
        dwo = pick(dwo, core) + swap(pick(dwo, 1 - core))

        def finish_cols(part):
            mine = lax.dynamic_index_in_dim(part, core, 1, keepdims=False)
            other = lax.dynamic_index_in_dim(part, 1 - core, 1, keepdims=False)
            return jnp.moveaxis(exchange(mine + swap(other)), 0, 1).reshape(loc, dim)

        dwv = finish_cols(weight_back(dv, hid_all))
        dq_raw, dk_raw, rowst = token_back(dq_tok, dk_tok, q_raw, k_raw, st, cos_t, sin_t, gains)
        row_all = spread(rowst)
        dwq, dgq = weight_back(dq, hid_all, (qh_hat, stats, row_all, cos_a, sin_a, gains_h), 0)
        dwk, dgk = weight_back(dk, hid_all, (kh_hat, stats, row_all, cos_a, sin_a, gains_h), 1)
        dwq, dwk = finish_cols(dwq), finish_cols(dwk)
        dg = jnp.stack([dgq[0], dgk[0]]).reshape(2, 2, loc)
        dg = jnp.moveaxis(dg, 1, 0)
        dg = pick(dg, core) + swap(pick(dg, 1 - core))

        d_hid = mm32_nt(flat(dv_tok), w_value) + mm32_nt(dq_raw, w_query) + mm32_nt(dk_raw, w_key)
        d_nrm = d_hid * g_norm.astype(F32)
        dxn = x_inv * (d_nrm - x_hat * jnp.mean(d_nrm * x_hat, axis=-1, keepdims=True))
        grad_x = (gy.astype(F32) + dxn).astype(BF)
        dgn = jnp.sum(d_hid * x_hat, axis=0).reshape(n_sp, loc)
        dgn = jnp.sum(lax.all_to_all(dgn, 'sp', split_axis=0, concat_axis=0), axis=0)
        return from_core(y), from_core(grad_x), dgn, dwq, dwk, dwv, dwo, dg[0], dg[1]

    seq_spec = P('dp', 'sp', None)
    mat_rep = P(None, None)
    vec_rep = P(None)
    row_spec = P(('dp', 'sp'), None)
    vec_spec = P(('dp', 'sp'))
    return jax.shard_map(device_step, mesh=mesh, in_specs=(seq_spec, seq_spec, P('dp', 'sp'), vec_rep, mat_rep, mat_rep, mat_rep, mat_rep, vec_rep, vec_rep), out_specs=(seq_spec, seq_spec, vec_spec, row_spec, row_spec, row_spec, row_spec, vec_spec, vec_spec), check_vma=False)
```

```python
import functools
import jax
import jax.numpy as jnp
from jax import lax
from jax.experimental import pallas as pl
from jax.experimental.pallas import tpu as pltpu
from jax.sharding import PartitionSpec as P

HEAD_DIM = 128
NORM_EPS = 1e-5
ROPE_BASE = 10000.0
NEG_BIG = -1e30
LOG2E = 1.4426950408889634
FWD_BLOCK = 512
CHUNKS = 4
BWD_BLOCK = 512
F32, BF = jnp.float32, jnp.bfloat16
NT = (((1,), (1,)), ((), ()))


def rope_rows():
    half = HEAD_DIM // 2
    inv_freq = ROPE_BASE ** (-jnp.arange(half, dtype=F32) * (2.0 / HEAD_DIM))
    sign = jnp.concatenate([-jnp.ones(half, F32), jnp.ones(half, F32)])
    return jnp.stack([jnp.concatenate([inv_freq, inv_freq]), sign])


def column(row):
    return jnp.broadcast_to(row, (HEAD_DIM, row.shape[1])).T


def as_row(col):
    return jnp.broadcast_to(col, (col.shape[0], HEAD_DIM)).T[0:1, :]


def half_roll(u):
    return pltpu.roll(u, HEAD_DIM // 2, 1)


def tok_kernel(dq_ref, dk_ref, qr_ref, kr_ref, st_ref, c_ref, s_ref, g_ref, qo_ref, ko_ref, row_ref, nrm_ref):
    n_chip, rows, cols = dq_ref.shape
    dim = n_chip * cols
    for idx, (d_ref, raw_ref, out) in enumerate(((dq_ref, qr_ref, qo_ref), (dk_ref, kr_ref, ko_ref))):
        inv = column(st_ref[idx:idx + 1, :])
        acc = jnp.zeros((rows, HEAD_DIM), F32)
        for lo in range(0, dim, HEAD_DIM):
            hs = slice(lo, lo + HEAD_DIM)
            d = d_ref[lo // cols, :, lo % cols:lo % cols + HEAD_DIM].astype(F32)
            nrm = (d * c_ref[...] - half_roll(d) * s_ref[...]) * g_ref[idx:idx + 1, hs]
            nrm_ref[:, hs] = nrm
            acc += nrm * (raw_ref[:, hs] * inv)
        row = jnp.sum(acc, axis=1, keepdims=True) / dim
        row_ref[idx:idx + 1, :] = as_row(row)
        for lo in range(0, dim, HEAD_DIM):
            hs = slice(lo, lo + HEAD_DIM)
            out[:, hs] = (inv * (nrm_ref[:, hs] - raw_ref[:, hs] * inv * row)).astype(BF)


def dw_qk_kernel(d_ref, hat_ref, st_ref, row_ref, c_ref, s_ref, g_ref, h_ref, out_ref, dg_ref, dt_ref, *, idx):
    n_chip, rows = row_ref.shape[0], row_ref.shape[2]
    cols = d_ref.shape[1]

    @pl.when(pl.program_id(0) == 0)
    def _():
        dg_ref[...] = jnp.zeros_like(dg_ref)
        for p in range(n_chip):
            ts = slice(p * rows, (p + 1) * rows)
            inv = column(st_ref[idx * n_chip + p:idx * n_chip + p + 1, :])
            row = column(row_ref[p, idx:idx + 1, :])
            for lo in range(0, cols, HEAD_DIM):
                hs = slice(lo, lo + HEAD_DIM)
                d = d_ref[ts, hs].astype(F32)
                rot = d * c_ref[ts, :] - half_roll(d) * s_ref[ts, :]
                hat = hat_ref[ts, hs]
                raw = inv * (rot * g_ref[idx:idx + 1, hs] - hat * row)
                dt_ref[hs, ts] = raw.astype(BF).T
                dg_ref[0:1, hs] += jnp.sum(rot * hat, axis=0, keepdims=True)

    dw_block(dt_ref, h_ref, out_ref)


def dw_v_kernel(d_ref, h_ref, out_ref, dt_ref):
    @pl.when(pl.program_id(0) == 0)
    def _():
        dt_ref[...] = d_ref[...].T

    dw_block(dt_ref, h_ref, out_ref)


def dw_block(dt_ref, h_ref, out_ref):
    dw = mm32(dt_ref[...], h_ref[...]).T
    half = out_ref.shape[2]
    out_ref[0, 0] = dw[:half]
    out_ref[0, 1] = dw[half:]


def front_kernel(h_ref, gy_ref, pos_ref, w_ref, wrow_ref, g_ref, f_ref,
                 hall_ref, q_ref, k_ref, v_ref, qh_ref, kh_ref, ot_ref, lse_ref, atok_ref, datt_ref, dwo_ref, c_ref, s_ref, inv_ref,
                 buf, att_ref, vt_ref, pos_all, ssq, ssq_all,
                 load_sem, out_sem, ssem, rsem, ps_sem, pr_sem, qs_sem, qr_sem, as_sem, ar_sem):
    me = lax.axis_index('sp')
    chip, core = me // 2, lax.rem(me, 2)
    n_chip, rows, dim = hall_ref.shape
    cols = q_ref.shape[1]
    part = rows // CHUNKS
    half = n_chip // 2
    heads = [slice(lo, lo + HEAD_DIM) for lo in range(0, cols, HEAD_DIM)]

    def spot(p):
        z, y = p // 2, lax.rem(p, 2)
        return z + y * (n_chip - 1 - 2 * z)

    def chip_at(r):
        y = r // half
        return 2 * (r + y * (n_chip - 1 - 2 * r)) + y

    ring = spot(chip)

    def slot_at(dr, dist):
        step = dist if dr == 0 else -dist
        return chip_at(lax.rem(ring - step + 2 * n_chip, n_chip))

    def dev(p):
        return {'sp': 2 * p + core}

    right = dev(slot_at(1, 1))
    left = dev(slot_at(0, 1))

    def hop(t, dr, s, c, dist):
        view = buf.at[t, slot_at(dr, dist), pl.ds(c * part, part)]
        return pltpu.make_async_remote_copy(
            src_ref=view, dst_ref=view, send_sem=ssem.at[t, dr, s, c], recv_sem=rsem.at[t, dr, s, c],
            device_id=right if dr == 0 else left, device_id_type=pl.DeviceIdType.MESH)

    def in_half(dr, c):
        return (c < CHUNKS // 2) == (dr == 0)

    def start_own(t):
        for c in range(CHUNKS):
            for dr in range(2):
                hop(t, dr, 0, c, 0).start()

    def stage(t, s):
        for c in range(CHUNKS):
            for dr in range(2):
                hop(t, dr, s, c, s + 1).wait_recv()
                if in_half(dr, c):
                    hop(t, dr, s + 1, c, s + 1).start()
                else:
                    @pl.when(s < half - 2)
                    def _():
                        hop(t, dr, s + 1, c, s + 1).start()

    def last_stage(t):
        for c in range(CHUNKS):
            for dr in range(2):
                if in_half(dr, c):
                    hop(t, dr, half - 1, c, half).wait_recv()

    def drain(t):
        for s in range(half):
            for c in range(CHUNKS):
                for dr in range(2):
                    if s < half - 1 or in_half(dr, c):
                        hop(t, dr, s, c, s).wait_send()

    def to_peers(src, dst, s_sem, r_sem):
        def make(p, owner):
            return pltpu.make_async_remote_copy(
                src_ref=src, dst_ref=dst.at[owner], send_sem=s_sem.at[p], recv_sem=r_sem.at[owner],
                device_id=dev(p), device_id_type=pl.DeviceIdType.MESH)
        return make

    def each_peer(fn):
        for p in range(n_chip):
            @pl.when(p != chip)
            def _():
                fn(p)

    loads = [pltpu.make_async_copy(src, buf.at[t, chip], load_sem.at[t]) for t, src in enumerate((h_ref, gy_ref))]
    for ld in loads:
        ld.start()
    barrier = pltpu.get_barrier_semaphore()
    each_peer(lambda p: pl.semaphore_signal(barrier, inc=1, device_id=dev(p), device_id_type=pl.DeviceIdType.MESH))
    pl.semaphore_wait(barrier, n_chip - 1)
    pos_copy = to_peers(pos_ref, pos_all, ps_sem, pr_sem)
    each_peer(lambda p: pos_copy(p, chip).start())
    pos_all[chip] = pos_ref[...]
    loads[0].wait()
    start_own(0)

    def project(p):
        ts = pl.ds(pl.multiple_of(p * rows, rows), rows)
        h = buf[0, p]
        for idx, out in enumerate((qh_ref, kh_ref)):
            raw = mm32(h, w_ref[:, idx * cols:(idx + 1) * cols])
            out[ts, :] = raw
            ssq[pl.ds(idx * n_chip + p, 1), :] = as_row(jnp.sum(raw * raw, axis=1, keepdims=True))
        v_ref[ts, :] = mm32(h, w_ref[:, 2 * cols:]).astype(BF)

    project(chip)
    each_peer(lambda p: pos_copy(p, p).wait_recv())
    for p in range(n_chip):
        angles = column(pos_all[p, 0:1, :]) * f_ref[0:1, :]
        c_ref[p * rows:(p + 1) * rows, :] = jnp.cos(angles)
        s_ref[p * rows:(p + 1) * rows, :] = jnp.sin(angles) * f_ref[1:2, :]

    def gather_step(s, _):
        stage(0, s)

        def both(dr, _):
            dist = (s + 1) * (1 - 2 * dr)
            project(chip_at(lax.rem(ring - dist + 2 * n_chip, n_chip)))
            return 0

        lax.fori_loop(0, 2, both, 0)
        return 0

    lax.fori_loop(0, half - 1, gather_step, 0)
    loads[1].wait()
    start_own(1)
    last_stage(0)
    project(slot_at(0, half))
    hall_copy = pltpu.make_async_copy(buf.at[0], hall_ref, out_sem)
    hall_copy.start()
    for hs in heads:
        vt_ref[hs, :] = v_ref[:, hs].T
    ssq_copy = to_peers(ssq, ssq_all, qs_sem, qr_sem)
    each_peer(lambda p: ssq_copy(p, chip).start())
    ssq_all[chip] = ssq[...]
    each_peer(lambda p: ssq_copy(p, p).wait_recv())
    total = ssq_all[0]
    for p in range(1, n_chip):
        total = total + ssq_all[p]
    inv_ref[...] = lax.rsqrt(total / dim + NORM_EPS)

    def finish_qk(p, _):
        ts = pl.ds(pl.multiple_of(p * rows, rows), rows)
        for idx, (hat_ref, out) in enumerate(((qh_ref, q_ref), (kh_ref, k_ref))):
            inv = column(inv_ref[pl.ds(idx * n_chip + p, 1), :])
            for hs in heads:
                hat = hat_ref[ts, hs] * inv
                hat_ref[ts, hs] = hat
                u = hat * g_ref[idx:idx + 1, hs]
                out[ts, hs] = (u * c_ref[ts, :] + half_roll(u) * s_ref[ts, :]).astype(BF)
        return 0

    lax.fori_loop(0, n_chip, finish_qk, 0)

    blk = FWD_BLOCK
    scale = HEAD_DIM ** -0.5 * LOG2E
    causal = lax.broadcasted_iota(jnp.int32, (blk, blk), 0) <= lax.broadcasted_iota(jnp.int32, (blk, blk), 1)

    def attend(j, _):
        qs = pl.ds(pl.multiple_of(j * blk, blk), blk)
        qb = [q_ref[qs, hs] for hs in heads]

        def tile(i, carry, diag):
            ks = pl.ds(pl.multiple_of(i * blk, blk), blk)
            out = []
            for h, hs in enumerate(heads):
                m, l, acc = carry[h]
                s = mm32_nt(k_ref[ks, hs], qb[h])
                if diag:
                    s = jnp.where(causal, s, NEG_BIG)
                mn = jnp.maximum(m, jnp.max(s, axis=0, keepdims=True))
                al = jnp.exp2((m - mn) * scale)
                p = jnp.exp2((s - mn) * scale)
                l = al * l + jnp.sum(p, axis=0, keepdims=True)
                out.append((mn, l, al * acc + mm32(vt_ref[hs, ks], p.astype(BF))))
            return tuple(out)

        st = tuple((jnp.full((1, blk), NEG_BIG, F32), jnp.zeros((1, blk), F32), jnp.zeros((HEAD_DIM, blk), F32)) for _ in heads)
        st = lax.fori_loop(0, j, lambda i, cr: tile(i, cr, False), st)
        st = tile(j, st, True)
        for h, hs in enumerate(heads):
            m, l, acc = st[h]
            ot = acc / l
            ot_ref[hs, qs] = ot
            att_ref[qs, hs] = ot.T.astype(BF)
            lse_ref[h:h + 1, qs] = m * scale + jnp.log2(l)
        return 0

    def att_copy(p, owner):
        return pltpu.make_async_remote_copy(
            src_ref=att_ref.at[pl.ds(p * rows, rows)], dst_ref=atok_ref.at[owner], send_sem=as_sem.at[p], recv_sem=ar_sem.at[owner],
            device_id=dev(p), device_id_type=pl.DeviceIdType.MESH)

    def send_att(lo, hi):
        for p in range(lo, hi):
            @pl.when(p != chip)
            def _():
                att_copy(p, chip).start()

    def use_gy(p):
        ts = pl.ds(pl.multiple_of(p * rows, rows), rows)
        gy = buf[1, p]
        datt_ref[ts, :] = mm32_nt(gy, wrow_ref[...]).astype(BF)
        dwo_ref[...] += mm32(ot_ref[:, ts].astype(BF), gy)

    n_att = n_chip * rows // blk
    lax.fori_loop(0, n_att // 2, attend, 0)
    stage(1, 0)
    send_att(0, half)
    lax.fori_loop(n_att // 2, n_att, attend, 0)
    stage(1, 1)
    send_att(half, n_chip)
    atok_ref[chip] = att_ref[pl.ds(pl.multiple_of(chip * rows, rows), rows), :]
    dwo_ref[...] = jnp.zeros_like(dwo_ref)

    def use_ring(n, _):
        dist = ((n + 1) // 2) * (2 * lax.rem(n, 2) - 1)
        use_gy(chip_at(lax.rem(ring - dist + 2 * n_chip, n_chip)))
        return 0

    lax.fori_loop(0, n_chip - 3, use_ring, 0)
    stage(1, half - 2)
    lax.fori_loop(n_chip - 3, n_chip - 1, use_ring, 0)
    last_stage(1)
    use_gy(slot_at(0, half))

    each_peer(lambda p: att_copy(p, p).wait_recv())
    each_peer(lambda p: att_copy(p, chip).wait_send())
    each_peer(lambda p: pos_copy(p, chip).wait_send())
    each_peer(lambda p: ssq_copy(p, chip).wait_send())
    drain(0)
    drain(1)
    hall_copy.wait()


def attn_bwd_kernel(q_ref,k_ref,v_ref,do_ref,ot_ref,lse_ref,dq_ref,dk_ref,dv_ref,kt_ref,dka_ref,dva_ref,*,blk,heads):
    n=q_ref.shape[0]; nb=n//blk
    sc=HEAD_DIM**-0.5; c=sc*LOG2E
    for h in range(heads):
        kt_ref[h*HEAD_DIM:(h+1)*HEAD_DIM,:]=k_ref[:,h*HEAD_DIM:(h+1)*HEAD_DIM].T
    dka_ref[...]=jnp.zeros_like(dka_ref); dva_ref[...]=jnp.zeros_like(dva_ref)
    causal=(lax.broadcasted_iota(jnp.int32,(blk,blk),0)<=lax.broadcasted_iota(jnp.int32,(blk,blk),1))
    def qstep(j,_):
        qs=pl.ds(pl.multiple_of(j*blk,blk),blk)
        hs=[slice(h*HEAD_DIM,(h+1)*HEAD_DIM) for h in range(heads)]
        qb=[q_ref[qs,s] for s in hs]; dob=[do_ref[qs,s] for s in hs]
        lse=[lse_ref[h:h+1,qs] for h in range(heads)]
        dl=[jnp.sum(ot_ref[hs[h],qs]*dob[h].astype(F32).T,axis=0,keepdims=True) for h in range(heads)]
        def tile(i,carry,diag):
            ks=pl.ds(pl.multiple_of(i*blk,blk),blk)
            out=[]
            for h in range(heads):
                s=mm32_nt(k_ref[ks,hs[h]],qb[h])
                dp=mm32_nt(v_ref[ks,hs[h]],dob[h])
                p=jnp.exp2(s*c-lse[h])
                if diag: p=jnp.where(causal,p,0.0)
                ds=(p*(dp-dl[h])).astype(BF)
                dva_ref[ks,hs[h]]+=mm32(p.astype(BF),dob[h])
                dka_ref[ks,hs[h]]+=mm32(ds,qb[h])
                out.append(carry[h]+mm32(kt_ref[hs[h],ks],ds))
            return tuple(out)
        st=tuple(jnp.zeros((HEAD_DIM,blk),F32) for _ in range(heads))
        st=lax.fori_loop(0,j,lambda i,cr:tile(i,cr,False),st)
        st=tile(j,st,True)
        for h in range(heads):
            dq_ref[qs,hs[h]]=(st[h]*sc).T.astype(BF)
        return 0
    lax.fori_loop(0,nb,qstep,0)
    dk_ref[...]=(dka_ref[...]*sc).astype(BF)
    dv_ref[...]=dva_ref[...].astype(BF)


VM = pl.BlockSpec(memory_space=pltpu.VMEM)


def attn_bwd(q, k, v, do, ot, lse):
    n, d = q.shape
    heads = d // HEAD_DIM
    return pl.pallas_call(
        functools.partial(attn_bwd_kernel, blk=BWD_BLOCK, heads=heads),
        out_shape=(jax.ShapeDtypeStruct((n, d), BF),) * 3,
        in_specs=[VM] * 6, out_specs=(VM,) * 3,
        scratch_shapes=[pltpu.VMEM((d, n), BF), pltpu.VMEM((n, d), F32), pltpu.VMEM((n, d), F32)], name='attn_bwd',
        cost_estimate=pl.CostEstimate(flops=12 * n * n * d, bytes_accessed=20 * n * d, transcendentals=n * n * heads // 2),
    )(q, k, v, do, ot, lse)


def mm32(a, b):
    return jnp.dot(a, b, preferred_element_type=F32)


def mm32_nt(a, b):
    return lax.dot_general(a, b, NT, preferred_element_type=F32)


def whole(shape):
    return pl.BlockSpec(shape, lambda p: (0,) * len(shape))


def front(hid, gy, pos, w_cat, w_rows, gains, freq, n_chip):
    rows, dim = hid.shape
    cols = w_rows.shape[0]
    n = n_chip * rows
    heads = cols // HEAD_DIM
    any_spec = pl.BlockSpec(memory_space=pl.ANY)
    half = n_chip // 2
    dma = pltpu.SemaphoreType.DMA
    outs = [((n_chip, rows, dim), BF), ((n, cols), BF), ((n, cols), BF), ((n, cols), BF), ((n, cols), F32), ((n, cols), F32), ((cols, n), F32), ((heads, n), F32),
            ((n_chip, rows, cols), BF), ((n, cols), BF), ((cols, dim), F32), ((n, HEAD_DIM), F32), ((n, HEAD_DIM), F32), ((2 * n_chip, rows), F32)]
    return pl.pallas_call(
        front_kernel, name='front', out_shape=tuple(jax.ShapeDtypeStruct(s, d) for s, d in outs),
        in_specs=[any_spec, any_spec] + [VM] * 5, out_specs=(any_spec,) + (VM,) * 13,
        scratch_shapes=[
            pltpu.VMEM((2, n_chip, rows, dim), BF), pltpu.VMEM((n, cols), BF), pltpu.VMEM((cols, n), BF),
            pltpu.VMEM((n_chip, 8, rows), F32), pltpu.VMEM((2 * n_chip, rows), F32), pltpu.VMEM((n_chip, 2 * n_chip, rows), F32),
            dma((2,)), dma(()), dma((2, 2, half, CHUNKS)), dma((2, 2, half, CHUNKS)),
            dma((n_chip,)), dma((n_chip,)), dma((n_chip,)), dma((n_chip,)), dma((n_chip,)), dma((n_chip,))],
        compiler_params=pltpu.CompilerParams(collective_id=0, has_side_effects=True, vmem_limit_bytes=67043328),
        cost_estimate=pl.CostEstimate(flops=400 * n * dim * cols, bytes_accessed=40 * n * dim, transcendentals=n * n * heads // 2),
    )(hid, gy, pos, w_cat, w_rows, gains, freq)


def token_back(dq, dk, q_raw, k_raw, st, cos_t, sin_t, gains):
    rows, dim = q_raw.shape
    return pl.pallas_call(
        tok_kernel, name='tok_back', in_specs=[VM] * 8, out_specs=(VM,) * 3,
        out_shape=(jax.ShapeDtypeStruct((rows, dim), BF),) * 2 + (jax.ShapeDtypeStruct((2, rows), F32),),
        scratch_shapes=[pltpu.VMEM((rows, dim), F32)],
        cost_estimate=pl.CostEstimate(flops=200 * rows * dim, bytes_accessed=16 * rows * dim, transcendentals=0),
    )(dq, dk, q_raw, k_raw, st, cos_t, sin_t, gains)


def weight_back(d, hid, extra=None, idx=0):
    n, cols = d.shape
    dim = hid.shape[1]
    n_chip = dim // cols
    out_shape = jax.ShapeDtypeStruct((n_chip, 2, cols // 2, cols), F32)
    out_spec = pl.BlockSpec((1, 2, cols // 2, cols), lambda p: (p, 0, 0, 0))
    h_spec = pl.BlockSpec((n, cols), lambda p: (0, p))
    scratch = [pltpu.VMEM((cols, n), BF)]
    cost = pl.CostEstimate(flops=2 * n * cols * dim, bytes_accessed=2 * n * dim + 4 * cols * dim, transcendentals=0)
    if extra is None:
        return pl.pallas_call(dw_v_kernel, grid=(n_chip,), name='dw_v', out_shape=out_shape, in_specs=[whole(d.shape), h_spec], out_specs=out_spec, scratch_shapes=scratch, cost_estimate=cost)(d, hid)
    return pl.pallas_call(
        functools.partial(dw_qk_kernel, idx=idx), grid=(n_chip,), name='dw_qk',
        out_shape=(out_shape, jax.ShapeDtypeStruct((8, cols), F32)),
        in_specs=[whole(d.shape)] + [whole(e.shape) for e in extra] + [h_spec],
        out_specs=(out_spec, whole((8, cols))), scratch_shapes=scratch, cost_estimate=cost,
    )(d, *extra, hid)


def solution(mesh):
    n_sp = mesh.shape['sp']
    n_chip = n_sp // 2
    same_core = [[2 * p + c for p in range(n_chip)] for c in range(2)]
    pairs = [(i, i ^ 1) for i in range(n_sp)]

    def swap(t):
        return lax.ppermute(t, 'sp', pairs)

    def exchange(t):
        return lax.all_to_all(t, 'sp', split_axis=0, concat_axis=0, axis_index_groups=same_core)

    def device_step(x_loc, gy_loc, positions, g_norm, w_query, w_key, w_value, w_out, g_query, g_key):
        me = lax.axis_index('sp')
        chip, core = me // 2, me % 2
        first = core == 0
        loc, dim = x_loc.shape[1], x_loc.shape[2]
        rows = 2 * loc
        cols = dim // n_chip

        def pick(t, idx):
            return lax.dynamic_index_in_dim(t, idx, 0, keepdims=False)

        def join(mine, other):
            return jnp.where(first, jnp.concatenate([mine, other], 0), jnp.concatenate([other, mine], 0))

        def to_core(t):
            return join(pick(t, core), swap(pick(t, 1 - core)))

        def from_core(t):
            halves = t.reshape(2, loc, dim)
            mine, other = pick(halves, core), swap(pick(halves, 1 - core))
            return jnp.where(first, jnp.stack([mine, other]), jnp.stack([other, mine]))

        def my_cols(w):
            return lax.dynamic_slice_in_dim(w, chip * cols, cols, axis=1)

        def inv_of(raw):
            return lax.rsqrt(jnp.mean(raw * raw, axis=-1, keepdims=True) + NORM_EPS)

        def spread(t):
            return exchange(jnp.broadcast_to(t[None], (n_chip,) + t.shape))

        x_f = to_core(x_loc).astype(F32)
        gy = to_core(gy_loc)
        pos = to_core(positions)
        x_inv = inv_of(x_f)
        x_hat = x_f * x_inv
        hidden = (x_hat * g_norm.astype(F32)).astype(BF)
        pos_f = jnp.broadcast_to(pos.astype(F32)[None], (8, rows))
        gains = jnp.stack([g_query, g_key]).astype(F32)
        gains_h = lax.dynamic_slice_in_dim(gains, chip * cols, cols, axis=1)
        w_cat = jnp.concatenate([my_cols(w_query), my_cols(w_key), my_cols(w_value)], 1)
        w_rows = lax.dynamic_slice_in_dim(w_out, chip * cols, cols, axis=0)
        hid_all, q, k, v, qh_hat, kh_hat, att_t, lse, att_tok, d_att, dwo, cos_a, sin_a, inv_all = front(
            hidden, gy, pos_f, w_cat, w_rows, gains_h, rope_rows(), n_chip)
        hid_all = hid_all.reshape(n_chip * rows, dim)

        def mine_of(t):
            return lax.dynamic_slice_in_dim(t, chip * rows, rows, axis=0)

        cos_t, sin_t = mine_of(cos_a), mine_of(sin_a)
        st = lax.dynamic_index_in_dim(inv_all.reshape(2, n_chip, rows), chip, 1, keepdims=False)
        hidden, _ = lax.optimization_barrier((hidden, inv_all))
        q_raw, k_raw = mm32(hidden, w_query), mm32(hidden, w_key)

        def to_tokens(t):
            return exchange(t.reshape(n_chip, rows, cols))

        def flat(t):
            return jnp.moveaxis(t, 0, 1).reshape(rows, dim)

        y = (x_f + mm32(flat(att_tok), w_out)).astype(BF)
        dq, dk, dv = attn_bwd(q, k, v, d_att, att_t, lse)
        dq_tok, dk_tok, dv_tok = to_tokens(dq), to_tokens(dk), to_tokens(dv)

        dwo = dwo.reshape(2, loc, dim)
        dwo = pick(dwo, core) + swap(pick(dwo, 1 - core))

        def finish_cols(part):
            mine = lax.dynamic_index_in_dim(part, core, 1, keepdims=False)
            other = lax.dynamic_index_in_dim(part, 1 - core, 1, keepdims=False)
            return jnp.moveaxis(exchange(mine + swap(other)), 0, 1).reshape(loc, dim)

        dwv = finish_cols(weight_back(dv, hid_all))
        dq_raw, dk_raw, rowst = token_back(dq_tok, dk_tok, q_raw, k_raw, st, cos_t, sin_t, gains)
        row_all = spread(rowst)
        dwq, dgq = weight_back(dq, hid_all, (qh_hat, inv_all, row_all, cos_a, sin_a, gains_h), 0)
        dwk, dgk = weight_back(dk, hid_all, (kh_hat, inv_all, row_all, cos_a, sin_a, gains_h), 1)
        dwq, dwk = finish_cols(dwq), finish_cols(dwk)
        dg = jnp.stack([dgq[0], dgk[0]]).reshape(2, 2, loc)
        dg = jnp.moveaxis(dg, 1, 0)
        dg = pick(dg, core) + swap(pick(dg, 1 - core))

        d_hid = mm32_nt(flat(dv_tok), w_value) + mm32_nt(dq_raw, w_query) + mm32_nt(dk_raw, w_key)
        d_nrm = d_hid * g_norm.astype(F32)
        dxn = x_inv * (d_nrm - x_hat * jnp.mean(d_nrm * x_hat, axis=-1, keepdims=True))
        grad_x = (gy.astype(F32) + dxn).astype(BF)
        dgn = jnp.sum(d_hid * x_hat, axis=0).reshape(n_sp, loc)
        dgn = jnp.sum(lax.all_to_all(dgn, 'sp', split_axis=0, concat_axis=0), axis=0)
        return from_core(y), from_core(grad_x), dgn, dwq, dwk, dwv, dwo, dg[0], dg[1]

    seq_spec = P('dp', 'sp', None)
    mat_rep = P(None, None)
    vec_rep = P(None)
    row_spec = P(('dp', 'sp'), None)
    vec_spec = P(('dp', 'sp'))
    return jax.shard_map(device_step, mesh=mesh, in_specs=(seq_spec, seq_spec, P('dp', 'sp'), vec_rep, mat_rep, mat_rep, mat_rep, mat_rep, vec_rep, vec_rep), out_specs=(seq_spec, seq_spec, vec_spec, row_spec, row_spec, row_spec, row_spec, vec_spec, vec_spec), check_vma=False)
```

```python
import functools
import jax
import jax.numpy as jnp
from jax import lax
from jax.experimental import pallas as pl
from jax.experimental.pallas import tpu as pltpu
from jax.sharding import PartitionSpec as P

HEAD_DIM = 128
NORM_EPS = 1e-5
ROPE_BASE = 10000.0
NEG_BIG = -1e30
LOG2E = 1.4426950408889634
FWD_BLOCK = 512
CHUNKS = 4
BWD_BLOCK = 512
F32, BF = jnp.float32, jnp.bfloat16
NT = (((1,), (1,)), ((), ()))


def rope_rows():
    half = HEAD_DIM // 2
    inv_freq = ROPE_BASE ** (-jnp.arange(half, dtype=F32) * (2.0 / HEAD_DIM))
    sign = jnp.concatenate([-jnp.ones(half, F32), jnp.ones(half, F32)])
    return jnp.stack([jnp.concatenate([inv_freq, inv_freq]), sign])


def column(row):
    return jnp.broadcast_to(row, (HEAD_DIM, row.shape[1])).T


def as_row(col):
    return jnp.broadcast_to(col, (col.shape[0], HEAD_DIM)).T[0:1, :]


def half_roll(u):
    return pltpu.roll(u, HEAD_DIM // 2, 1)


def front_kernel(h_ref, gy_ref, wq_ref, wk_ref, pos_ref, w_ref, wrow_ref, g_ref, f_ref,
                 hall_ref, q_ref, k_ref, v_ref, qh_ref, kh_ref, ot_ref, lse_ref, atok_ref, datt_ref, dwo_ref, c_ref, s_ref, inv_ref, qr_ref, kr_ref,
                 buf, att_ref, vt_ref, pos_all, ssq, ssq_all, wbuf,
                 w_sem, load_sem, out_sem, ssem, rsem, ps_sem, pr_sem, qs_sem, qr_sem, as_sem, ar_sem):
    me = lax.axis_index('sp')
    chip, core = me // 2, lax.rem(me, 2)
    n_chip, rows, dim = hall_ref.shape
    cols = q_ref.shape[1]
    part = rows // CHUNKS
    half = n_chip // 2
    heads = [slice(lo, lo + HEAD_DIM) for lo in range(0, cols, HEAD_DIM)]

    def spot(p):
        z, y = p // 2, lax.rem(p, 2)
        return z + y * (n_chip - 1 - 2 * z)

    def chip_at(r):
        y = r // half
        return 2 * (r + y * (n_chip - 1 - 2 * r)) + y

    ring = spot(chip)

    def slot_at(dr, dist):
        step = dist if dr == 0 else -dist
        return chip_at(lax.rem(ring - step + 2 * n_chip, n_chip))

    def dev(p):
        return {'sp': 2 * p + core}

    right = dev(slot_at(1, 1))
    left = dev(slot_at(0, 1))

    def hop(t, dr, s, c, dist):
        view = buf.at[t, slot_at(dr, dist), pl.ds(c * part, part)]
        return pltpu.make_async_remote_copy(
            src_ref=view, dst_ref=view, send_sem=ssem.at[t, dr, s, c], recv_sem=rsem.at[t, dr, s, c],
            device_id=right if dr == 0 else left, device_id_type=pl.DeviceIdType.MESH)

    def in_half(dr, c):
        return (c < CHUNKS // 2) == (dr == 0)

    def start_own(t):
        for c in range(CHUNKS):
            for dr in range(2):
                hop(t, dr, 0, c, 0).start()

    def stage(t, s):
        for c in range(CHUNKS):
            for dr in range(2):
                hop(t, dr, s, c, s + 1).wait_recv()
                if in_half(dr, c):
                    hop(t, dr, s + 1, c, s + 1).start()
                else:
                    @pl.when(s < half - 2)
                    def _():
                        hop(t, dr, s + 1, c, s + 1).start()

    def last_stage(t):
        for c in range(CHUNKS):
            for dr in range(2):
                if in_half(dr, c):
                    hop(t, dr, half - 1, c, half).wait_recv()

    def drain(t):
        for s in range(half):
            for c in range(CHUNKS):
                for dr in range(2):
                    if s < half - 1 or in_half(dr, c):
                        hop(t, dr, s, c, s).wait_send()

    def to_peers(src, dst, s_sem, r_sem):
        def make(p, owner):
            return pltpu.make_async_remote_copy(
                src_ref=src, dst_ref=dst.at[owner], send_sem=s_sem.at[p], recv_sem=r_sem.at[owner],
                device_id=dev(p), device_id_type=pl.DeviceIdType.MESH)
        return make

    def each_peer(fn):
        for p in range(n_chip):
            @pl.when(p != chip)
            def _():
                fn(p)

    loads = [pltpu.make_async_copy(src, buf.at[t, chip], load_sem.at[t]) for t, src in enumerate((h_ref, gy_ref))]
    for ld in loads:
        ld.start()
    barrier = pltpu.get_barrier_semaphore()
    each_peer(lambda p: pl.semaphore_signal(barrier, inc=1, device_id=dev(p), device_id_type=pl.DeviceIdType.MESH))
    pl.semaphore_wait(barrier, n_chip - 1)
    pos_copy = to_peers(pos_ref, pos_all, ps_sem, pr_sem)
    each_peer(lambda p: pos_copy(p, chip).start())
    pos_all[chip] = pos_ref[...]
    loads[0].wait()
    start_own(0)

    def project(p):
        ts = pl.ds(pl.multiple_of(p * rows, rows), rows)
        h = buf[0, p]
        for idx, out in enumerate((qh_ref, kh_ref)):
            raw = mm32(h, w_ref[:, idx * cols:(idx + 1) * cols])
            out[ts, :] = raw
            ssq[pl.ds(idx * n_chip + p, 1), :] = as_row(jnp.sum(raw * raw, axis=1, keepdims=True))
        v_ref[ts, :] = mm32(h, w_ref[:, 2 * cols:]).astype(BF)

    project(chip)
    each_peer(lambda p: pos_copy(p, p).wait_recv())
    for p in range(n_chip):
        angles = column(pos_all[p, 0:1, :]) * f_ref[0:1, :]
        c_ref[p * rows:(p + 1) * rows, :] = jnp.cos(angles)
        s_ref[p * rows:(p + 1) * rows, :] = jnp.sin(angles) * f_ref[1:2, :]

    def gather_step(s, _):
        stage(0, s)

        def both(dr, _):
            dist = (s + 1) * (1 - 2 * dr)
            project(chip_at(lax.rem(ring - dist + 2 * n_chip, n_chip)))
            return 0

        lax.fori_loop(0, 2, both, 0)
        return 0

    lax.fori_loop(0, half - 1, gather_step, 0)
    loads[1].wait()
    start_own(1)
    last_stage(0)
    project(slot_at(0, half))
    hall_copy = pltpu.make_async_copy(buf.at[0], hall_ref, out_sem)
    hall_copy.start()
    for hs in heads:
        vt_ref[hs, :] = v_ref[:, hs].T
    ssq_copy = to_peers(ssq, ssq_all, qs_sem, qr_sem)
    each_peer(lambda p: ssq_copy(p, chip).start())
    ssq_all[chip] = ssq[...]
    each_peer(lambda p: ssq_copy(p, p).wait_recv())
    total = ssq_all[0]
    for p in range(1, n_chip):
        total = total + ssq_all[p]
    inv_ref[...] = lax.rsqrt(total / dim + NORM_EPS)

    def finish_qk(p, _):
        ts = pl.ds(pl.multiple_of(p * rows, rows), rows)
        for idx, (hat_ref, out) in enumerate(((qh_ref, q_ref), (kh_ref, k_ref))):
            inv = column(inv_ref[pl.ds(idx * n_chip + p, 1), :])
            for hs in heads:
                hat = hat_ref[ts, hs] * inv
                hat_ref[ts, hs] = hat
                u = hat * g_ref[idx:idx + 1, hs]
                out[ts, hs] = (u * c_ref[ts, :] + half_roll(u) * s_ref[ts, :]).astype(BF)
        return 0

    lax.fori_loop(0, n_chip, finish_qk, 0)

    blk = FWD_BLOCK
    scale = HEAD_DIM ** -0.5 * LOG2E
    causal = lax.broadcasted_iota(jnp.int32, (blk, blk), 0) <= lax.broadcasted_iota(jnp.int32, (blk, blk), 1)

    def attend(j, _):
        qs = pl.ds(pl.multiple_of(j * blk, blk), blk)
        qb = [q_ref[qs, hs] for hs in heads]

        def tile(i, carry, diag):
            ks = pl.ds(pl.multiple_of(i * blk, blk), blk)
            out = []
            for h, hs in enumerate(heads):
                m, l, acc = carry[h]
                s = mm32_nt(k_ref[ks, hs], qb[h])
                if diag:
                    s = jnp.where(causal, s, NEG_BIG)
                mn = jnp.maximum(m, jnp.max(s, axis=0, keepdims=True))
                al = jnp.exp2((m - mn) * scale)
                p = jnp.exp2((s - mn) * scale)
                l = al * l + jnp.sum(p, axis=0, keepdims=True)
                out.append((mn, l, al * acc + mm32(vt_ref[hs, ks], p.astype(BF))))
            return tuple(out)

        st = tuple((jnp.full((1, blk), NEG_BIG, F32), jnp.zeros((1, blk), F32), jnp.zeros((HEAD_DIM, blk), F32)) for _ in heads)
        st = lax.fori_loop(0, j, lambda i, cr: tile(i, cr, False), st)
        st = tile(j, st, True)
        for h, hs in enumerate(heads):
            m, l, acc = st[h]
            ot = acc / l
            ot_ref[hs, qs] = ot
            att_ref[qs, hs] = ot.T.astype(BF)
            lse_ref[h:h + 1, qs] = m * scale + jnp.log2(l)
        return 0

    def att_copy(p, owner):
        return pltpu.make_async_remote_copy(
            src_ref=att_ref.at[pl.ds(p * rows, rows)], dst_ref=atok_ref.at[:, pl.ds(pl.multiple_of(owner * cols, cols), cols)], send_sem=as_sem.at[p], recv_sem=ar_sem.at[owner],
            device_id=dev(p), device_id_type=pl.DeviceIdType.MESH)

    def send_att(lo, hi):
        for p in range(lo, hi):
            @pl.when(p != chip)
            def _():
                att_copy(p, chip).start()

    def use_gy(p):
        ts = pl.ds(pl.multiple_of(p * rows, rows), rows)
        gy = buf[1, p]
        datt_ref[ts, :] = mm32_nt(gy, wrow_ref[...]).astype(BF)
        dwo_ref[...] += mm32(ot_ref[:, ts].astype(BF), gy)

    n_att = n_chip * rows // blk
    lax.fori_loop(0, n_att // 2, attend, 0)
    stage(1, 0)
    send_att(0, half)
    lax.fori_loop(n_att // 2, n_att, attend, 0)

    def raw_of(w, out):
        def load(m, slot):
            return pltpu.make_async_copy(w.at[:, pl.ds(pl.multiple_of(m * cols, cols), cols)], wbuf.at[slot], w_sem.at[slot])

        load(0, 0).start()

        def step(m, _):
            slot = lax.rem(m, 2)
            load(m, slot).wait()

            @pl.when(m + 1 < n_chip)
            def _():
                load(m + 1, 1 - slot).start()
            out[:, pl.ds(pl.multiple_of(m * cols, cols), cols)] = mm32(buf[0, chip], wbuf[slot])
            return 0

        lax.fori_loop(0, n_chip, step, 0)

    raw_of(wq_ref, qr_ref)
    raw_of(wk_ref, kr_ref)
    stage(1, 1)
    send_att(half, n_chip)
    atok_ref[:, pl.ds(pl.multiple_of(chip * cols, cols), cols)] = att_ref[pl.ds(pl.multiple_of(chip * rows, rows), rows), :]
    dwo_ref[...] = jnp.zeros_like(dwo_ref)

    def use_ring(n, _):
        dist = ((n + 1) // 2) * (2 * lax.rem(n, 2) - 1)
        use_gy(chip_at(lax.rem(ring - dist + 2 * n_chip, n_chip)))
        return 0

    lax.fori_loop(0, n_chip - 3, use_ring, 0)
    stage(1, half - 2)
    lax.fori_loop(n_chip - 3, n_chip - 1, use_ring, 0)
    last_stage(1)
    use_gy(slot_at(0, half))

    each_peer(lambda p: att_copy(p, p).wait_recv())
    each_peer(lambda p: att_copy(p, chip).wait_send())
    each_peer(lambda p: pos_copy(p, chip).wait_send())
    each_peer(lambda p: ssq_copy(p, chip).wait_send())
    drain(0)
    drain(1)
    hall_copy.wait()


def back_kernel(q_ref, k_ref, v_ref, do_ref, ot_ref, lse_ref, g_ref, gt_ref, inv_ref,
                hall_ref, qh_hbm, kh_hbm, c_hbm, s_hbm, qr_hbm, kr_hbm, wq_ref, wk_ref, wv_ref, dwo_ref,
                dwq_ref, dwk_ref, dwv_ref, dwo_out, dhid_ref, dg_ref,
                dq_ref, dk_ref, dv_ref, dka_ref, dva_ref, kt_ref, qh_ref, kh_ref, c_ref, s_ref, qr_ref, kr_ref,
                tok, pairs, pair_in, dt_ref, hblk, wblk, dwo_in, row_ref, row_all,
                load_sem, h_sem, w_sem, xs_sem, xr_sem, ps_sem, pr_sem, rs_sem, rr_sem, own_sem, do_sem):
    me = lax.axis_index('sp')
    chip, core = me // 2, lax.rem(me, 2)
    n, cols = q_ref.shape
    rows, dim = qr_ref.shape
    n_chip = n // rows
    partner = {'sp': me + 1 - 2 * core}
    heads = [slice(lo, lo + HEAD_DIM) for lo in range(0, cols, HEAD_DIM)]
    own_rows = pl.ds(pl.multiple_of(chip * rows, rows), rows)
    own_cols = pl.ds(pl.multiple_of(chip * cols, cols), cols)
    MESH = pl.DeviceIdType.MESH

    def dev(p):
        return {'sp': 2 * p + core}

    def each_peer(fn):
        for p in range(n_chip):
            @pl.when(p != chip)
            def _():
                fn(p)

    sides = ((qh_hbm, qh_ref), (kh_hbm, kh_ref), (c_hbm, c_ref), (s_hbm, s_ref), (qr_hbm, qr_ref), (kr_hbm, kr_ref), (dwo_ref.at[core], dwo_out))
    loads = [pltpu.make_async_copy(src, dst, load_sem.at[i]) for i, (src, dst) in enumerate(sides)]
    for ld in loads:
        ld.start()

    def load_h(p, slot):
        return pltpu.make_async_copy(hall_ref.at[:, pl.ds(pl.multiple_of(p * cols, cols), cols)], hblk.at[slot], h_sem.at[slot])

    load_h(0, 0).start()
    barrier = pltpu.get_barrier_semaphore()
    each_peer(lambda p: pl.semaphore_signal(barrier, inc=1, device_id=dev(p), device_id_type=MESH))
    pl.semaphore_signal(barrier, inc=1, device_id=partner, device_id_type=MESH)
    pl.semaphore_wait(barrier, n_chip)

    dwo_copy = pltpu.make_async_remote_copy(
        src_ref=dwo_ref.at[1 - core], dst_ref=dwo_in, send_sem=do_sem.at[0], recv_sem=do_sem.at[1], device_id=partner, device_id_type=MESH)
    dwo_copy.start()

    def tok_copy(t, p, owner):
        src = (dq_ref, dk_ref, dv_ref)[t].at[pl.ds(pl.multiple_of(p * rows, rows), rows)]
        dst = tok.at[t, :, pl.ds(pl.multiple_of(owner * cols, cols), cols)]
        return pltpu.make_async_remote_copy(src_ref=src, dst_ref=dst, send_sem=xs_sem.at[t, p], recv_sem=xr_sem.at[t, owner], device_id=dev(p), device_id_type=MESH)

    blk = BWD_BLOCK
    span = blk // rows
    n_blk = n // blk
    sc = HEAD_DIM ** -0.5
    scale = sc * LOG2E
    for hs in heads:
        kt_ref[hs, :] = k_ref[:, hs].T
    dka_ref[...] = jnp.zeros_like(dka_ref)
    dva_ref[...] = jnp.zeros_like(dva_ref)
    causal = lax.broadcasted_iota(jnp.int32, (blk, blk), 0) <= lax.broadcasted_iota(jnp.int32, (blk, blk), 1)

    def send_dq(j):
        for u in range(span):
            p = j * span + u

            @pl.when(p != chip)
            def _():
                tok_copy(0, p, chip).start()

    def q_step(j, _):
        qs = pl.ds(pl.multiple_of(j * blk, blk), blk)
        qb = [q_ref[qs, hs] for hs in heads]
        dob = [do_ref[qs, hs] for hs in heads]
        lse = [lse_ref[h:h + 1, qs] for h in range(len(heads))]
        dl = [jnp.sum(ot_ref[hs, qs] * dob[h].astype(F32).T, axis=0, keepdims=True) for h, hs in enumerate(heads)]

        def tile(i, carry, diag):
            ks = pl.ds(pl.multiple_of(i * blk, blk), blk)
            out = []
            for h, hs in enumerate(heads):
                s = mm32_nt(k_ref[ks, hs], qb[h])
                dp = mm32_nt(v_ref[ks, hs], dob[h])
                p = jnp.exp2(s * scale - lse[h])
                if diag:
                    p = jnp.where(causal, p, 0.0)
                ds = (p * (dp - dl[h])).astype(BF)
                dva_ref[ks, hs] += mm32(p.astype(BF), dob[h])
                dka_ref[ks, hs] += mm32(ds, qb[h])
                out.append(carry[h] + mm32(kt_ref[hs, ks], ds))
            return tuple(out)

        st = tuple(jnp.zeros((HEAD_DIM, blk), F32) for _ in heads)
        st = lax.fori_loop(0, j, lambda i, cr: tile(i, cr, False), st)
        st = tile(j, st, True)
        for h, hs in enumerate(heads):
            dq_ref[qs, hs] = (st[h] * sc).T.astype(BF)

        @pl.when(j > 0)
        def _():
            send_dq(j - 1)
        return 0

    lax.fori_loop(0, n_blk, q_step, 0)
    dk_ref[...] = (dka_ref[...] * sc).astype(BF)
    dv_ref[...] = dva_ref[...].astype(BF)
    send_dq(n_blk - 1)
    for t, src in enumerate((dq_ref, dk_ref, dv_ref)):
        tok[t, :, own_cols] = src[own_rows, :]
    for t in (1, 2):
        each_peer(lambda p: tok_copy(t, p, chip).start())

    def pair_copy(w, p):
        return pltpu.make_async_remote_copy(
            src_ref=pairs.at[w, p, 1 - core], dst_ref=pair_in.at[w, p], send_sem=ps_sem.at[w, p], recv_sem=pr_sem.at[w, p], device_id=partner, device_id_type=MESH)

    grads = (dwq_ref, dwk_ref, dwv_ref)

    def dw_copy(w, p, owner):
        dst = grads[w].at[:, pl.ds(pl.multiple_of(owner * cols, cols), cols)]
        return pltpu.make_async_remote_copy(src_ref=pairs.at[w, p, core], dst_ref=dst, send_sem=xs_sem.at[3 + w, p], recv_sem=xr_sem.at[3 + w, owner], device_id=dev(p), device_id_type=MESH)

    def own_copy(w):
        return pltpu.make_async_copy(pairs.at[w, chip, core], grads[w].at[:, own_cols], own_sem.at[w])

    def partial(w, slot_t, h, p):
        dw = mm32(dt_ref[slot_t], h).T
        pairs[w, p, 0] = dw[:rows // 2]
        pairs[w, p, 1] = dw[rows // 2:]

    def merge(w, p):
        pair_copy(w, p).wait_recv()
        pairs[w, p, core] += pair_in[w, p]

    def send_dw(w, p):
        @pl.when(p != chip)
        def _():
            dw_copy(w, p, chip).start()

        @pl.when(p == chip)
        def _():
            own_copy(w).start()

    def each_h(ws, tail_fn):
        def step(p, _):
            slot = lax.rem(p, 2)
            load_h(p, slot).wait()

            @pl.when(p + 1 < n_chip)
            def _():
                load_h(p + 1, 1 - slot).start()
            for w, slot_t in ws:
                partial(w, slot_t, hblk[slot], p)
            tail_fn(p)
            for w, _ in ws:
                pair_copy(w, p).start()
            return 0

        lax.fori_loop(0, n_chip, step, 0)

    dt_ref[0] = dv_ref[...].T
    each_h(((2, 0),), lambda p: None)
    load_h(0, 0).start()
    for ld in loads:
        ld.wait()

    hats = ((qr_ref, 0), (kr_ref, 1))
    row_ref[...] = jnp.zeros_like(row_ref)
    inv_t = [column(inv_ref[pl.ds(idx * n_chip + chip, 1), :]) for idx in range(2)]
    c_t, s_t = c_ref[own_rows, :], s_ref[own_rows, :]

    def normed(idx, hs):
        d = tok[idx, :, hs].astype(F32)
        return (d * c_t - half_roll(d) * s_t) * gt_ref[idx:idx + 1, hs]

    row_cols = []
    for raw_ref, idx in hats:
        each_peer(lambda p: tok_copy(idx, p, p).wait_recv())
        acc = jnp.zeros((rows, HEAD_DIM), F32)
        for lo in range(0, dim, HEAD_DIM):
            hs = slice(lo, lo + HEAD_DIM)
            acc += normed(idx, hs) * (raw_ref[:, hs] * inv_t[idx])
        row = jnp.sum(acc, axis=1, keepdims=True) / dim
        row_ref[idx:idx + 1, :] = as_row(row)
        row_cols.append(row)

    def row_copy(p, owner):
        return pltpu.make_async_remote_copy(src_ref=row_ref, dst_ref=row_all.at[owner], send_sem=rs_sem.at[p], recv_sem=rr_sem.at[owner], device_id=dev(p), device_id_type=MESH)

    for raw_ref, idx in hats:
        for lo in range(0, dim, HEAD_DIM):
            hs = slice(lo, lo + HEAD_DIM)
            tok[idx, :, hs] = (inv_t[idx] * (normed(idx, hs) - raw_ref[:, hs] * inv_t[idx] * row_cols[idx])).astype(BF)
        if idx == 0:
            each_peer(lambda p: row_copy(p, chip).start())
            row_all[chip] = row_ref[...]

    def merge_v(p, _):
        merge(2, p)
        return 0

    def send_v(p, _):
        send_dw(2, p)
        return 0

    lax.fori_loop(0, n_chip, merge_v, 0)

    def load_w(m, slot):
        return [pltpu.make_async_copy(w.at[pl.ds(pl.multiple_of(m * cols, cols), cols)], wblk.at[slot, i], w_sem.at[slot, i]) for i, w in enumerate((wq_ref, wk_ref, wv_ref))]

    for ld in load_w(0, 0):
        ld.start()
    lax.fori_loop(0, n_chip, send_v, 0)
    each_peer(lambda p: row_copy(p, p).wait_recv())

    dg_ref[...] = jnp.zeros_like(dg_ref)

    def head_step(p, _):
        ts = pl.ds(pl.multiple_of(p * rows, rows), rows)
        for idx, (d_ref, hat_ref) in enumerate(((dq_ref, qh_ref), (dk_ref, kh_ref))):
            inv = column(inv_ref[pl.ds(idx * n_chip + p, 1), :])
            row = column(row_all[p, idx:idx + 1, :])
            for hs in heads:
                d = d_ref[ts, hs].astype(F32)
                rot = d * c_ref[ts, :] - half_roll(d) * s_ref[ts, :]
                hat = hat_ref[ts, hs]
                raw = inv * (rot * g_ref[idx:idx + 1, hs] - hat * row)
                dt_ref[idx, hs, ts] = raw.astype(BF).T
                dg_ref[idx:idx + 1, hs] += jnp.sum(rot * hat, axis=0, keepdims=True)
        return 0

    lax.fori_loop(0, n_chip, head_step, 0)

    def lagged(p):
        @pl.when(p > 0)
        def _():
            for w in range(2):
                merge(w, p - 1)

        @pl.when(p > 1)
        def _():
            for w in range(2):
                send_dw(w, p - 2)

    each_h(((0, 0), (1, 1)), lagged)
    for w in range(2):
        send_dw(w, n_chip - 2)
        merge(w, n_chip - 1)
    dwo_copy.wait_recv()
    dwo_out[...] += dwo_in[...]
    for w in range(2):
        send_dw(w, n_chip - 1)

    each_peer(lambda p: tok_copy(2, p, p).wait_recv())

    def hid_step(m, _):
        slot = lax.rem(m, 2)
        for ld in load_w(m, slot):
            ld.wait()

        @pl.when(m + 1 < n_chip)
        def _():
            for ld in load_w(m + 1, 1 - slot):
                ld.start()
        out = pl.ds(pl.multiple_of(m * cols, cols), cols)
        dhid_ref[:, out] = mm32_nt(tok[0], wblk[slot, 0]) + mm32_nt(tok[1], wblk[slot, 1]) + mm32_nt(tok[2], wblk[slot, 2])
        return 0

    lax.fori_loop(0, n_chip, hid_step, 0)

    for w in range(3):
        each_peer(lambda p: dw_copy(w, p, p).wait_recv())
        each_peer(lambda p: dw_copy(w, p, chip).wait_send())
        each_peer(lambda p: tok_copy(w, p, chip).wait_send())
        own_copy(w).wait()
        for p in range(n_chip):
            pair_copy(w, p).wait_send()
    each_peer(lambda p: row_copy(p, chip).wait_send())
    dwo_copy.wait_send()


VM = pl.BlockSpec(memory_space=pltpu.VMEM)


def mm32(a, b):
    return jnp.dot(a, b, preferred_element_type=F32)


def mm32_nt(a, b):
    return lax.dot_general(a, b, NT, preferred_element_type=F32)


def front(hid, gy, w_query, w_key, pos, w_cat, w_rows, gains, freq, n_chip):
    rows, dim = hid.shape
    cols = w_rows.shape[0]
    n = n_chip * rows
    heads = cols // HEAD_DIM
    any_spec = pl.BlockSpec(memory_space=pl.ANY)
    half = n_chip // 2
    dma = pltpu.SemaphoreType.DMA
    outs = [((n_chip, rows, dim), BF), ((n, cols), BF), ((n, cols), BF), ((n, cols), BF), ((n, cols), F32), ((n, cols), F32), ((cols, n), F32), ((heads, n), F32),
            ((rows, dim), BF), ((n, cols), BF), ((cols, dim), F32), ((n, HEAD_DIM), F32), ((n, HEAD_DIM), F32), ((2 * n_chip, rows), F32), ((rows, dim), F32), ((rows, dim), F32)]
    return pl.pallas_call(
        front_kernel, name='front', out_shape=tuple(jax.ShapeDtypeStruct(s, d) for s, d in outs),
        in_specs=[any_spec] * 4 + [VM] * 5, out_specs=(any_spec,) + (VM,) * 15,
        scratch_shapes=[
            pltpu.VMEM((2, n_chip, rows, dim), BF), pltpu.VMEM((n, cols), BF), pltpu.VMEM((cols, n), BF),
            pltpu.VMEM((n_chip, 8, rows), F32), pltpu.VMEM((2 * n_chip, rows), F32), pltpu.VMEM((n_chip, 2 * n_chip, rows), F32), pltpu.VMEM((2, dim, cols), BF),
            dma((2,)), dma((2,)), dma(()), dma((2, 2, half, CHUNKS)), dma((2, 2, half, CHUNKS)),
            dma((n_chip,)), dma((n_chip,)), dma((n_chip,)), dma((n_chip,)), dma((n_chip,)), dma((n_chip,))],
        compiler_params=pltpu.CompilerParams(collective_id=0, has_side_effects=True, vmem_limit_bytes=67043328),
        cost_estimate=pl.CostEstimate(flops=400 * n * dim * cols, bytes_accessed=40 * n * dim, transcendentals=n * n * heads // 2),
    )(hid, gy, w_query, w_key, pos, w_cat, w_rows, gains, freq)


def back(q, k, v, d_att, att_t, lse, gains_h, gains, inv, hid, qh, kh, cos_a, sin_a, q_raw, k_raw, w_query, w_key, w_value, dwo):
    n, cols = q.shape
    rows, dim = q_raw.shape
    n_chip = n // rows
    any_spec = pl.BlockSpec(memory_space=pl.ANY)
    dma = pltpu.SemaphoreType.DMA
    grad = jax.ShapeDtypeStruct((rows // 2, dim), F32)
    vmem = pltpu.VMEM
    return pl.pallas_call(
        back_kernel, name='back', in_specs=[VM] * 9 + [any_spec] * 11, out_specs=(any_spec,) * 3 + (VM,) * 3,
        out_shape=(grad,) * 4 + (jax.ShapeDtypeStruct((rows, dim), F32), jax.ShapeDtypeStruct((8, cols), F32)),
        scratch_shapes=[
            vmem((n, cols), BF), vmem((n, cols), BF), vmem((n, cols), BF), vmem((n, cols), F32), vmem((n, cols), F32), vmem((cols, n), BF),
            vmem((n, cols), F32), vmem((n, cols), F32), vmem((n, HEAD_DIM), F32), vmem((n, HEAD_DIM), F32), vmem((rows, dim), F32), vmem((rows, dim), F32),
            vmem((3, rows, dim), BF), vmem((3, n_chip, 2, rows // 2, cols), F32), vmem((3, n_chip, rows // 2, cols), F32),
            vmem((2, cols, n), BF), vmem((2, n, cols), BF), vmem((2, 3, cols, dim), BF), vmem((rows // 2, dim), F32),
            vmem((8, rows), F32), vmem((n_chip, 8, rows), F32),
            dma((7,)), dma((2,)), dma((2, 3)), dma((6, n_chip)), dma((6, n_chip)), dma((3, n_chip)), dma((3, n_chip)),
            dma((n_chip,)), dma((n_chip,)), dma((3,)), dma((2,))],
        compiler_params=pltpu.CompilerParams(collective_id=1, has_side_effects=True, vmem_limit_bytes=67043328),
        cost_estimate=pl.CostEstimate(flops=400 * n * dim * cols, bytes_accessed=40 * n * dim, transcendentals=n * n),
    )(q, k, v, d_att, att_t, lse, gains_h, gains, inv, hid, qh, kh, cos_a, sin_a, q_raw, k_raw, w_query, w_key, w_value, dwo)


def solution(mesh):
    n_sp = mesh.shape['sp']
    n_chip = n_sp // 2
    pairs = [(i, i ^ 1) for i in range(n_sp)]

    def swap(t):
        return lax.ppermute(t, 'sp', pairs)

    def device_step(x_loc, gy_loc, positions, g_norm, w_query, w_key, w_value, w_out, g_query, g_key):
        me = lax.axis_index('sp')
        chip, core = me // 2, me % 2
        first = core == 0
        loc, dim = x_loc.shape[1], x_loc.shape[2]
        rows = 2 * loc
        cols = dim // n_chip

        def pick(t, idx):
            return lax.dynamic_index_in_dim(t, idx, 0, keepdims=False)

        def join(mine, other):
            return jnp.where(first, jnp.concatenate([mine, other], 0), jnp.concatenate([other, mine], 0))

        def to_core(t):
            return join(pick(t, core), swap(pick(t, 1 - core)))

        def from_core(t):
            halves = t.reshape(2, loc, dim)
            mine, other = pick(halves, core), swap(pick(halves, 1 - core))
            return jnp.where(first, jnp.stack([mine, other]), jnp.stack([other, mine]))

        def my_cols(w):
            return lax.dynamic_slice_in_dim(w, chip * cols, cols, axis=1)

        def inv_of(raw):
            return lax.rsqrt(jnp.mean(raw * raw, axis=-1, keepdims=True) + NORM_EPS)

        x_f = to_core(x_loc).astype(F32)
        gy = to_core(gy_loc)
        pos = to_core(positions)
        x_inv = inv_of(x_f)
        x_hat = x_f * x_inv
        hidden = (x_hat * g_norm.astype(F32)).astype(BF)
        pos_f = jnp.broadcast_to(pos.astype(F32)[None], (8, rows))
        gains = jnp.stack([g_query, g_key]).astype(F32)
        gains_h = lax.dynamic_slice_in_dim(gains, chip * cols, cols, axis=1)
        w_cat = jnp.concatenate([my_cols(w_query), my_cols(w_key), my_cols(w_value)], 1)
        w_rows = lax.dynamic_slice_in_dim(w_out, chip * cols, cols, axis=0)
        hid_all, q, k, v, qh_hat, kh_hat, att_t, lse, att_tok, d_att, dwo, cos_a, sin_a, inv_all, q_raw, k_raw = front(
            hidden, gy, w_query, w_key, pos_f, w_cat, w_rows, gains_h, rope_rows(), n_chip)
        dwq, dwk, dwv, dwo, d_hid, dg = back(
            q, k, v, d_att, att_t, lse, gains_h, gains, inv_all, hid_all.reshape(n_chip * rows, dim), qh_hat, kh_hat, cos_a, sin_a,
            q_raw, k_raw, w_query, w_key, w_value, dwo.reshape(2, loc, dim))
        y = (x_f + mm32(att_tok, w_out)).astype(BF)
        dg = jnp.moveaxis(dg[:2].reshape(2, 2, loc), 1, 0)
        dg = pick(dg, core) + swap(pick(dg, 1 - core))

        d_nrm = d_hid * g_norm.astype(F32)
        dxn = x_inv * (d_nrm - x_hat * jnp.mean(d_nrm * x_hat, axis=-1, keepdims=True))
        grad_x = (gy.astype(F32) + dxn).astype(BF)
        dgn = jnp.sum(d_hid * x_hat, axis=0).reshape(n_sp, loc)
        dgn = jnp.sum(lax.all_to_all(dgn, 'sp', split_axis=0, concat_axis=0), axis=0)
        return from_core(y), from_core(grad_x), dgn, dwq, dwk, dwv, dwo, dg[0], dg[1]

    seq_spec = P('dp', 'sp', None)
    mat_rep = P(None, None)
    vec_rep = P(None)
    row_spec = P(('dp', 'sp'), None)
    vec_spec = P(('dp', 'sp'))
    return jax.shard_map(device_step, mesh=mesh, in_specs=(seq_spec, seq_spec, P('dp', 'sp'), vec_rep, mat_rep, mat_rep, mat_rep, mat_rep, vec_rep, vec_rep), out_specs=(seq_spec, seq_spec, vec_spec, row_spec, row_spec, row_spec, row_spec, vec_spec, vec_spec), check_vma=False)
```

```python
import functools
import jax
import jax.numpy as jnp
from jax import lax
from jax.experimental import pallas as pl
from jax.experimental.pallas import tpu as pltpu
from jax.sharding import PartitionSpec as P

HEAD_DIM = 128
NORM_EPS = 1e-5
ROPE_BASE = 10000.0
NEG_BIG = -1e30
LOG2E = 1.4426950408889634
FWD_BLOCK = 512
CHUNKS = 4
BWD_BLOCK = 512
F32, BF = jnp.float32, jnp.bfloat16
NT = (((1,), (1,)), ((), ()))


def rope_rows():
    half = HEAD_DIM // 2
    inv_freq = ROPE_BASE ** (-jnp.arange(half, dtype=F32) * (2.0 / HEAD_DIM))
    sign = jnp.concatenate([-jnp.ones(half, F32), jnp.ones(half, F32)])
    return jnp.stack([jnp.concatenate([inv_freq, inv_freq]), sign])


def column(row):
    return jnp.broadcast_to(row, (HEAD_DIM, row.shape[1])).T


def as_row(col):
    return jnp.broadcast_to(col, (col.shape[0], HEAD_DIM)).T[0:1, :]


def half_roll(u):
    return pltpu.roll(u, HEAD_DIM // 2, 1)


def front_kernel(x_ref, gy_ref, wq_ref, wk_ref, wv_ref, wo_ref, pos_ref, g_ref, gt_ref, f_ref,
                 hall_ref, q_ref, k_ref, v_ref, qh_ref, kh_ref, ot_ref, lse_ref, atok_ref, datt_ref, dwo_ref, c_ref, s_ref, inv_ref, qr_ref, kr_ref, xs_ref, gys_ref,
                 buf, w_ref, wrow_ref, att_ref, vt_ref, pos_all, ssq, ssq_all, wbuf,
                 w_sem, load_sem, swap_sem, out_sem, ssem, rsem, ps_sem, pr_sem, qs_sem, qr_sem, as_sem, ar_sem):
    me = lax.axis_index('sp')
    chip, core = me // 2, lax.rem(me, 2)
    n_chip, rows, dim = hall_ref.shape
    cols = q_ref.shape[1]
    part = rows // CHUNKS
    half = n_chip // 2
    heads = [slice(lo, lo + HEAD_DIM) for lo in range(0, cols, HEAD_DIM)]

    def spot(p):
        z, y = p // 2, lax.rem(p, 2)
        return z + y * (n_chip - 1 - 2 * z)

    def chip_at(r):
        y = r // half
        return 2 * (r + y * (n_chip - 1 - 2 * r)) + y

    ring = spot(chip)

    def slot_at(dr, dist):
        step = dist if dr == 0 else -dist
        return chip_at(lax.rem(ring - step + 2 * n_chip, n_chip))

    def dev(p):
        return {'sp': 2 * p + core}

    right = dev(slot_at(1, 1))
    left = dev(slot_at(0, 1))

    def hop(t, dr, s, c, dist):
        view = buf.at[t, slot_at(dr, dist), pl.ds(c * part, part)]
        return pltpu.make_async_remote_copy(
            src_ref=view, dst_ref=view, send_sem=ssem.at[t, dr, s, c], recv_sem=rsem.at[t, dr, s, c],
            device_id=right if dr == 0 else left, device_id_type=pl.DeviceIdType.MESH)

    def in_half(dr, c):
        return (c < CHUNKS // 2) == (dr == 0)

    def start_own(t):
        for c in range(CHUNKS):
            for dr in range(2):
                hop(t, dr, 0, c, 0).start()

    def stage(t, s):
        for c in range(CHUNKS):
            for dr in range(2):
                hop(t, dr, s, c, s + 1).wait_recv()
                if in_half(dr, c):
                    hop(t, dr, s + 1, c, s + 1).start()
                else:
                    @pl.when(s < half - 2)
                    def _():
                        hop(t, dr, s + 1, c, s + 1).start()

    def last_stage(t):
        for c in range(CHUNKS):
            for dr in range(2):
                if in_half(dr, c):
                    hop(t, dr, half - 1, c, half).wait_recv()

    def drain(t):
        for s in range(half):
            for c in range(CHUNKS):
                for dr in range(2):
                    if s < half - 1 or in_half(dr, c):
                        hop(t, dr, s, c, s).wait_send()

    def to_peers(src, dst, s_sem, r_sem):
        def make(p, owner):
            return pltpu.make_async_remote_copy(
                src_ref=src, dst_ref=dst.at[owner], send_sem=s_sem.at[p], recv_sem=r_sem.at[owner],
                device_id=dev(p), device_id_type=pl.DeviceIdType.MESH)
        return make

    def each_peer(fn):
        for p in range(n_chip):
            @pl.when(p != chip)
            def _():
                fn(p)

    partner = {'sp': me + 1 - 2 * core}
    own_cols = pl.ds(pl.multiple_of(chip * cols, cols), cols)
    gy_own = buf.at[1, chip, pl.ds(pl.multiple_of(core * (rows // 2), rows // 2), rows // 2)]
    local = [(x_ref.at[core], xs_ref.at[core]), (gy_ref.at[core], gy_own)]
    local += [(w.at[:, own_cols], w_ref.at[i]) for i, w in enumerate((wq_ref, wk_ref, wv_ref))] + [(wo_ref.at[own_cols], wrow_ref)]
    loads = [pltpu.make_async_copy(src, dst, load_sem.at[i]) for i, (src, dst) in enumerate(local)]
    for ld in loads:
        ld.start()
    barrier = pltpu.get_barrier_semaphore()
    each_peer(lambda p: pl.semaphore_signal(barrier, inc=1, device_id=dev(p), device_id_type=pl.DeviceIdType.MESH))
    pl.semaphore_signal(barrier, inc=1, device_id=partner, device_id_type=pl.DeviceIdType.MESH)
    pl.semaphore_wait(barrier, n_chip)

    swaps = [pltpu.make_async_remote_copy(
        src_ref=src, dst_ref=dst, send_sem=swap_sem.at[0, i], recv_sem=swap_sem.at[1, i], device_id=partner, device_id_type=pl.DeviceIdType.MESH)
        for i, (src, dst) in enumerate(((x_ref.at[1 - core], xs_ref.at[core]), (pos_ref.at[1 - core], pos_all.at[chip, core]), (gy_ref.at[1 - core], gy_own)))]
    for sw in swaps:
        sw.start()
    pos_copy = to_peers(pos_all.at[chip], pos_all, ps_sem, pr_sem)
    pos_all[chip, core] = pos_ref[core]
    loads[0].wait()
    swaps[0].wait_recv()
    for c in range(CHUNKS):
        top = (c * part) % (rows // 2)
        piece, ts = c * part // (rows // 2), slice(top, top + part)
        acc = jnp.zeros((part, HEAD_DIM), F32)
        for lo in range(0, dim, HEAD_DIM):
            x = xs_ref[piece, ts, lo:lo + HEAD_DIM].astype(F32)
            acc += x * x
        inv = lax.rsqrt(jnp.sum(acc, axis=1, keepdims=True) / dim + NORM_EPS)
        for lo in range(0, dim, HEAD_DIM):
            hs = slice(lo, lo + HEAD_DIM)
            x = xs_ref[piece, ts, hs].astype(F32)
            buf[0, chip, c * part:(c + 1) * part, hs] = (x * inv * gt_ref[2:3, hs]).astype(BF)
    swaps[1].wait_recv()
    each_peer(lambda p: pos_copy(p, chip).start())
    start_own(0)
    for ld in loads[2:]:
        ld.wait()

    def project(p):
        ts = pl.ds(pl.multiple_of(p * rows, rows), rows)
        h = buf[0, p]
        for idx, out in enumerate((qh_ref, kh_ref)):
            raw = mm32(h, w_ref[idx])
            out[ts, :] = raw
            ssq[pl.ds(idx * n_chip + p, 1), :] = as_row(jnp.sum(raw * raw, axis=1, keepdims=True))
        v_ref[ts, :] = mm32(h, w_ref[2]).astype(BF)

    project(chip)
    each_peer(lambda p: pos_copy(p, p).wait_recv())
    for p in range(n_chip):
        for u in range(2):
            ts = slice(p * rows + u * (rows // 2), p * rows + (u + 1) * (rows // 2))
            angles = column(pos_all[p, u, 0:1, :]) * f_ref[0:1, :]
            c_ref[ts, :] = jnp.cos(angles)
            s_ref[ts, :] = jnp.sin(angles) * f_ref[1:2, :]

    def gather_step(s, _):
        stage(0, s)

        def both(dr, _):
            dist = (s + 1) * (1 - 2 * dr)
            project(chip_at(lax.rem(ring - dist + 2 * n_chip, n_chip)))
            return 0

        lax.fori_loop(0, 2, both, 0)
        return 0

    lax.fori_loop(0, half - 1, gather_step, 0)
    loads[1].wait()
    swaps[2].wait_recv()
    start_own(1)
    gys_copy = pltpu.make_async_copy(buf.at[1, chip], gys_ref, out_sem.at[1])
    gys_copy.start()
    last_stage(0)
    project(slot_at(0, half))
    hall_copy = pltpu.make_async_copy(buf.at[0], hall_ref, out_sem.at[0])
    hall_copy.start()
    for hs in heads:
        vt_ref[hs, :] = v_ref[:, hs].T
    ssq_copy = to_peers(ssq, ssq_all, qs_sem, qr_sem)
    each_peer(lambda p: ssq_copy(p, chip).start())
    ssq_all[chip] = ssq[...]
    each_peer(lambda p: ssq_copy(p, p).wait_recv())
    total = ssq_all[0]
    for p in range(1, n_chip):
        total = total + ssq_all[p]
    inv_ref[...] = lax.rsqrt(total / dim + NORM_EPS)

    def finish_qk(p, _):
        ts = pl.ds(pl.multiple_of(p * rows, rows), rows)
        for idx, (hat_ref, out) in enumerate(((qh_ref, q_ref), (kh_ref, k_ref))):
            inv = column(inv_ref[pl.ds(idx * n_chip + p, 1), :])
            for hs in heads:
                hat = hat_ref[ts, hs] * inv
                hat_ref[ts, hs] = hat
                u = hat * g_ref[idx:idx + 1, hs]
                out[ts, hs] = (u * c_ref[ts, :] + half_roll(u) * s_ref[ts, :]).astype(BF)
        return 0

    lax.fori_loop(0, n_chip, finish_qk, 0)

    blk = FWD_BLOCK
    scale = HEAD_DIM ** -0.5 * LOG2E
    causal = lax.broadcasted_iota(jnp.int32, (blk, blk), 0) <= lax.broadcasted_iota(jnp.int32, (blk, blk), 1)

    def attend(j, _):
        qs = pl.ds(pl.multiple_of(j * blk, blk), blk)
        qb = [q_ref[qs, hs] for hs in heads]

        def tile(i, carry, diag):
            ks = pl.ds(pl.multiple_of(i * blk, blk), blk)
            out = []
            for h, hs in enumerate(heads):
                m, l, acc = carry[h]
                s = mm32_nt(k_ref[ks, hs], qb[h])
                if diag:
                    s = jnp.where(causal, s, NEG_BIG)
                mn = jnp.maximum(m, jnp.max(s, axis=0, keepdims=True))
                al = jnp.exp2((m - mn) * scale)
                p = jnp.exp2((s - mn) * scale)
                l = al * l + jnp.sum(p, axis=0, keepdims=True)
                out.append((mn, l, al * acc + mm32(vt_ref[hs, ks], p.astype(BF))))
            return tuple(out)

        st = tuple((jnp.full((1, blk), NEG_BIG, F32), jnp.zeros((1, blk), F32), jnp.zeros((HEAD_DIM, blk), F32)) for _ in heads)
        st = lax.fori_loop(0, j, lambda i, cr: tile(i, cr, False), st)
        st = tile(j, st, True)
        for h, hs in enumerate(heads):
            m, l, acc = st[h]
            ot = acc / l
            ot_ref[hs, qs] = ot
            att_ref[qs, hs] = ot.T.astype(BF)
            lse_ref[h:h + 1, qs] = m * scale + jnp.log2(l)
        return 0

    def att_copy(p, owner):
        return pltpu.make_async_remote_copy(
            src_ref=att_ref.at[pl.ds(p * rows, rows)], dst_ref=atok_ref.at[:, pl.ds(pl.multiple_of(owner * cols, cols), cols)], send_sem=as_sem.at[p], recv_sem=ar_sem.at[owner],
            device_id=dev(p), device_id_type=pl.DeviceIdType.MESH)

    def send_att(lo, hi):
        for p in range(lo, hi):
            @pl.when(p != chip)
            def _():
                att_copy(p, chip).start()

    def use_gy(p):
        ts = pl.ds(pl.multiple_of(p * rows, rows), rows)
        gy = buf[1, p]
        datt_ref[ts, :] = mm32_nt(gy, wrow_ref[...]).astype(BF)
        dwo_ref[...] += mm32(ot_ref[:, ts].astype(BF), gy)

    n_att = n_chip * rows // blk
    lax.fori_loop(0, n_att // 2, attend, 0)
    stage(1, 0)
    send_att(0, half)
    lax.fori_loop(n_att // 2, n_att, attend, 0)

    def raw_of(w, out):
        def load(m, slot):
            return pltpu.make_async_copy(w.at[:, pl.ds(pl.multiple_of(m * cols, cols), cols)], wbuf.at[slot], w_sem.at[slot])

        load(0, 0).start()

        def step(m, _):
            slot = lax.rem(m, 2)
            load(m, slot).wait()

            @pl.when(m + 1 < n_chip)
            def _():
                load(m + 1, 1 - slot).start()
            out[:, pl.ds(pl.multiple_of(m * cols, cols), cols)] = mm32(buf[0, chip], wbuf[slot])
            return 0

        lax.fori_loop(0, n_chip, step, 0)

    raw_of(wq_ref, qr_ref)
    raw_of(wk_ref, kr_ref)
    stage(1, 1)
    send_att(half, n_chip)
    atok_ref[:, pl.ds(pl.multiple_of(chip * cols, cols), cols)] = att_ref[pl.ds(pl.multiple_of(chip * rows, rows), rows), :]
    dwo_ref[...] = jnp.zeros_like(dwo_ref)

    def use_ring(n, _):
        dist = ((n + 1) // 2) * (2 * lax.rem(n, 2) - 1)
        use_gy(chip_at(lax.rem(ring - dist + 2 * n_chip, n_chip)))
        return 0

    lax.fori_loop(0, n_chip - 3, use_ring, 0)
    stage(1, half - 2)
    lax.fori_loop(n_chip - 3, n_chip - 1, use_ring, 0)
    last_stage(1)
    use_gy(slot_at(0, half))

    each_peer(lambda p: att_copy(p, p).wait_recv())
    each_peer(lambda p: att_copy(p, chip).wait_send())
    each_peer(lambda p: pos_copy(p, chip).wait_send())
    each_peer(lambda p: ssq_copy(p, chip).wait_send())
    for sw in swaps:
        sw.wait_send()
    drain(0)
    drain(1)
    hall_copy.wait()
    gys_copy.wait()


def back_kernel(q_ref, k_ref, v_ref, do_ref, ot_ref, lse_ref, g_ref, gt_ref, inv_ref,
                hall_ref, qh_hbm, kh_hbm, c_hbm, s_hbm, qr_hbm, kr_hbm, wq_ref, wk_ref, wv_ref, dwo_ref, wo_ref, at_hbm, x_hbm, gy_hbm,
                dwq_ref, dwk_ref, dwv_ref, y_ref, gx_ref, dwo_out, dg_out, dgn_out,
                dq_ref, dk_ref, dv_ref, dka_ref, dva_ref, kt_ref, qh_ref, kh_ref, c_ref, s_ref, qr_ref, kr_ref,
                tok, pairs, pair_in, dt_ref, hblk, wblk, dwo_in, row_ref, row_all,
                dhid_ref, dg_ref, at_ref, x_ref, gy_ref, ys_ref, gxs_ref, dgp, dgp_in, gpart, gpair_in, gsel, gsel_in,
                sw_sem, gs_sem, gr_sem, load_sem, h_sem, w_sem, xs_sem, xr_sem, ps_sem, pr_sem, rs_sem, rr_sem, own_sem, do_sem):
    me = lax.axis_index('sp')
    chip, core = me // 2, lax.rem(me, 2)
    n, cols = q_ref.shape
    rows, dim = qr_ref.shape
    n_chip = n // rows
    partner = {'sp': me + 1 - 2 * core}
    heads = [slice(lo, lo + HEAD_DIM) for lo in range(0, cols, HEAD_DIM)]
    own_rows = pl.ds(pl.multiple_of(chip * rows, rows), rows)
    own_cols = pl.ds(pl.multiple_of(chip * cols, cols), cols)
    MESH = pl.DeviceIdType.MESH

    def dev(p):
        return {'sp': 2 * p + core}

    def each_peer(fn):
        for p in range(n_chip):
            @pl.when(p != chip)
            def _():
                fn(p)

    sides = ((qh_hbm, qh_ref), (kh_hbm, kh_ref), (c_hbm, c_ref), (s_hbm, s_ref), (qr_hbm, qr_ref), (kr_hbm, kr_ref), (dwo_ref.at[core], dwo_out), (at_hbm, at_ref), (x_hbm, x_ref), (gy_hbm, gy_ref))
    loads = [pltpu.make_async_copy(src, dst, load_sem.at[i]) for i, (src, dst) in enumerate(sides)]
    for ld in loads:
        ld.start()

    def load_h(p, slot):
        return pltpu.make_async_copy(hall_ref.at[:, pl.ds(pl.multiple_of(p * cols, cols), cols)], hblk.at[slot], h_sem.at[slot])

    def load_o(m, slot):
        return pltpu.make_async_copy(wo_ref.at[pl.ds(pl.multiple_of(m * cols, cols), cols)], wblk.at[slot, 0], w_sem.at[slot, 0])

    load_h(0, 0).start()
    load_o(0, 0).start()
    barrier = pltpu.get_barrier_semaphore()
    each_peer(lambda p: pl.semaphore_signal(barrier, inc=1, device_id=dev(p), device_id_type=MESH))
    pl.semaphore_signal(barrier, inc=1, device_id=partner, device_id_type=MESH)
    pl.semaphore_wait(barrier, n_chip)

    dwo_copy = pltpu.make_async_remote_copy(
        src_ref=dwo_ref.at[1 - core], dst_ref=dwo_in, send_sem=do_sem.at[0], recv_sem=do_sem.at[1], device_id=partner, device_id_type=MESH)
    dwo_copy.start()

    def to_partner(src, dst, i):
        return pltpu.make_async_remote_copy(src_ref=src, dst_ref=dst, send_sem=sw_sem.at[0, i], recv_sem=sw_sem.at[1, i], device_id=partner, device_id_type=MESH)

    y_swap = to_partner(ys_ref.at[1 - core], y_ref.at[core], 0)
    gx_swap = to_partner(gxs_ref.at[1 - core], gx_ref.at[core], 1)
    dg_swap = to_partner(dgp.at[1 - core], dgp_in, 2)
    gn_swap = to_partner(gpart.at[1 - core], gpair_in, 3)
    y_own = pltpu.make_async_copy(ys_ref.at[core], y_ref.at[core], sw_sem.at[0, 4])
    gx_own = pltpu.make_async_copy(gxs_ref.at[core], gx_ref.at[core], sw_sem.at[1, 4])

    def tok_copy(t, p, owner):
        src = (dq_ref, dk_ref, dv_ref)[t].at[pl.ds(pl.multiple_of(p * rows, rows), rows)]
        dst = tok.at[t, :, pl.ds(pl.multiple_of(owner * cols, cols), cols)]
        return pltpu.make_async_remote_copy(src_ref=src, dst_ref=dst, send_sem=xs_sem.at[t, p], recv_sem=xr_sem.at[t, owner], device_id=dev(p), device_id_type=MESH)

    blk = BWD_BLOCK
    span = blk // rows
    n_blk = n // blk
    sc = HEAD_DIM ** -0.5
    scale = sc * LOG2E
    for hs in heads:
        kt_ref[hs, :] = k_ref[:, hs].T
    dka_ref[...] = jnp.zeros_like(dka_ref)
    dva_ref[...] = jnp.zeros_like(dva_ref)
    causal = lax.broadcasted_iota(jnp.int32, (blk, blk), 0) <= lax.broadcasted_iota(jnp.int32, (blk, blk), 1)

    def send_dq(j):
        for u in range(span):
            p = j * span + u

            @pl.when(p != chip)
            def _():
                tok_copy(0, p, chip).start()

    def q_step(j, _):
        qs = pl.ds(pl.multiple_of(j * blk, blk), blk)
        qb = [q_ref[qs, hs] for hs in heads]
        dob = [do_ref[qs, hs] for hs in heads]
        lse = [lse_ref[h:h + 1, qs] for h in range(len(heads))]
        dl = [jnp.sum(ot_ref[hs, qs] * dob[h].astype(F32).T, axis=0, keepdims=True) for h, hs in enumerate(heads)]

        def tile(i, carry, diag):
            ks = pl.ds(pl.multiple_of(i * blk, blk), blk)
            out = []
            for h, hs in enumerate(heads):
                s = mm32_nt(k_ref[ks, hs], qb[h])
                dp = mm32_nt(v_ref[ks, hs], dob[h])
                p = jnp.exp2(s * scale - lse[h])
                if diag:
                    p = jnp.where(causal, p, 0.0)
                ds = (p * (dp - dl[h])).astype(BF)
                dva_ref[ks, hs] += mm32(p.astype(BF), dob[h])
                dka_ref[ks, hs] += mm32(ds, qb[h])
                out.append(carry[h] + mm32(kt_ref[hs, ks], ds))
            return tuple(out)

        st = tuple(jnp.zeros((HEAD_DIM, blk), F32) for _ in heads)
        st = lax.fori_loop(0, j, lambda i, cr: tile(i, cr, False), st)
        st = tile(j, st, True)
        for h, hs in enumerate(heads):
            dq_ref[qs, hs] = (st[h] * sc).T.astype(BF)

        @pl.when(j > 0)
        def _():
            send_dq(j - 1)
        return 0

    lax.fori_loop(0, n_blk, q_step, 0)
    dk_ref[...] = (dka_ref[...] * sc).astype(BF)
    dv_ref[...] = dva_ref[...].astype(BF)
    send_dq(n_blk - 1)
    for t, src in enumerate((dq_ref, dk_ref, dv_ref)):
        tok[t, :, own_cols] = src[own_rows, :]
    for t in (1, 2):
        each_peer(lambda p: tok_copy(t, p, chip).start())

    def pair_copy(w, p):
        return pltpu.make_async_remote_copy(
            src_ref=pairs.at[w, p, 1 - core], dst_ref=pair_in.at[w, p], send_sem=ps_sem.at[w, p], recv_sem=pr_sem.at[w, p], device_id=partner, device_id_type=MESH)

    grads = (dwq_ref, dwk_ref, dwv_ref)

    def dw_copy(w, p, owner):
        dst = grads[w].at[:, pl.ds(pl.multiple_of(owner * cols, cols), cols)]
        return pltpu.make_async_remote_copy(src_ref=pairs.at[w, p, core], dst_ref=dst, send_sem=xs_sem.at[3 + w, p], recv_sem=xr_sem.at[3 + w, owner], device_id=dev(p), device_id_type=MESH)

    def own_copy(w):
        return pltpu.make_async_copy(pairs.at[w, chip, core], grads[w].at[:, own_cols], own_sem.at[w])

    def partial(w, slot_t, h, p):
        dw = mm32(dt_ref[slot_t], h).T
        pairs[w, p, 0] = dw[:rows // 2]
        pairs[w, p, 1] = dw[rows // 2:]

    def merge(w, p):
        pair_copy(w, p).wait_recv()
        pairs[w, p, core] += pair_in[w, p]

    def send_dw(w, p):
        @pl.when(p != chip)
        def _():
            dw_copy(w, p, chip).start()

        @pl.when(p == chip)
        def _():
            own_copy(w).start()

    def each_h(ws, tail_fn):
        def step(p, _):
            slot = lax.rem(p, 2)
            load_h(p, slot).wait()

            @pl.when(p + 1 < n_chip)
            def _():
                load_h(p + 1, 1 - slot).start()
            for w, slot_t in ws:
                partial(w, slot_t, hblk[slot], p)
            tail_fn(p)
            for w, _ in ws:
                pair_copy(w, p).start()
            return 0

        lax.fori_loop(0, n_chip, step, 0)

    dt_ref[0] = dv_ref[...].T
    each_h(((2, 0),), lambda p: None)
    load_h(0, 0).start()
    for ld in loads:
        ld.wait()

    dhid_ref[...] = x_ref[...].astype(F32)

    def y_step(m, _):
        slot = lax.rem(m, 2)
        load_o(m, slot).wait()

        @pl.when(m + 1 < n_chip)
        def _():
            load_o(m + 1, 1 - slot).start()
        dhid_ref[...] += mm32(at_ref[:, pl.ds(pl.multiple_of(m * cols, cols), cols)], wblk[slot, 0])
        return 0

    lax.fori_loop(0, n_chip, y_step, 0)
    half = rows // 2
    for u in range(2):
        ys_ref[u] = dhid_ref[u * half:(u + 1) * half, :].astype(BF)

    hats = ((qr_ref, 0), (kr_ref, 1))
    row_ref[...] = jnp.zeros_like(row_ref)
    inv_t = [column(inv_ref[pl.ds(idx * n_chip + chip, 1), :]) for idx in range(2)]
    c_t, s_t = c_ref[own_rows, :], s_ref[own_rows, :]

    def normed(idx, hs):
        d = tok[idx, :, hs].astype(F32)
        return (d * c_t - half_roll(d) * s_t) * gt_ref[idx:idx + 1, hs]

    row_cols = []
    for raw_ref, idx in hats:
        each_peer(lambda p: tok_copy(idx, p, p).wait_recv())
        acc = jnp.zeros((rows, HEAD_DIM), F32)
        for lo in range(0, dim, HEAD_DIM):
            hs = slice(lo, lo + HEAD_DIM)
            acc += normed(idx, hs) * (raw_ref[:, hs] * inv_t[idx])
        row = jnp.sum(acc, axis=1, keepdims=True) / dim
        row_ref[idx:idx + 1, :] = as_row(row)
        row_cols.append(row)

    y_swap.start()
    y_own.start()

    def row_copy(p, owner):
        return pltpu.make_async_remote_copy(src_ref=row_ref, dst_ref=row_all.at[owner], send_sem=rs_sem.at[p], recv_sem=rr_sem.at[owner], device_id=dev(p), device_id_type=MESH)

    for raw_ref, idx in hats:
        for lo in range(0, dim, HEAD_DIM):
            hs = slice(lo, lo + HEAD_DIM)
            tok[idx, :, hs] = (inv_t[idx] * (normed(idx, hs) - raw_ref[:, hs] * inv_t[idx] * row_cols[idx])).astype(BF)
        if idx == 0:
            each_peer(lambda p: row_copy(p, chip).start())
            row_all[chip] = row_ref[...]

    def merge_v(p, _):
        merge(2, p)
        return 0

    def send_v(p, _):
        send_dw(2, p)
        return 0

    lax.fori_loop(0, n_chip, merge_v, 0)

    def load_w(m, slot):
        return [pltpu.make_async_copy(w.at[pl.ds(pl.multiple_of(m * cols, cols), cols)], wblk.at[slot, i], w_sem.at[slot, i]) for i, w in enumerate((wq_ref, wk_ref, wv_ref))]

    for ld in load_w(0, 0):
        ld.start()
    lax.fori_loop(0, n_chip, send_v, 0)
    each_peer(lambda p: row_copy(p, p).wait_recv())

    dg_ref[...] = jnp.zeros_like(dg_ref)

    def head_step(p, _):
        ts = pl.ds(pl.multiple_of(p * rows, rows), rows)
        for idx, (d_ref, hat_ref) in enumerate(((dq_ref, qh_ref), (dk_ref, kh_ref))):
            inv = column(inv_ref[pl.ds(idx * n_chip + p, 1), :])
            row = column(row_all[p, idx:idx + 1, :])
            for hs in heads:
                d = d_ref[ts, hs].astype(F32)
                rot = d * c_ref[ts, :] - half_roll(d) * s_ref[ts, :]
                hat = hat_ref[ts, hs]
                raw = inv * (rot * g_ref[idx:idx + 1, hs] - hat * row)
                dt_ref[idx, hs, ts] = raw.astype(BF).T
                dg_ref[idx:idx + 1, hs] += jnp.sum(rot * hat, axis=0, keepdims=True)
        return 0

    lax.fori_loop(0, n_chip, head_step, 0)
    dgp[...] = jnp.zeros_like(dgp)
    for u in range(2):
        dgp[u, 0:2, :] = dg_ref[0:2, u * half:(u + 1) * half]

    def lagged(p):
        @pl.when(p > 0)
        def _():
            for w in range(2):
                merge(w, p - 1)

        @pl.when(p > 1)
        def _():
            for w in range(2):
                send_dw(w, p - 2)

    each_h(((0, 0), (1, 1)), lagged)
    for w in range(2):
        send_dw(w, n_chip - 2)
        merge(w, n_chip - 1)
    dwo_copy.wait_recv()
    dwo_out[...] += dwo_in[...]
    for w in range(2):
        send_dw(w, n_chip - 1)
    dg_swap.start()

    each_peer(lambda p: tok_copy(2, p, p).wait_recv())

    def hid_step(m, _):
        slot = lax.rem(m, 2)
        for ld in load_w(m, slot):
            ld.wait()

        @pl.when(m + 1 < n_chip)
        def _():
            for ld in load_w(m + 1, 1 - slot):
                ld.start()
        out = pl.ds(pl.multiple_of(m * cols, cols), cols)
        dhid_ref[:, out] = mm32_nt(tok[0], wblk[slot, 0]) + mm32_nt(tok[1], wblk[slot, 1]) + mm32_nt(tok[2], wblk[slot, 2])
        return 0

    lax.fori_loop(0, n_chip, hid_step, 0)

    blocks = [slice(lo, lo + HEAD_DIM) for lo in range(0, dim, HEAD_DIM)]
    acc = jnp.zeros((rows, HEAD_DIM), F32)
    dot = jnp.zeros((rows, HEAD_DIM), F32)
    for hs in blocks:
        x = x_ref[:, hs].astype(F32)
        acc += x * x
        dot += x * dhid_ref[:, hs] * gt_ref[2:3, hs]
    x_inv = lax.rsqrt(jnp.sum(acc, axis=1, keepdims=True) / dim + NORM_EPS)
    mean = jnp.sum(dot, axis=1, keepdims=True) * x_inv / dim
    gpart[...] = jnp.zeros_like(gpart)
    for i, hs in enumerate(blocks):
        x_hat = x_ref[:, hs].astype(F32) * x_inv
        d = dhid_ref[:, hs]
        gx = (gy_ref[:, hs].astype(F32) + x_inv * (d * gt_ref[2:3, hs] - x_hat * mean)).astype(BF)
        gxs_ref[0, :, hs] = gx[:half]
        gxs_ref[1, :, hs] = gx[half:]
        gpart[i % 2, i // 2, 0:1, :] = jnp.sum(d * x_hat, axis=0, keepdims=True)
    gn_swap.start()
    gx_swap.start()
    gx_own.start()
    dg_swap.wait_recv()
    dg_out[...] = dgp[core] + dgp_in[...]
    gn_swap.wait_recv()
    gsel[...] = gpart[core] + gpair_in[...]

    def gn_copy(p, owner):
        return pltpu.make_async_remote_copy(src_ref=gsel.at[p], dst_ref=gsel_in.at[owner], send_sem=gs_sem.at[p], recv_sem=gr_sem.at[owner], device_id=dev(p), device_id_type=MESH)

    each_peer(lambda p: gn_copy(p, chip).start())
    gsel_in[chip] = gsel[chip]
    each_peer(lambda p: gn_copy(p, p).wait_recv())
    total = gsel_in[0]
    for p in range(1, n_chip):
        total = total + gsel_in[p]
    dgn_out[...] = total
    each_peer(lambda p: gn_copy(p, chip).wait_send())
    for sw in (y_swap, gx_swap):
        sw.wait_recv()
    for sw in (y_swap, gx_swap, dg_swap, gn_swap):
        sw.wait_send()
    y_own.wait()
    gx_own.wait()

    for w in range(3):
        each_peer(lambda p: dw_copy(w, p, p).wait_recv())
        each_peer(lambda p: dw_copy(w, p, chip).wait_send())
        each_peer(lambda p: tok_copy(w, p, chip).wait_send())
        own_copy(w).wait()
        for p in range(n_chip):
            pair_copy(w, p).wait_send()
    each_peer(lambda p: row_copy(p, chip).wait_send())
    dwo_copy.wait_send()


VM = pl.BlockSpec(memory_space=pltpu.VMEM)


def mm32(a, b):
    return jnp.dot(a, b, preferred_element_type=F32)


def mm32_nt(a, b):
    return lax.dot_general(a, b, NT, preferred_element_type=F32)


def front(x, gy, w_query, w_key, w_value, w_out, pos, gains_h, gains, freq, n_chip):
    loc, dim = x.shape[1:]
    rows = 2 * loc
    cols = gains_h.shape[1]
    n = n_chip * rows
    heads = cols // HEAD_DIM
    any_spec = pl.BlockSpec(memory_space=pl.ANY)
    half = n_chip // 2
    dma, vmem = pltpu.SemaphoreType.DMA, pltpu.VMEM
    outs = [((n_chip, rows, dim), BF), ((n, cols), BF), ((n, cols), BF), ((n, cols), BF), ((n, cols), F32), ((n, cols), F32), ((cols, n), F32), ((heads, n), F32),
            ((rows, dim), BF), ((n, cols), BF), ((cols, dim), F32), ((n, HEAD_DIM), F32), ((n, HEAD_DIM), F32), ((2 * n_chip, rows), F32), ((rows, dim), F32), ((rows, dim), F32),
            ((2, loc, dim), BF), ((rows, dim), BF)]
    return pl.pallas_call(
        front_kernel, name='front', out_shape=tuple(jax.ShapeDtypeStruct(s, d) for s, d in outs),
        in_specs=[any_spec] * 6 + [VM] * 4, out_specs=(any_spec,) + (VM,) * 16 + (any_spec,),
        scratch_shapes=[
            vmem((2, n_chip, rows, dim), BF), vmem((3, dim, cols), BF), vmem((cols, dim), BF), vmem((n, cols), BF), vmem((cols, n), BF),
            vmem((n_chip, 2, 8, loc), F32), vmem((2 * n_chip, rows), F32), vmem((n_chip, 2 * n_chip, rows), F32), vmem((2, dim, cols), BF),
            dma((2,)), dma((6,)), dma((2, 3)), dma((2,)), dma((2, 2, half, CHUNKS)), dma((2, 2, half, CHUNKS)),
            dma((n_chip,)), dma((n_chip,)), dma((n_chip,)), dma((n_chip,)), dma((n_chip,)), dma((n_chip,))],
        compiler_params=pltpu.CompilerParams(collective_id=0, has_side_effects=True, vmem_limit_bytes=67043328),
        cost_estimate=pl.CostEstimate(flops=400 * n * dim * cols, bytes_accessed=40 * n * dim, transcendentals=n * n * heads // 2),
    )(x, gy, w_query, w_key, w_value, w_out, pos, gains_h, gains, freq)


def back(q, k, v, d_att, att_t, lse, gains_h, gains, inv, hid, qh, kh, cos_a, sin_a, q_raw, k_raw, w_query, w_key, w_value, dwo, w_out, att_tok, x, gy):
    n, cols = q.shape
    rows, dim = q_raw.shape
    n_chip = n // rows
    any_spec = pl.BlockSpec(memory_space=pl.ANY)
    dma = pltpu.SemaphoreType.DMA
    grad = jax.ShapeDtypeStruct((rows // 2, dim), F32)
    seq = jax.ShapeDtypeStruct((2, rows // 2, dim), BF)
    small = jax.ShapeDtypeStruct((8, cols // 2), F32)
    tile = (n_chip, 8, cols // 2)
    vmem = pltpu.VMEM
    return pl.pallas_call(
        back_kernel, name='back', in_specs=[VM] * 9 + [any_spec] * 15, out_specs=(any_spec,) * 5 + (VM,) * 3,
        out_shape=(grad,) * 3 + (seq, seq, grad, small, small),
        scratch_shapes=[
            vmem((n, cols), BF), vmem((n, cols), BF), vmem((n, cols), BF), vmem((n, cols), F32), vmem((n, cols), F32), vmem((cols, n), BF),
            vmem((n, cols), F32), vmem((n, cols), F32), vmem((n, HEAD_DIM), F32), vmem((n, HEAD_DIM), F32), vmem((rows, dim), F32), vmem((rows, dim), F32),
            vmem((3, rows, dim), BF), vmem((3, n_chip, 2, rows // 2, cols), F32), vmem((3, n_chip, rows // 2, cols), F32),
            vmem((2, cols, n), BF), vmem((2, n, cols), BF), vmem((2, 3, cols, dim), BF), vmem((rows // 2, dim), F32),
            vmem((8, rows), F32), vmem((n_chip, 8, rows), F32),
            vmem((rows, dim), F32), vmem((8, cols), F32), vmem((rows, dim), BF), vmem((rows, dim), BF), vmem((rows, dim), BF), vmem((2, rows // 2, dim), BF), vmem((2, rows // 2, dim), BF),
            vmem((2, 8, cols // 2), F32), vmem((8, cols // 2), F32), vmem((2,) + tile, F32), vmem(tile, F32), vmem(tile, F32), vmem(tile, F32),
            dma((2, 5)), dma((n_chip,)), dma((n_chip,)), dma((10,)), dma((2,)), dma((2, 3)), dma((6, n_chip)), dma((6, n_chip)), dma((3, n_chip)), dma((3, n_chip)),
            dma((n_chip,)), dma((n_chip,)), dma((3,)), dma((2,))],
        compiler_params=pltpu.CompilerParams(collective_id=1, has_side_effects=True, vmem_limit_bytes=67043328),
        cost_estimate=pl.CostEstimate(flops=400 * n * dim * cols, bytes_accessed=40 * n * dim, transcendentals=n * n),
    )(q, k, v, d_att, att_t, lse, gains_h, gains, inv, hid, qh, kh, cos_a, sin_a, q_raw, k_raw, w_query, w_key, w_value, dwo, w_out, att_tok, x, gy)


def solution(mesh):
    n_chip = mesh.shape['sp'] // 2

    def device_step(x_loc, gy_loc, positions, g_norm, w_query, w_key, w_value, w_out, g_query, g_key):
        chip = lax.axis_index('sp') // 2
        loc, dim = x_loc.shape[1], x_loc.shape[2]
        rows = 2 * loc
        cols = dim // n_chip
        pos = jnp.broadcast_to(positions.astype(F32)[:, None, :], (2, 8, loc))
        gains = jnp.stack([g_query, g_key, g_norm]).astype(F32)
        gains_h = lax.dynamic_slice_in_dim(gains, chip * cols, cols, axis=1)
        hid_all, q, k, v, qh_hat, kh_hat, att_t, lse, att_tok, d_att, dwo, cos_a, sin_a, inv_all, q_raw, k_raw, x_sw, gy_sw = front(
            x_loc, gy_loc, w_query, w_key, w_value, w_out, pos, gains_h, gains, rope_rows(), n_chip)
        dwq, dwk, dwv, y, grad_x, dwo, dg, dgn = back(
            q, k, v, d_att, att_t, lse, gains_h, gains, inv_all, hid_all.reshape(n_chip * rows, dim), qh_hat, kh_hat, cos_a, sin_a,
            q_raw, k_raw, w_query, w_key, w_value, dwo.reshape(2, loc, dim), w_out, att_tok, x_sw.reshape(rows, dim), gy_sw)
        return y, grad_x, dgn[0], dwq, dwk, dwv, dwo, dg[0], dg[1]

    seq_spec = P('dp', 'sp', None)
    mat_rep = P(None, None)
    vec_rep = P(None)
    row_spec = P(('dp', 'sp'), None)
    vec_spec = P(('dp', 'sp'))
    return jax.shard_map(device_step, mesh=mesh, in_specs=(seq_spec, seq_spec, P('dp', 'sp'), vec_rep, mat_rep, mat_rep, mat_rep, mat_rep, vec_rep, vec_rep), out_specs=(seq_spec, seq_spec, vec_spec, row_spec, row_spec, row_spec, row_spec, vec_spec, vec_spec), check_vma=False)
```

```python
import functools
import jax
import jax.numpy as jnp
from jax import lax
from jax.experimental import pallas as pl
from jax.experimental.pallas import tpu as pltpu
from jax.sharding import PartitionSpec as P

HEAD_DIM = 128
NORM_EPS = 1e-5
ROPE_BASE = 10000.0
NEG_BIG = -1e30
LOG2E = 1.4426950408889634
FWD_BLOCK = 512
CHUNKS = 4
EARLY = 3
BWD_BLOCK = 512
F32, BF = jnp.float32, jnp.bfloat16
NT = (((1,), (1,)), ((), ()))


def rope_rows():
    half = HEAD_DIM // 2
    inv_freq = ROPE_BASE ** (-jnp.arange(half, dtype=F32) * (2.0 / HEAD_DIM))
    sign = jnp.concatenate([-jnp.ones(half, F32), jnp.ones(half, F32)])
    return jnp.stack([jnp.concatenate([inv_freq, inv_freq]), sign])


def column(row):
    return jnp.broadcast_to(row, (HEAD_DIM, row.shape[1])).T


def as_row(col):
    return jnp.broadcast_to(col, (col.shape[0], HEAD_DIM)).T[0:1, :]


def half_roll(u):
    return pltpu.roll(u, HEAD_DIM // 2, 1)


def flip(a, b, bits=3):
    out = 0
    for i in range(bits):
        x, y = (a // 2 ** i) % 2, (b // 2 ** i) % 2
        out = out + 2 ** i * (x + y - 2 * x * y)
    return out


def front_kernel(x_ref, gy_ref, wq_ref, wk_ref, wv_ref, wo_ref, pos_ref, g_ref, gt_ref, f_ref,
                 hall_ref, q_out, k_out, v_out, qh_out, kh_out, ot_out, lse_ref, att_out, datt_ref, dwo_ref, c_out, s_out, inv_ref, qr_out, kr_out, xs_out, gys_ref,
                 q_ref, k_ref, v_ref, qh_ref, kh_ref, ot_ref, c_ref, s_ref, qr_ref, kr_ref, xs_ref, flush_sem,
                 buf, w_ref, wrow_ref, att_ref, vt_ref, pos_all, ssq, ssq_all, wbuf,
                 w_sem, load_sem, swap_sem, out_sem, ssem, rsem, ps_sem, pr_sem, qs_sem, qr_sem):
    me = lax.axis_index('sp')
    chip, core = me // 2, lax.rem(me, 2)
    n_chip, rows, dim = hall_ref.shape
    cols = q_ref.shape[1]
    part = rows // CHUNKS
    half = n_chip // 2
    heads = [slice(lo, lo + HEAD_DIM) for lo in range(0, cols, HEAD_DIM)]

    def spot(p):
        z, y = p // 2, lax.rem(p, 2)
        return z + y * (n_chip - 1 - 2 * z)

    def chip_at(r):
        y = r // half
        return 2 * (r + y * (n_chip - 1 - 2 * r)) + y

    ring = spot(chip)

    def slot_at(dr, dist):
        step = dist if dr == 0 else -dist
        return chip_at(lax.rem(ring - step + 2 * n_chip, n_chip))

    def dev(p):
        return {'sp': 2 * p + core}

    right = dev(slot_at(1, 1))
    left = dev(slot_at(0, 1))

    def hop(t, dr, s, c, dist):
        view = buf.at[t, slot_at(dr, dist), pl.ds(c * part, part)]
        return pltpu.make_async_remote_copy(
            src_ref=view, dst_ref=view, send_sem=ssem.at[t, dr, s, c], recv_sem=rsem.at[t, dr, s, c],
            device_id=right if dr == 0 else left, device_id_type=pl.DeviceIdType.MESH)

    def in_half(dr, c):
        return (c < CHUNKS // 2) == (dr == 0)

    def start_own(t):
        for c in range(CHUNKS):
            for dr in range(2):
                hop(t, dr, 0, c, 0).start()

    def stage(t, s):
        for c in range(CHUNKS):
            for dr in range(2):
                hop(t, dr, s, c, s + 1).wait_recv()
                if in_half(dr, c):
                    hop(t, dr, s + 1, c, s + 1).start()
                else:
                    @pl.when(s < half - 2)
                    def _():
                        hop(t, dr, s + 1, c, s + 1).start()

    def last_stage(t):
        for c in range(CHUNKS):
            for dr in range(2):
                if in_half(dr, c):
                    hop(t, dr, half - 1, c, half).wait_recv()

    def drain(t):
        for s in range(half):
            for c in range(CHUNKS):
                for dr in range(2):
                    if s < half - 1 or in_half(dr, c):
                        hop(t, dr, s, c, s).wait_send()

    def to_peers(src, dst, s_sem, r_sem):
        def make(p, owner):
            return pltpu.make_async_remote_copy(
                src_ref=src, dst_ref=dst.at[owner], send_sem=s_sem.at[p], recv_sem=r_sem.at[owner],
                device_id=dev(p), device_id_type=pl.DeviceIdType.MESH)
        return make

    def each_peer(fn):
        for step in range(1, n_chip):
            fn(flip(chip, step))

    partner = {'sp': me + 1 - 2 * core}
    own_cols = pl.ds(pl.multiple_of(chip * cols, cols), cols)
    gy_own = buf.at[1, chip, pl.ds(pl.multiple_of(core * (rows // 2), rows // 2), rows // 2)]
    local = [(x_ref.at[core], xs_ref.at[core]), (gy_ref.at[core], gy_own)]
    local += [(w.at[:, own_cols], w_ref.at[i]) for i, w in enumerate((wq_ref, wk_ref, wv_ref))] + [(wo_ref.at[own_cols], wrow_ref)]
    loads = [pltpu.make_async_copy(src, dst, load_sem.at[i]) for i, (src, dst) in enumerate(local)]
    for ld in loads:
        ld.start()
    barrier = pltpu.get_barrier_semaphore()
    each_peer(lambda p: pl.semaphore_signal(barrier, inc=1, device_id=dev(p), device_id_type=pl.DeviceIdType.MESH))
    pl.semaphore_signal(barrier, inc=1, device_id=partner, device_id_type=pl.DeviceIdType.MESH)
    pl.semaphore_wait(barrier, n_chip)

    pending = []

    def flush(*pairs):
        for src, dst in pairs:
            copy = pltpu.make_async_copy(src, dst, flush_sem.at[len(pending)])
            copy.start()
            pending.append(copy)

    swaps = [pltpu.make_async_remote_copy(
        src_ref=src, dst_ref=dst, send_sem=swap_sem.at[0, i], recv_sem=swap_sem.at[1, i], device_id=partner, device_id_type=pl.DeviceIdType.MESH)
        for i, (src, dst) in enumerate(((x_ref.at[1 - core], xs_ref.at[core]), (pos_ref.at[1 - core], pos_all.at[chip, core]), (gy_ref.at[1 - core], gy_own)))]
    for sw in swaps:
        sw.start()
    pos_copy = to_peers(pos_all.at[chip], pos_all, ps_sem, pr_sem)
    pos_all[chip, core] = pos_ref[core]
    loads[0].wait()
    swaps[0].wait_recv()
    for c in range(CHUNKS):
        top = (c * part) % (rows // 2)
        piece, ts = c * part // (rows // 2), slice(top, top + part)
        acc = jnp.zeros((part, HEAD_DIM), F32)
        for lo in range(0, dim, HEAD_DIM):
            x = xs_ref[piece, ts, lo:lo + HEAD_DIM].astype(F32)
            acc += x * x
        inv = lax.rsqrt(jnp.sum(acc, axis=1, keepdims=True) / dim + NORM_EPS)
        for lo in range(0, dim, HEAD_DIM):
            hs = slice(lo, lo + HEAD_DIM)
            x = xs_ref[piece, ts, hs].astype(F32)
            buf[0, chip, c * part:(c + 1) * part, hs] = (x * inv * gt_ref[2:3, hs]).astype(BF)
    swaps[1].wait_recv()
    each_peer(lambda p: pos_copy(p, chip).start())
    start_own(0)
    for ld in loads[2:]:
        ld.wait()

    def project(p):
        ts = pl.ds(pl.multiple_of(p * rows, rows), rows)
        h = buf[0, p]
        for idx, out in enumerate((qh_ref, kh_ref)):
            raw = mm32(h, w_ref[idx])
            out[ts, :] = raw
            ssq[pl.ds(idx * n_chip + p, 1), :] = as_row(jnp.sum(raw * raw, axis=1, keepdims=True))
        v_ref[ts, :] = mm32(h, w_ref[2]).astype(BF)

    project(chip)
    each_peer(lambda p: pos_copy(p, p).wait_recv())
    for p in range(n_chip):
        for u in range(2):
            ts = slice(p * rows + u * (rows // 2), p * rows + (u + 1) * (rows // 2))
            angles = column(pos_all[p, u, 0:1, :]) * f_ref[0:1, :]
            c_ref[ts, :] = jnp.cos(angles)
            s_ref[ts, :] = jnp.sin(angles) * f_ref[1:2, :]

    def gather_step(s, _):
        stage(0, s)

        def both(dr, _):
            dist = (s + 1) * (1 - 2 * dr)
            project(chip_at(lax.rem(ring - dist + 2 * n_chip, n_chip)))
            return 0

        lax.fori_loop(0, 2, both, 0)
        return 0

    lax.fori_loop(0, half - 1, gather_step, 0)
    loads[1].wait()
    swaps[2].wait_recv()
    start_own(1)
    gys_copy = pltpu.make_async_copy(buf.at[1, chip], gys_ref, out_sem.at[1])
    gys_copy.start()
    last_stage(0)
    project(slot_at(0, half))
    hall_copy = pltpu.make_async_copy(buf.at[0], hall_ref, out_sem.at[0])
    hall_copy.start()
    for hs in heads:
        vt_ref[hs, :] = v_ref[:, hs].T
    ssq_copy = to_peers(ssq, ssq_all, qs_sem, qr_sem)
    each_peer(lambda p: ssq_copy(p, chip).start())
    ssq_all[chip] = ssq[...]
    each_peer(lambda p: ssq_copy(p, p).wait_recv())
    total = ssq_all[0]
    for p in range(1, n_chip):
        total = total + ssq_all[p]
    inv_ref[...] = lax.rsqrt(total / dim + NORM_EPS)

    def finish_qk(p, _):
        ts = pl.ds(pl.multiple_of(p * rows, rows), rows)
        for idx, (hat_ref, out) in enumerate(((qh_ref, q_ref), (kh_ref, k_ref))):
            inv = column(inv_ref[pl.ds(idx * n_chip + p, 1), :])
            for hs in heads:
                hat = hat_ref[ts, hs] * inv
                hat_ref[ts, hs] = hat
                u = hat * g_ref[idx:idx + 1, hs]
                out[ts, hs] = (u * c_ref[ts, :] + half_roll(u) * s_ref[ts, :]).astype(BF)
        return 0

    lax.fori_loop(0, n_chip, finish_qk, 0)
    flush((xs_ref, xs_out), (c_ref, c_out), (s_ref, s_out), (v_ref, v_out))

    blk = FWD_BLOCK
    scale = HEAD_DIM ** -0.5 * LOG2E
    causal = lax.broadcasted_iota(jnp.int32, (blk, blk), 0) <= lax.broadcasted_iota(jnp.int32, (blk, blk), 1)

    def attend(t, _):
        j = flip(chip // 2, t, 2)
        qs = pl.ds(pl.multiple_of(j * blk, blk), blk)
        qb = [q_ref[qs, hs] for hs in heads]

        def tile(i, carry, diag):
            ks = pl.ds(pl.multiple_of(i * blk, blk), blk)
            out = []
            for h, hs in enumerate(heads):
                m, l, acc = carry[h]
                s = mm32_nt(k_ref[ks, hs], qb[h])
                if diag:
                    s = jnp.where(causal, s, NEG_BIG)
                mn = jnp.maximum(m, jnp.max(s, axis=0, keepdims=True))
                al = jnp.exp2((m - mn) * scale)
                p = jnp.exp2((s - mn) * scale)
                l = al * l + jnp.sum(p, axis=0, keepdims=True)
                out.append((mn, l, al * acc + mm32(vt_ref[hs, ks], p.astype(BF))))
            return tuple(out)

        st = tuple((jnp.full((1, blk), NEG_BIG, F32), jnp.zeros((1, blk), F32), jnp.zeros((HEAD_DIM, blk), F32)) for _ in heads)
        st = lax.fori_loop(0, j, lambda i, cr: tile(i, cr, False), st)
        st = tile(j, st, True)
        for h, hs in enumerate(heads):
            m, l, acc = st[h]
            ot = acc / l
            ot_ref[hs, qs] = ot
            att_ref[qs, hs] = ot.T.astype(BF)
            lse_ref[h:h + 1, qs] = m * scale + jnp.log2(l)
        return 0

    def use_gy(p):
        ts = pl.ds(pl.multiple_of(p * rows, rows), rows)
        gy = buf[1, p]
        datt_ref[ts, :] = mm32_nt(gy, wrow_ref[...]).astype(BF)
        dwo_ref[...] += mm32(ot_ref[:, ts].astype(BF), gy)

    n_att = n_chip * rows // blk
    lax.fori_loop(0, n_att // 2, attend, 0)
    stage(1, 0)
    lax.fori_loop(n_att // 2, n_att, attend, 0)

    flush((q_ref, q_out), (k_ref, k_out), (qh_ref, qh_out), (kh_ref, kh_out), (ot_ref, ot_out), (att_ref, att_out))

    def raw_of(w, out):
        def load(m, slot):
            return pltpu.make_async_copy(w.at[:, pl.ds(pl.multiple_of(m * cols, cols), cols)], wbuf.at[slot], w_sem.at[slot])

        load(0, 0).start()

        def step(m, _):
            slot = lax.rem(m, 2)
            load(m, slot).wait()

            @pl.when(m + 1 < n_chip)
            def _():
                load(m + 1, 1 - slot).start()
            out[:, pl.ds(pl.multiple_of(m * cols, cols), cols)] = mm32(buf[0, chip], wbuf[slot])
            return 0

        lax.fori_loop(0, n_chip, step, 0)

    raw_of(wq_ref, qr_ref)
    raw_of(wk_ref, kr_ref)
    stage(1, 1)
    dwo_ref[...] = jnp.zeros_like(dwo_ref)
    flush((qr_ref, qr_out), (kr_ref, kr_out))

    def use_ring(n, _):
        dist = ((n + 1) // 2) * (2 * lax.rem(n, 2) - 1)
        use_gy(chip_at(lax.rem(ring - dist + 2 * n_chip, n_chip)))
        return 0

    lax.fori_loop(0, n_chip - 3, use_ring, 0)
    stage(1, half - 2)
    lax.fori_loop(n_chip - 3, n_chip - 1, use_ring, 0)
    last_stage(1)
    use_gy(slot_at(0, half))

    each_peer(lambda p: pos_copy(p, chip).wait_send())
    each_peer(lambda p: ssq_copy(p, chip).wait_send())
    for sw in swaps:
        sw.wait_send()
    drain(0)
    drain(1)
    hall_copy.wait()
    gys_copy.wait()
    for copy in pending:
        copy.wait()


def back_kernel(q_ref, k_ref, v_ref, do_ref, ot_ref, lse_ref, g_ref, gt_ref, inv_ref,
                hall_ref, qh_hbm, kh_hbm, c_hbm, s_hbm, qr_hbm, kr_hbm, wq_ref, wk_ref, wv_ref, dwo_ref, wo_ref, at_hbm, x_hbm, gy_hbm,
                dwq_ref, dwk_ref, dwv_ref, y_ref, gx_ref, dwo_out, dg_out, dgn_out,
                dq_ref, dk_ref, dv_ref, dka_ref, dva_ref, kt_ref, qh_ref, kh_ref, c_ref, s_ref, qr_ref, kr_ref,
                tok, pairs, pair_in, dt_ref, hblk, wblk, dwo_in, row_ref, row_all,
                dhid_ref, dg_ref, at_ref, x_ref, gy_ref, ys_ref, gxs_ref, dgp, dgp_in, gpart, gpair_in, gsel, gsel_in,
                as_sem, ar_sem, sw_sem, gs_sem, gr_sem, load_sem, h_sem, w_sem, xs_sem, xr_sem, ps_sem, pr_sem, rs_sem, rr_sem, own_sem, do_sem):
    me = lax.axis_index('sp')
    chip, core = me // 2, lax.rem(me, 2)
    n, cols = q_ref.shape
    rows, dim = qr_ref.shape
    n_chip = n // rows
    partner = {'sp': me + 1 - 2 * core}
    heads = [slice(lo, lo + HEAD_DIM) for lo in range(0, cols, HEAD_DIM)]
    own_rows = pl.ds(pl.multiple_of(chip * rows, rows), rows)
    own_cols = pl.ds(pl.multiple_of(chip * cols, cols), cols)
    MESH = pl.DeviceIdType.MESH

    def dev(p):
        return {'sp': 2 * p + core}

    def each_peer(fn):
        for step in range(1, n_chip):
            fn(flip(chip, step))

    sides = ((qh_hbm, qh_ref), (kh_hbm, kh_ref), (c_hbm, c_ref), (s_hbm, s_ref), (qr_hbm, qr_ref), (kr_hbm, kr_ref), (dwo_ref.at[core], dwo_out), (at_hbm.at[own_rows], at_ref.at[:, own_cols]), (x_hbm, x_ref), (gy_hbm, gy_ref))
    loads = [pltpu.make_async_copy(src, dst, load_sem.at[i]) for i, (src, dst) in enumerate(sides)]
    for ld in loads:
        ld.start()

    def load_h(p, slot):
        return pltpu.make_async_copy(hall_ref.at[:, pl.ds(pl.multiple_of(p * cols, cols), cols)], hblk.at[slot], h_sem.at[slot])

    def load_o(m, slot):
        return pltpu.make_async_copy(wo_ref.at[pl.ds(pl.multiple_of(m * cols, cols), cols)], wblk.at[slot, 0], w_sem.at[slot, 0])

    load_h(chip, 0).start()
    load_o(0, 0).start()
    barrier = pltpu.get_barrier_semaphore()
    each_peer(lambda p: pl.semaphore_signal(barrier, inc=1, device_id=dev(p), device_id_type=MESH))
    pl.semaphore_signal(barrier, inc=1, device_id=partner, device_id_type=MESH)
    pl.semaphore_wait(barrier, n_chip)

    dwo_copy = pltpu.make_async_remote_copy(
        src_ref=dwo_ref.at[1 - core], dst_ref=dwo_in, send_sem=do_sem.at[0], recv_sem=do_sem.at[1], device_id=partner, device_id_type=MESH)
    dwo_copy.start()

    def at_copy(p, owner):
        src = at_hbm.at[pl.ds(pl.multiple_of(p * rows, rows), rows)]
        dst = at_ref.at[:, pl.ds(pl.multiple_of(owner * cols, cols), cols)]
        return pltpu.make_async_remote_copy(src_ref=src, dst_ref=dst, send_sem=as_sem.at[p], recv_sem=ar_sem.at[owner], device_id=dev(p), device_id_type=MESH)

    each_peer(lambda p: at_copy(p, chip).start())

    def to_partner(src, dst, i):
        return pltpu.make_async_remote_copy(src_ref=src, dst_ref=dst, send_sem=sw_sem.at[0, i], recv_sem=sw_sem.at[1, i], device_id=partner, device_id_type=MESH)

    y_swap = to_partner(ys_ref.at[1 - core], y_ref.at[core], 0)
    gx_swap = to_partner(gxs_ref.at[1 - core], gx_ref.at[core], 1)
    dg_swap = to_partner(dgp.at[1 - core], dgp_in, 2)
    gn_swap = to_partner(gpart.at[1 - core], gpair_in, 3)
    y_own = pltpu.make_async_copy(ys_ref.at[core], y_ref.at[core], sw_sem.at[0, 4])
    gx_own = pltpu.make_async_copy(gxs_ref.at[core], gx_ref.at[core], sw_sem.at[1, 4])

    def tok_copy(t, p, owner):
        src = (dq_ref, dk_ref, dv_ref)[t].at[pl.ds(pl.multiple_of(p * rows, rows), rows)]
        dst = tok.at[t, :, pl.ds(pl.multiple_of(owner * cols, cols), cols)]
        return pltpu.make_async_remote_copy(src_ref=src, dst_ref=dst, send_sem=xs_sem.at[t, p], recv_sem=xr_sem.at[t, owner], device_id=dev(p), device_id_type=MESH)

    blk = BWD_BLOCK
    span = blk // rows
    n_blk = n // blk
    sc = HEAD_DIM ** -0.5
    scale = sc * LOG2E
    for hs in heads:
        kt_ref[hs, :] = k_ref[:, hs].T
    dka_ref[...] = jnp.zeros_like(dka_ref)
    dva_ref[...] = jnp.zeros_like(dva_ref)
    causal = lax.broadcasted_iota(jnp.int32, (blk, blk), 0) <= lax.broadcasted_iota(jnp.int32, (blk, blk), 1)

    def send_dq(j):
        for u in range(span):
            p = j * span + u

            @pl.when(p != chip)
            def _():
                tok_copy(0, p, chip).start()

    def q_step(j, _):
        qs = pl.ds(pl.multiple_of(j * blk, blk), blk)
        qb = [q_ref[qs, hs] for hs in heads]
        dob = [do_ref[qs, hs] for hs in heads]
        lse = [lse_ref[h:h + 1, qs] for h in range(len(heads))]
        dl = [jnp.sum(ot_ref[hs, qs] * dob[h].astype(F32).T, axis=0, keepdims=True) for h, hs in enumerate(heads)]

        def tile(i, carry, diag):
            ks = pl.ds(pl.multiple_of(i * blk, blk), blk)
            out = []
            for h, hs in enumerate(heads):
                s = mm32_nt(k_ref[ks, hs], qb[h])
                dp = mm32_nt(v_ref[ks, hs], dob[h])
                p = jnp.exp2(s * scale - lse[h])
                if diag:
                    p = jnp.where(causal, p, 0.0)
                ds = (p * (dp - dl[h])).astype(BF)
                dva_ref[ks, hs] += mm32(p.astype(BF), dob[h])
                dka_ref[ks, hs] += mm32(ds, qb[h])
                out.append(carry[h] + mm32(kt_ref[hs, ks], ds))
            return tuple(out)

        st = tuple(jnp.zeros((HEAD_DIM, blk), F32) for _ in heads)
        st = lax.fori_loop(0, j, lambda i, cr: tile(i, cr, False), st)
        st = tile(j, st, True)
        for h, hs in enumerate(heads):
            dq_ref[qs, hs] = (st[h] * sc).T.astype(BF)

        @pl.when(j > 0)
        def _():
            send_dq(j - 1)
        return 0

    lax.fori_loop(0, n_blk, q_step, 0)
    dk_ref[...] = (dka_ref[...] * sc).astype(BF)
    dv_ref[...] = dva_ref[...].astype(BF)
    send_dq(n_blk - 1)
    for t, src in enumerate((dq_ref, dk_ref, dv_ref)):
        tok[t, :, own_cols] = src[own_rows, :]
    each_peer(lambda p: tok_copy(1, p, chip).start())
    for step in range(1, EARLY):
        tok_copy(2, flip(chip, step), chip).start()

    def pair_copy(w, p):
        return pltpu.make_async_remote_copy(
            src_ref=pairs.at[w, p, 1 - core], dst_ref=pair_in.at[w, p], send_sem=ps_sem.at[w, p], recv_sem=pr_sem.at[w, p], device_id=partner, device_id_type=MESH)

    grads = (dwq_ref, dwk_ref, dwv_ref)

    def dw_copy(w, p, owner):
        dst = grads[w].at[:, pl.ds(pl.multiple_of(owner * cols, cols), cols)]
        return pltpu.make_async_remote_copy(src_ref=pairs.at[w, p, core], dst_ref=dst, send_sem=xs_sem.at[3 + w, p], recv_sem=xr_sem.at[3 + w, owner], device_id=dev(p), device_id_type=MESH)

    def own_copy(w):
        return pltpu.make_async_copy(pairs.at[w, chip, core], grads[w].at[:, own_cols], own_sem.at[w])

    def partial(w, slot_t, h, p):
        dw = mm32(dt_ref[slot_t], h).T
        pairs[w, p, 0] = dw[:rows // 2]
        pairs[w, p, 1] = dw[rows // 2:]

    def merge(w, p):
        pair_copy(w, p).wait_recv()
        pairs[w, p, core] += pair_in[w, p]

    def send_dw(w, p):
        @pl.when(p != chip)
        def _():
            dw_copy(w, p, chip).start()

        @pl.when(p == chip)
        def _():
            own_copy(w).start()

    def each_h(ws, tail_fn):
        def step(i, _):
            p = flip(chip, i)
            slot = lax.rem(i, 2)
            load_h(p, slot).wait()

            @pl.when(i + 1 < n_chip)
            def _():
                load_h(flip(chip, i + 1), 1 - slot).start()
            for w, slot_t in ws:
                partial(w, slot_t, hblk[slot], p)
            tail_fn(i)
            for w, _ in ws:
                pair_copy(w, p).start()
            return 0

        lax.fori_loop(0, n_chip, step, 0)

    dt_ref[0] = dv_ref[...].T
    each_h(((2, 0),), lambda p: None)
    load_h(chip, 0).start()
    for ld in loads:
        ld.wait()

    each_peer(lambda p: at_copy(p, p).wait_recv())
    dhid_ref[...] = x_ref[...].astype(F32)

    def y_step(m, _):
        slot = lax.rem(m, 2)
        load_o(m, slot).wait()

        @pl.when(m + 1 < n_chip)
        def _():
            load_o(m + 1, 1 - slot).start()
        dhid_ref[...] += mm32(at_ref[:, pl.ds(pl.multiple_of(m * cols, cols), cols)], wblk[slot, 0])
        return 0

    lax.fori_loop(0, n_chip, y_step, 0)
    half = rows // 2
    for u in range(2):
        ys_ref[u] = dhid_ref[u * half:(u + 1) * half, :].astype(BF)

    hats = ((qr_ref, 0), (kr_ref, 1))
    row_ref[...] = jnp.zeros_like(row_ref)
    inv_t = [column(inv_ref[pl.ds(idx * n_chip + chip, 1), :]) for idx in range(2)]
    c_t, s_t = c_ref[own_rows, :], s_ref[own_rows, :]

    def normed(idx, hs):
        d = tok[idx, :, hs].astype(F32)
        return (d * c_t - half_roll(d) * s_t) * gt_ref[idx:idx + 1, hs]

    row_cols = []
    for raw_ref, idx in hats:
        each_peer(lambda p: tok_copy(idx, p, p).wait_recv())
        acc = jnp.zeros((rows, HEAD_DIM), F32)
        for lo in range(0, dim, HEAD_DIM):
            hs = slice(lo, lo + HEAD_DIM)
            acc += normed(idx, hs) * (raw_ref[:, hs] * inv_t[idx])
        row = jnp.sum(acc, axis=1, keepdims=True) / dim
        row_ref[idx:idx + 1, :] = as_row(row)
        row_cols.append(row)

    y_swap.start()
    y_own.start()

    def row_copy(p, owner):
        return pltpu.make_async_remote_copy(src_ref=row_ref, dst_ref=row_all.at[owner], send_sem=rs_sem.at[p], recv_sem=rr_sem.at[owner], device_id=dev(p), device_id_type=MESH)

    for raw_ref, idx in hats:
        for lo in range(0, dim, HEAD_DIM):
            hs = slice(lo, lo + HEAD_DIM)
            tok[idx, :, hs] = (inv_t[idx] * (normed(idx, hs) - raw_ref[:, hs] * inv_t[idx] * row_cols[idx])).astype(BF)
        if idx == 0:
            each_peer(lambda p: row_copy(p, chip).start())
            for step in range(EARLY, n_chip):
                tok_copy(2, flip(chip, step), chip).start()
            row_all[chip] = row_ref[...]

    def merge_v(p, _):
        merge(2, p)
        return 0

    def send_v(i, _):
        send_dw(2, flip(chip, i))
        return 0

    lax.fori_loop(0, n_chip, merge_v, 0)

    def load_w(m, slot):
        return [pltpu.make_async_copy(w.at[pl.ds(pl.multiple_of(m * cols, cols), cols)], wblk.at[slot, i], w_sem.at[slot, i]) for i, w in enumerate((wq_ref, wk_ref, wv_ref))]

    for ld in load_w(0, 0):
        ld.start()
    lax.fori_loop(0, n_chip, send_v, 0)
    each_peer(lambda p: row_copy(p, p).wait_recv())

    dg_ref[...] = jnp.zeros_like(dg_ref)

    def head_step(p, _):
        ts = pl.ds(pl.multiple_of(p * rows, rows), rows)
        for idx, (d_ref, hat_ref) in enumerate(((dq_ref, qh_ref), (dk_ref, kh_ref))):
            inv = column(inv_ref[pl.ds(idx * n_chip + p, 1), :])
            row = column(row_all[p, idx:idx + 1, :])
            for hs in heads:
                d = d_ref[ts, hs].astype(F32)
                rot = d * c_ref[ts, :] - half_roll(d) * s_ref[ts, :]
                hat = hat_ref[ts, hs]
                raw = inv * (rot * g_ref[idx:idx + 1, hs] - hat * row)
                dt_ref[idx, hs, ts] = raw.astype(BF).T
                dg_ref[idx:idx + 1, hs] += jnp.sum(rot * hat, axis=0, keepdims=True)
        return 0

    lax.fori_loop(0, n_chip, head_step, 0)
    dgp[...] = jnp.zeros_like(dgp)
    for u in range(2):
        dgp[u, 0:2, :] = dg_ref[0:2, u * half:(u + 1) * half]

    def lagged(i):
        @pl.when(i > 0)
        def _():
            for w in range(2):
                merge(w, flip(chip, i - 1))

        @pl.when(i > 1)
        def _():
            for w in range(2):
                send_dw(w, flip(chip, i - 2))

    each_h(((0, 0), (1, 1)), lagged)
    for w in range(2):
        send_dw(w, flip(chip, n_chip - 2))
        merge(w, flip(chip, n_chip - 1))
    dwo_copy.wait_recv()
    dwo_out[...] += dwo_in[...]
    for w in range(2):
        send_dw(w, flip(chip, n_chip - 1))
    dg_swap.start()

    each_peer(lambda p: tok_copy(2, p, p).wait_recv())

    def hid_step(m, _):
        slot = lax.rem(m, 2)
        for ld in load_w(m, slot):
            ld.wait()

        @pl.when(m + 1 < n_chip)
        def _():
            for ld in load_w(m + 1, 1 - slot):
                ld.start()
        out = pl.ds(pl.multiple_of(m * cols, cols), cols)
        dhid_ref[:, out] = mm32_nt(tok[0], wblk[slot, 0]) + mm32_nt(tok[1], wblk[slot, 1]) + mm32_nt(tok[2], wblk[slot, 2])
        return 0

    lax.fori_loop(0, n_chip, hid_step, 0)

    blocks = [slice(lo, lo + HEAD_DIM) for lo in range(0, dim, HEAD_DIM)]
    acc = jnp.zeros((rows, HEAD_DIM), F32)
    dot = jnp.zeros((rows, HEAD_DIM), F32)
    for hs in blocks:
        x = x_ref[:, hs].astype(F32)
        acc += x * x
        dot += x * dhid_ref[:, hs] * gt_ref[2:3, hs]
    x_inv = lax.rsqrt(jnp.sum(acc, axis=1, keepdims=True) / dim + NORM_EPS)
    mean = jnp.sum(dot, axis=1, keepdims=True) * x_inv / dim
    gpart[...] = jnp.zeros_like(gpart)
    for i, hs in enumerate(blocks):
        x_hat = x_ref[:, hs].astype(F32) * x_inv
        d = dhid_ref[:, hs]
        gx = (gy_ref[:, hs].astype(F32) + x_inv * (d * gt_ref[2:3, hs] - x_hat * mean)).astype(BF)
        gxs_ref[0, :, hs] = gx[:half]
        gxs_ref[1, :, hs] = gx[half:]
        gpart[i % 2, i // 2, 0:1, :] = jnp.sum(d * x_hat, axis=0, keepdims=True)
    gn_swap.start()
    gx_swap.start()
    gx_own.start()
    dg_swap.wait_recv()
    dg_out[...] = dgp[core] + dgp_in[...]
    gn_swap.wait_recv()
    gsel[...] = gpart[core] + gpair_in[...]

    def gn_copy(p, owner):
        return pltpu.make_async_remote_copy(src_ref=gsel.at[p], dst_ref=gsel_in.at[owner], send_sem=gs_sem.at[p], recv_sem=gr_sem.at[owner], device_id=dev(p), device_id_type=MESH)

    each_peer(lambda p: gn_copy(p, chip).start())
    gsel_in[chip] = gsel[chip]
    each_peer(lambda p: gn_copy(p, p).wait_recv())
    total = gsel_in[0]
    for p in range(1, n_chip):
        total = total + gsel_in[p]
    dgn_out[...] = total
    each_peer(lambda p: gn_copy(p, chip).wait_send())
    for sw in (y_swap, gx_swap):
        sw.wait_recv()
    for sw in (y_swap, gx_swap, dg_swap, gn_swap):
        sw.wait_send()
    y_own.wait()
    gx_own.wait()

    for w in range(3):
        each_peer(lambda p: dw_copy(w, p, p).wait_recv())
        each_peer(lambda p: dw_copy(w, p, chip).wait_send())
        each_peer(lambda p: tok_copy(w, p, chip).wait_send())
        own_copy(w).wait()
        for p in range(n_chip):
            pair_copy(w, p).wait_send()
    each_peer(lambda p: row_copy(p, chip).wait_send())
    each_peer(lambda p: at_copy(p, chip).wait_send())
    dwo_copy.wait_send()


VM = pl.BlockSpec(memory_space=pltpu.VMEM)


def mm32(a, b):
    return jnp.dot(a, b, preferred_element_type=F32)


def mm32_nt(a, b):
    return lax.dot_general(a, b, NT, preferred_element_type=F32)


def front(x, gy, w_query, w_key, w_value, w_out, pos, gains_h, gains, freq, n_chip):
    loc, dim = x.shape[1:]
    rows = 2 * loc
    cols = gains_h.shape[1]
    n = n_chip * rows
    heads = cols // HEAD_DIM
    any_spec = pl.BlockSpec(memory_space=pl.ANY)
    half = n_chip // 2
    dma, vmem = pltpu.SemaphoreType.DMA, pltpu.VMEM
    outs = [((n_chip, rows, dim), BF), ((n, cols), BF), ((n, cols), BF), ((n, cols), BF), ((n, cols), F32), ((n, cols), F32), ((cols, n), F32), ((heads, n), F32),
            ((n, cols), BF), ((n, cols), BF), ((cols, dim), F32), ((n, HEAD_DIM), F32), ((n, HEAD_DIM), F32), ((2 * n_chip, rows), F32), ((rows, dim), F32), ((rows, dim), F32),
            ((2, loc, dim), BF), ((rows, dim), BF)]
    return pl.pallas_call(
        front_kernel, name='front', out_shape=tuple(jax.ShapeDtypeStruct(s, d) for s, d in outs),
        in_specs=[any_spec] * 6 + [VM] * 4, out_specs=(any_spec,) * 7 + (VM,) + (any_spec,) + (VM,) * 2 + (any_spec,) * 2 + (VM,) + (any_spec,) * 4,
        scratch_shapes=[vmem(*outs[i]) for i in (1, 2, 3, 4, 5, 6, 11, 12, 14, 15, 16)] + [dma((12,)),
            vmem((2, n_chip, rows, dim), BF), vmem((3, dim, cols), BF), vmem((cols, dim), BF), vmem((n, cols), BF), vmem((cols, n), BF),
            vmem((n_chip, 2, 8, loc), F32), vmem((2 * n_chip, rows), F32), vmem((n_chip, 2 * n_chip, rows), F32), vmem((2, dim, cols), BF),
            dma((2,)), dma((6,)), dma((2, 3)), dma((2,)), dma((2, 2, half, CHUNKS)), dma((2, 2, half, CHUNKS)),
            dma((n_chip,)), dma((n_chip,)), dma((n_chip,)), dma((n_chip,))],
        compiler_params=pltpu.CompilerParams(collective_id=0, has_side_effects=True, vmem_limit_bytes=67043328),
        cost_estimate=pl.CostEstimate(flops=400 * n * dim * cols, bytes_accessed=40 * n * dim, transcendentals=n * n * heads // 2),
    )(x, gy, w_query, w_key, w_value, w_out, pos, gains_h, gains, freq)


def back(q, k, v, d_att, att_t, lse, gains_h, gains, inv, hid, qh, kh, cos_a, sin_a, q_raw, k_raw, w_query, w_key, w_value, dwo, w_out, att, x, gy):
    n, cols = q.shape
    rows, dim = q_raw.shape
    n_chip = n // rows
    any_spec = pl.BlockSpec(memory_space=pl.ANY)
    dma = pltpu.SemaphoreType.DMA
    grad = jax.ShapeDtypeStruct((rows // 2, dim), F32)
    seq = jax.ShapeDtypeStruct((2, rows // 2, dim), BF)
    small = jax.ShapeDtypeStruct((8, cols // 2), F32)
    tile = (n_chip, 8, cols // 2)
    vmem = pltpu.VMEM
    return pl.pallas_call(
        back_kernel, name='back', in_specs=[VM] * 9 + [any_spec] * 15, out_specs=(any_spec,) * 5 + (VM,) * 3,
        out_shape=(grad,) * 3 + (seq, seq, grad, small, small),
        scratch_shapes=[
            vmem((n, cols), BF), vmem((n, cols), BF), vmem((n, cols), BF), vmem((n, cols), F32), vmem((n, cols), F32), vmem((cols, n), BF),
            vmem((n, cols), F32), vmem((n, cols), F32), vmem((n, HEAD_DIM), F32), vmem((n, HEAD_DIM), F32), vmem((rows, dim), F32), vmem((rows, dim), F32),
            vmem((3, rows, dim), BF), vmem((3, n_chip, 2, rows // 2, cols), F32), vmem((3, n_chip, rows // 2, cols), F32),
            vmem((2, cols, n), BF), vmem((2, n, cols), BF), vmem((2, 3, cols, dim), BF), vmem((rows // 2, dim), F32),
            vmem((8, rows), F32), vmem((n_chip, 8, rows), F32),
            vmem((rows, dim), F32), vmem((8, cols), F32), vmem((rows, dim), BF), vmem((rows, dim), BF), vmem((rows, dim), BF), vmem((2, rows // 2, dim), BF), vmem((2, rows // 2, dim), BF),
            vmem((2, 8, cols // 2), F32), vmem((8, cols // 2), F32), vmem((2,) + tile, F32), vmem(tile, F32), vmem(tile, F32), vmem(tile, F32),
            dma((n_chip,)), dma((n_chip,)), dma((2, 5)), dma((n_chip,)), dma((n_chip,)), dma((10,)), dma((2,)), dma((2, 3)), dma((6, n_chip)), dma((6, n_chip)), dma((3, n_chip)), dma((3, n_chip)),
            dma((n_chip,)), dma((n_chip,)), dma((3,)), dma((2,))],
        compiler_params=pltpu.CompilerParams(collective_id=1, has_side_effects=True, vmem_limit_bytes=67043328),
        cost_estimate=pl.CostEstimate(flops=400 * n * dim * cols, bytes_accessed=40 * n * dim, transcendentals=n * n),
    )(q, k, v, d_att, att_t, lse, gains_h, gains, inv, hid, qh, kh, cos_a, sin_a, q_raw, k_raw, w_query, w_key, w_value, dwo, w_out, att, x, gy)


def solution(mesh):
    n_chip = mesh.shape['sp'] // 2

    def device_step(x_loc, gy_loc, positions, g_norm, w_query, w_key, w_value, w_out, g_query, g_key):
        chip = lax.axis_index('sp') // 2
        loc, dim = x_loc.shape[1], x_loc.shape[2]
        rows = 2 * loc
        cols = dim // n_chip
        pos = jnp.broadcast_to(positions.astype(F32)[:, None, :], (2, 8, loc))
        gains = jnp.stack([g_query, g_key, g_norm]).astype(F32)
        gains_h = lax.dynamic_slice_in_dim(gains, chip * cols, cols, axis=1)
        hid_all, q, k, v, qh_hat, kh_hat, att_t, lse, att, d_att, dwo, cos_a, sin_a, inv_all, q_raw, k_raw, x_sw, gy_sw = front(
            x_loc, gy_loc, w_query, w_key, w_value, w_out, pos, gains_h, gains, rope_rows(), n_chip)
        dwq, dwk, dwv, y, grad_x, dwo, dg, dgn = back(
            q, k, v, d_att, att_t, lse, gains_h, gains, inv_all, hid_all.reshape(n_chip * rows, dim), qh_hat, kh_hat, cos_a, sin_a,
            q_raw, k_raw, w_query, w_key, w_value, dwo.reshape(2, loc, dim), w_out, att, x_sw.reshape(rows, dim), gy_sw)
        return y, grad_x, dgn[0], dwq, dwk, dwv, dwo, dg[0], dg[1]

    seq_spec = P('dp', 'sp', None)
    mat_rep = P(None, None)
    vec_rep = P(None)
    row_spec = P(('dp', 'sp'), None)
    vec_spec = P(('dp', 'sp'))
    return jax.shard_map(device_step, mesh=mesh, in_specs=(seq_spec, seq_spec, P('dp', 'sp'), vec_rep, mat_rep, mat_rep, mat_rep, mat_rep, vec_rep, vec_rep), out_specs=(seq_spec, seq_spec, vec_spec, row_spec, row_spec, row_spec, row_spec, vec_spec, vec_spec), check_vma=False)
```

```python
import jax
import numpy as np
import jax.numpy as jnp
from jax import lax
from jax.experimental import pallas as pl
from jax.experimental.pallas import tpu as pltpu
from jax.sharding import PartitionSpec as P

HEAD_DIM = 128
NORM_EPS = 1e-5
ROPE_BASE = 10000.0
NEG_BIG = -1e30
LOG2E = 1.4426950408889634
FWD_BLOCK = 512
CHUNKS = 4
EARLY = 3
BWD_BLOCK = 512
F32, BF = jnp.float32, jnp.bfloat16
NT = (((1,), (1,)), ((), ()))


def rope_rows():
    half = HEAD_DIM // 2
    inv_freq = ROPE_BASE ** (-np.arange(half) * (2.0 / HEAD_DIM))
    sign = np.ones(half)
    return jnp.asarray(np.stack([np.concatenate([inv_freq, inv_freq]), np.concatenate([-sign, sign])]).astype(np.float32))


def fill_gains(ins, gt_ref, g_ref, own_cols):
    for i, ref in enumerate(ins):
        gt_ref[i:i + 1, :] = ref[...].astype(F32).reshape(1, -1)
    g_ref[...] = gt_ref[0:2, own_cols]


def column(row):
    return jnp.broadcast_to(row, (HEAD_DIM, row.shape[1])).T


def as_row(col):
    return jnp.broadcast_to(col, (col.shape[0], HEAD_DIM)).T[0:1, :]


def half_roll(u):
    return pltpu.roll(u, HEAD_DIM // 2, 1)


def flip(a, b, bits=3):
    out = 0
    for i in range(bits):
        x, y = (a // 2 ** i) % 2, (b // 2 ** i) % 2
        out = out + 2 ** i * (x + y - 2 * x * y)
    return out


def front_kernel(x_ref, gy_ref, wq_ref, wk_ref, wv_ref, wo_ref, pos_in, gq_in, gk_in, gn_in, f_ref,
                 hall_ref, q_out, k_out, v_out, qh_out, kh_out, ot_out, lse_ref, att_out, datt_ref, dwo_ref, c_out, s_out, inv_ref, qr_out, kr_out, xs_out, gys_ref,
                 q_ref, k_ref, v_ref, qh_ref, kh_ref, ot_ref, c_ref, s_ref, qr_ref, kr_ref, xs_ref, flush_sem,
                 pos_ref, g_ref, gt_ref, buf, w_ref, wrow_ref, att_ref, vt_ref, pos_all, ssq, ssq_all, wbuf,
                 w_sem, load_sem, swap_sem, out_sem, ssem, rsem, ps_sem, pr_sem, qs_sem, qr_sem):
    me = lax.axis_index('sp')
    chip, core = me // 2, lax.rem(me, 2)
    n_chip, rows, dim = hall_ref.shape
    cols = q_ref.shape[1]
    part = rows // CHUNKS
    half = n_chip // 2
    heads = [slice(lo, lo + HEAD_DIM) for lo in range(0, cols, HEAD_DIM)]

    def spot(p):
        z, y = p // 2, lax.rem(p, 2)
        return z + y * (n_chip - 1 - 2 * z)

    def chip_at(r):
        y = r // half
        return 2 * (r + y * (n_chip - 1 - 2 * r)) + y

    ring = spot(chip)

    def slot_at(dr, dist):
        step = dist if dr == 0 else -dist
        return chip_at(lax.rem(ring - step + 2 * n_chip, n_chip))

    def dev(p):
        return {'sp': 2 * p + core}

    right = dev(slot_at(1, 1))
    left = dev(slot_at(0, 1))

    def hop(t, dr, s, c, dist):
        view = buf.at[t, slot_at(dr, dist), pl.ds(c * part, part)]
        return pltpu.make_async_remote_copy(
            src_ref=view, dst_ref=view, send_sem=ssem.at[t, dr, s, c], recv_sem=rsem.at[t, dr, s, c],
            device_id=right if dr == 0 else left, device_id_type=pl.DeviceIdType.MESH)

    def in_half(dr, c):
        return (c < CHUNKS // 2) == (dr == 0)

    def start_own(t):
        for c in range(CHUNKS):
            for dr in range(2):
                hop(t, dr, 0, c, 0).start()

    def stage(t, s):
        for c in range(CHUNKS):
            for dr in range(2):
                hop(t, dr, s, c, s + 1).wait_recv()
                if in_half(dr, c):
                    hop(t, dr, s + 1, c, s + 1).start()
                else:
                    @pl.when(s < half - 2)
                    def _():
                        hop(t, dr, s + 1, c, s + 1).start()

    def last_stage(t):
        for c in range(CHUNKS):
            for dr in range(2):
                if in_half(dr, c):
                    hop(t, dr, half - 1, c, half).wait_recv()

    def drain(t):
        for s in range(half):
            for c in range(CHUNKS):
                for dr in range(2):
                    if s < half - 1 or in_half(dr, c):
                        hop(t, dr, s, c, s).wait_send()

    def to_peers(src, dst, s_sem, r_sem):
        def make(p, owner):
            return pltpu.make_async_remote_copy(
                src_ref=src, dst_ref=dst.at[owner], send_sem=s_sem.at[p], recv_sem=r_sem.at[owner],
                device_id=dev(p), device_id_type=pl.DeviceIdType.MESH)
        return make

    def each_peer(fn):
        for step in range(1, n_chip):
            fn(flip(chip, step))

    partner = {'sp': me + 1 - 2 * core}
    own_cols = pl.ds(pl.multiple_of(chip * cols, cols), cols)
    gy_own = buf.at[1, chip, pl.ds(pl.multiple_of(core * (rows // 2), rows // 2), rows // 2)]
    local = [(x_ref.at[core], xs_ref.at[core]), (gy_ref.at[core], gy_own)]
    local += [(w.at[:, own_cols], w_ref.at[i]) for i, w in enumerate((wq_ref, wk_ref, wv_ref))] + [(wo_ref.at[own_cols], wrow_ref)]
    loads = [pltpu.make_async_copy(src, dst, load_sem.at[i]) for i, (src, dst) in enumerate(local)]
    for ld in loads:
        ld.start()
    fill_gains((gq_in, gk_in, gn_in), gt_ref, g_ref, own_cols)
    for u in range(2):
        pos_ref[u] = jnp.broadcast_to(pos_in[u:u + 1, :].astype(F32), pos_ref.shape[1:])
    barrier = pltpu.get_barrier_semaphore()
    each_peer(lambda p: pl.semaphore_signal(barrier, inc=1, device_id=dev(p), device_id_type=pl.DeviceIdType.MESH))
    pl.semaphore_signal(barrier, inc=1, device_id=partner, device_id_type=pl.DeviceIdType.MESH)
    pl.semaphore_wait(barrier, n_chip)

    pending = []

    def flush(*pairs):
        for src, dst in pairs:
            copy = pltpu.make_async_copy(src, dst, flush_sem.at[len(pending)])
            copy.start()
            pending.append(copy)

    swaps = [pltpu.make_async_remote_copy(
        src_ref=src, dst_ref=dst, send_sem=swap_sem.at[0, i], recv_sem=swap_sem.at[1, i], device_id=partner, device_id_type=pl.DeviceIdType.MESH)
        for i, (src, dst) in enumerate(((x_ref.at[1 - core], xs_ref.at[core]), (pos_ref.at[1 - core], pos_all.at[chip, core]), (gy_ref.at[1 - core], gy_own)))]
    for sw in swaps:
        sw.start()
    pos_copy = to_peers(pos_all.at[chip], pos_all, ps_sem, pr_sem)
    pos_all[chip, core] = pos_ref[core]
    loads[0].wait()
    swaps[0].wait_recv()
    for c in range(CHUNKS):
        top = (c * part) % (rows // 2)
        piece, ts = c * part // (rows // 2), slice(top, top + part)
        acc = jnp.zeros((part, HEAD_DIM), F32)
        for lo in range(0, dim, HEAD_DIM):
            x = xs_ref[piece, ts, lo:lo + HEAD_DIM].astype(F32)
            acc += x * x
        inv = lax.rsqrt(jnp.sum(acc, axis=1, keepdims=True) / dim + NORM_EPS)
        for lo in range(0, dim, HEAD_DIM):
            hs = slice(lo, lo + HEAD_DIM)
            x = xs_ref[piece, ts, hs].astype(F32)
            buf[0, chip, c * part:(c + 1) * part, hs] = (x * inv * gt_ref[2:3, hs]).astype(BF)
    swaps[1].wait_recv()
    each_peer(lambda p: pos_copy(p, chip).start())
    start_own(0)
    for ld in loads[2:]:
        ld.wait()

    def project(p):
        ts = pl.ds(pl.multiple_of(p * rows, rows), rows)
        h = buf[0, p]
        for idx, out in enumerate((qh_ref, kh_ref)):
            raw = mm32(h, w_ref[idx])
            out[ts, :] = raw
            ssq[pl.ds(idx * n_chip + p, 1), :] = as_row(jnp.sum(raw * raw, axis=1, keepdims=True))
        v_ref[ts, :] = mm32(h, w_ref[2]).astype(BF)

    project(chip)
    each_peer(lambda p: pos_copy(p, p).wait_recv())
    for p in range(n_chip):
        for u in range(2):
            ts = slice(p * rows + u * (rows // 2), p * rows + (u + 1) * (rows // 2))
            angles = column(pos_all[p, u, 0:1, :]) * f_ref[0:1, :]
            c_ref[ts, :] = jnp.cos(angles)
            s_ref[ts, :] = jnp.sin(angles) * f_ref[1:2, :]

    def gather_step(s, _):
        stage(0, s)

        def both(dr, _):
            dist = (s + 1) * (1 - 2 * dr)
            project(chip_at(lax.rem(ring - dist + 2 * n_chip, n_chip)))
            return 0

        lax.fori_loop(0, 2, both, 0)
        return 0

    lax.fori_loop(0, half - 1, gather_step, 0)
    loads[1].wait()
    swaps[2].wait_recv()
    start_own(1)
    gys_copy = pltpu.make_async_copy(buf.at[1, chip], gys_ref, out_sem.at[1])
    gys_copy.start()
    last_stage(0)
    project(slot_at(0, half))
    hall_copy = pltpu.make_async_copy(buf.at[0], hall_ref, out_sem.at[0])
    hall_copy.start()
    for hs in heads:
        vt_ref[hs, :] = v_ref[:, hs].T
    ssq_copy = to_peers(ssq, ssq_all, qs_sem, qr_sem)
    each_peer(lambda p: ssq_copy(p, chip).start())
    ssq_all[chip] = ssq[...]
    each_peer(lambda p: ssq_copy(p, p).wait_recv())
    total = ssq_all[0]
    for p in range(1, n_chip):
        total = total + ssq_all[p]
    inv_ref[...] = lax.rsqrt(total / dim + NORM_EPS)

    def finish_qk(p, _):
        ts = pl.ds(pl.multiple_of(p * rows, rows), rows)
        for idx, (hat_ref, out) in enumerate(((qh_ref, q_ref), (kh_ref, k_ref))):
            inv = column(inv_ref[pl.ds(idx * n_chip + p, 1), :])
            for hs in heads:
                hat = hat_ref[ts, hs] * inv
                hat_ref[ts, hs] = hat
                u = hat * g_ref[idx:idx + 1, hs]
                out[ts, hs] = (u * c_ref[ts, :] + half_roll(u) * s_ref[ts, :]).astype(BF)
        return 0

    lax.fori_loop(0, n_chip, finish_qk, 0)
    flush((xs_ref, xs_out), (c_ref, c_out), (s_ref, s_out), (v_ref, v_out))

    blk = FWD_BLOCK
    scale = HEAD_DIM ** -0.5 * LOG2E
    causal = lax.broadcasted_iota(jnp.int32, (blk, blk), 0) <= lax.broadcasted_iota(jnp.int32, (blk, blk), 1)

    def attend(t, _):
        j = flip(chip // 2, t, 2)
        qs = pl.ds(pl.multiple_of(j * blk, blk), blk)
        qb = [q_ref[qs, hs] for hs in heads]

        def tile(i, carry, diag):
            ks = pl.ds(pl.multiple_of(i * blk, blk), blk)
            out = []
            for h, hs in enumerate(heads):
                m, l, acc = carry[h]
                s = mm32_nt(k_ref[ks, hs], qb[h])
                if diag:
                    s = jnp.where(causal, s, NEG_BIG)
                mn = jnp.maximum(m, jnp.max(s, axis=0, keepdims=True))
                al = jnp.exp2((m - mn) * scale)
                p = jnp.exp2((s - mn) * scale)
                l = al * l + jnp.sum(p, axis=0, keepdims=True)
                out.append((mn, l, al * acc + mm32(vt_ref[hs, ks], p.astype(BF))))
            return tuple(out)

        st = tuple((jnp.full((1, blk), NEG_BIG, F32), jnp.zeros((1, blk), F32), jnp.zeros((HEAD_DIM, blk), F32)) for _ in heads)
        st = lax.fori_loop(0, j, lambda i, cr: tile(i, cr, False), st)
        st = tile(j, st, True)
        for h, hs in enumerate(heads):
            m, l, acc = st[h]
            ot = acc / l
            ot_ref[hs, qs] = ot
            att_ref[qs, hs] = ot.T.astype(BF)
            lse_ref[h:h + 1, qs] = m * scale + jnp.log2(l)
        return 0

    def use_gy(p):
        ts = pl.ds(pl.multiple_of(p * rows, rows), rows)
        gy = buf[1, p]
        datt_ref[ts, :] = mm32_nt(gy, wrow_ref[...]).astype(BF)
        dwo_ref[...] += mm32(ot_ref[:, ts].astype(BF), gy)

    n_att = n_chip * rows // blk
    lax.fori_loop(0, n_att // 2, attend, 0)
    stage(1, 0)
    lax.fori_loop(n_att // 2, n_att, attend, 0)

    flush((q_ref, q_out), (k_ref, k_out), (qh_ref, qh_out), (kh_ref, kh_out), (ot_ref, ot_out), (att_ref, att_out))

    def raw_of(w, out):
        def load(m, slot):
            return pltpu.make_async_copy(w.at[:, pl.ds(pl.multiple_of(m * cols, cols), cols)], wbuf.at[slot], w_sem.at[slot])

        load(0, 0).start()

        def step(m, _):
            slot = lax.rem(m, 2)
            load(m, slot).wait()

            @pl.when(m + 1 < n_chip)
            def _():
                load(m + 1, 1 - slot).start()
            out[:, pl.ds(pl.multiple_of(m * cols, cols), cols)] = mm32(buf[0, chip], wbuf[slot])
            return 0

        lax.fori_loop(0, n_chip, step, 0)

    raw_of(wq_ref, qr_ref)
    raw_of(wk_ref, kr_ref)
    stage(1, 1)
    dwo_ref[...] = jnp.zeros_like(dwo_ref)
    flush((qr_ref, qr_out), (kr_ref, kr_out))

    def use_ring(n, _):
        dist = ((n + 1) // 2) * (2 * lax.rem(n, 2) - 1)
        use_gy(chip_at(lax.rem(ring - dist + 2 * n_chip, n_chip)))
        return 0

    lax.fori_loop(0, n_chip - 3, use_ring, 0)
    stage(1, half - 2)
    lax.fori_loop(n_chip - 3, n_chip - 1, use_ring, 0)
    last_stage(1)
    use_gy(slot_at(0, half))

    each_peer(lambda p: pos_copy(p, chip).wait_send())
    each_peer(lambda p: ssq_copy(p, chip).wait_send())
    for sw in swaps:
        sw.wait_send()
    drain(0)
    drain(1)
    hall_copy.wait()
    gys_copy.wait()
    for copy in pending:
        copy.wait()


def back_kernel(q_ref, k_ref, v_ref, do_ref, ot_ref, lse_ref, gq_in, gk_in, gn_in, inv_ref,
                hall_ref, qh_hbm, kh_hbm, c_hbm, s_hbm, qr_hbm, kr_hbm, wq_ref, wk_ref, wv_ref, dwo_ref, wo_ref, at_hbm, x_hbm, gy_hbm,
                dwq_ref, dwk_ref, dwv_ref, y_ref, gx_ref, dwo_out, dg_out, dgn_out,
                dq_ref, dk_ref, dv_ref, dka_ref, dva_ref, kt_ref, qh_ref, kh_ref, c_ref, s_ref, qr_ref, kr_ref,
                tok, pairs, pair_in, dt_ref, hblk, wblk, dwo_in, row_ref, row_all,
                g_ref, gt_ref, dhid_ref, dg_ref, at_ref, x_ref, gy_ref, ys_ref, gxs_ref, dgp, dgp_in, gpart, gpair_in, gsel, gsel_in,
                as_sem, ar_sem, sw_sem, gs_sem, gr_sem, load_sem, h_sem, w_sem, xs_sem, xr_sem, ps_sem, pr_sem, rs_sem, rr_sem, own_sem, do_sem):
    me = lax.axis_index('sp')
    chip, core = me // 2, lax.rem(me, 2)
    n, cols = q_ref.shape
    rows, dim = qr_ref.shape
    n_chip = n // rows
    partner = {'sp': me + 1 - 2 * core}
    heads = [slice(lo, lo + HEAD_DIM) for lo in range(0, cols, HEAD_DIM)]
    own_rows = pl.ds(pl.multiple_of(chip * rows, rows), rows)
    own_cols = pl.ds(pl.multiple_of(chip * cols, cols), cols)
    MESH = pl.DeviceIdType.MESH

    def dev(p):
        return {'sp': 2 * p + core}

    def each_peer(fn):
        for step in range(1, n_chip):
            fn(flip(chip, step))

    sides = ((qh_hbm, qh_ref), (kh_hbm, kh_ref), (c_hbm, c_ref), (s_hbm, s_ref), (qr_hbm, qr_ref), (kr_hbm, kr_ref), (dwo_ref.at[core], dwo_out), (at_hbm.at[own_rows], at_ref.at[:, own_cols]), (x_hbm, x_ref), (gy_hbm, gy_ref))
    loads = [pltpu.make_async_copy(src, dst, load_sem.at[i]) for i, (src, dst) in enumerate(sides)]
    for ld in loads:
        ld.start()

    def load_h(p, slot):
        return pltpu.make_async_copy(hall_ref.at[:, pl.ds(pl.multiple_of(p * cols, cols), cols)], hblk.at[slot], h_sem.at[slot])

    def load_o(m, slot):
        return pltpu.make_async_copy(wo_ref.at[pl.ds(pl.multiple_of(m * cols, cols), cols)], wblk.at[slot, 0], w_sem.at[slot, 0])

    load_h(chip, 0).start()
    load_o(0, 0).start()
    fill_gains((gq_in, gk_in, gn_in), gt_ref, g_ref, own_cols)
    barrier = pltpu.get_barrier_semaphore()
    each_peer(lambda p: pl.semaphore_signal(barrier, inc=1, device_id=dev(p), device_id_type=MESH))
    pl.semaphore_signal(barrier, inc=1, device_id=partner, device_id_type=MESH)
    pl.semaphore_wait(barrier, n_chip)

    dwo_copy = pltpu.make_async_remote_copy(
        src_ref=dwo_ref.at[1 - core], dst_ref=dwo_in, send_sem=do_sem.at[0], recv_sem=do_sem.at[1], device_id=partner, device_id_type=MESH)
    dwo_copy.start()

    def at_copy(p, owner):
        src = at_hbm.at[pl.ds(pl.multiple_of(p * rows, rows), rows)]
        dst = at_ref.at[:, pl.ds(pl.multiple_of(owner * cols, cols), cols)]
        return pltpu.make_async_remote_copy(src_ref=src, dst_ref=dst, send_sem=as_sem.at[p], recv_sem=ar_sem.at[owner], device_id=dev(p), device_id_type=MESH)

    each_peer(lambda p: at_copy(p, chip).start())

    def to_partner(src, dst, i):
        return pltpu.make_async_remote_copy(src_ref=src, dst_ref=dst, send_sem=sw_sem.at[0, i], recv_sem=sw_sem.at[1, i], device_id=partner, device_id_type=MESH)

    y_swap = to_partner(ys_ref.at[1 - core], y_ref.at[core], 0)
    gx_swap = to_partner(gxs_ref.at[1 - core], gx_ref.at[core], 1)
    dg_swap = to_partner(dgp.at[1 - core], dgp_in, 2)
    gn_swap = to_partner(gpart.at[1 - core], gpair_in, 3)
    y_own = pltpu.make_async_copy(ys_ref.at[core], y_ref.at[core], sw_sem.at[0, 4])
    gx_own = pltpu.make_async_copy(gxs_ref.at[core], gx_ref.at[core], sw_sem.at[1, 4])

    def tok_copy(t, p, owner):
        src = (dq_ref, dk_ref, dv_ref)[t].at[pl.ds(pl.multiple_of(p * rows, rows), rows)]
        dst = tok.at[t, :, pl.ds(pl.multiple_of(owner * cols, cols), cols)]
        return pltpu.make_async_remote_copy(src_ref=src, dst_ref=dst, send_sem=xs_sem.at[t, p], recv_sem=xr_sem.at[t, owner], device_id=dev(p), device_id_type=MESH)

    blk = BWD_BLOCK
    span = blk // rows
    n_blk = n // blk
    sc = HEAD_DIM ** -0.5
    scale = sc * LOG2E
    for hs in heads:
        kt_ref[hs, :] = k_ref[:, hs].T
    dka_ref[...] = jnp.zeros_like(dka_ref)
    dva_ref[...] = jnp.zeros_like(dva_ref)
    causal = lax.broadcasted_iota(jnp.int32, (blk, blk), 0) <= lax.broadcasted_iota(jnp.int32, (blk, blk), 1)

    def send_dq(j):
        for u in range(span):
            p = j * span + u

            @pl.when(p != chip)
            def _():
                tok_copy(0, p, chip).start()

    def q_step(j, _):
        qs = pl.ds(pl.multiple_of(j * blk, blk), blk)
        qb = [q_ref[qs, hs] for hs in heads]
        dob = [do_ref[qs, hs] for hs in heads]
        lse = [lse_ref[h:h + 1, qs] for h in range(len(heads))]
        dl = [jnp.sum(ot_ref[hs, qs] * dob[h].astype(F32).T, axis=0, keepdims=True) for h, hs in enumerate(heads)]

        def tile(i, carry, diag):
            ks = pl.ds(pl.multiple_of(i * blk, blk), blk)
            out = []
            for h, hs in enumerate(heads):
                s = mm32_nt(k_ref[ks, hs], qb[h])
                dp = mm32_nt(v_ref[ks, hs], dob[h])
                p = jnp.exp2(s * scale - lse[h])
                if diag:
                    p = jnp.where(causal, p, 0.0)
                ds = (p * (dp - dl[h])).astype(BF)
                dva_ref[ks, hs] += mm32(p.astype(BF), dob[h])
                dka_ref[ks, hs] += mm32(ds, qb[h])
                out.append(carry[h] + mm32(kt_ref[hs, ks], ds))
            return tuple(out)

        st = tuple(jnp.zeros((HEAD_DIM, blk), F32) for _ in heads)
        st = lax.fori_loop(0, j, lambda i, cr: tile(i, cr, False), st)
        st = tile(j, st, True)
        for h, hs in enumerate(heads):
            dq_ref[qs, hs] = (st[h] * sc).T.astype(BF)

        @pl.when(j > 0)
        def _():
            send_dq(j - 1)
        return 0

    lax.fori_loop(0, n_blk, q_step, 0)
    dk_ref[...] = (dka_ref[...] * sc).astype(BF)
    dv_ref[...] = dva_ref[...].astype(BF)
    send_dq(n_blk - 1)
    for t, src in enumerate((dq_ref, dk_ref, dv_ref)):
        tok[t, :, own_cols] = src[own_rows, :]
    each_peer(lambda p: tok_copy(1, p, chip).start())
    for step in range(1, EARLY):
        tok_copy(2, flip(chip, step), chip).start()

    def pair_copy(w, p):
        return pltpu.make_async_remote_copy(
            src_ref=pairs.at[w, p, 1 - core], dst_ref=pair_in.at[w, p], send_sem=ps_sem.at[w, p], recv_sem=pr_sem.at[w, p], device_id=partner, device_id_type=MESH)

    grads = (dwq_ref, dwk_ref, dwv_ref)

    def dw_copy(w, p, owner):
        dst = grads[w].at[:, pl.ds(pl.multiple_of(owner * cols, cols), cols)]
        return pltpu.make_async_remote_copy(src_ref=pairs.at[w, p, core], dst_ref=dst, send_sem=xs_sem.at[3 + w, p], recv_sem=xr_sem.at[3 + w, owner], device_id=dev(p), device_id_type=MESH)

    def own_copy(w):
        return pltpu.make_async_copy(pairs.at[w, chip, core], grads[w].at[:, own_cols], own_sem.at[w])

    def partial(w, slot_t, h, p):
        dw = mm32(dt_ref[slot_t], h).T
        pairs[w, p, 0] = dw[:rows // 2]
        pairs[w, p, 1] = dw[rows // 2:]

    def merge(w, p):
        pair_copy(w, p).wait_recv()
        pairs[w, p, core] += pair_in[w, p]

    def send_dw(w, p):
        @pl.when(p != chip)
        def _():
            dw_copy(w, p, chip).start()

        @pl.when(p == chip)
        def _():
            own_copy(w).start()

    def each_h(ws, tail_fn):
        def step(i, _):
            p = flip(chip, i)
            slot = lax.rem(i, 2)
            load_h(p, slot).wait()

            @pl.when(i + 1 < n_chip)
            def _():
                load_h(flip(chip, i + 1), 1 - slot).start()
            for w, slot_t in ws:
                partial(w, slot_t, hblk[slot], p)
            tail_fn(i)
            for w, _ in ws:
                pair_copy(w, p).start()
            return 0

        lax.fori_loop(0, n_chip, step, 0)

    dt_ref[0] = dv_ref[...].T
    each_h(((2, 0),), lambda p: None)
    load_h(chip, 0).start()
    for ld in loads:
        ld.wait()

    each_peer(lambda p: at_copy(p, p).wait_recv())
    dhid_ref[...] = x_ref[...].astype(F32)

    def y_step(m, _):
        slot = lax.rem(m, 2)
        load_o(m, slot).wait()

        @pl.when(m + 1 < n_chip)
        def _():
            load_o(m + 1, 1 - slot).start()
        dhid_ref[...] += mm32(at_ref[:, pl.ds(pl.multiple_of(m * cols, cols), cols)], wblk[slot, 0])
        return 0

    lax.fori_loop(0, n_chip, y_step, 0)
    half = rows // 2
    for u in range(2):
        ys_ref[u] = dhid_ref[u * half:(u + 1) * half, :].astype(BF)

    hats = ((qr_ref, 0), (kr_ref, 1))
    row_ref[...] = jnp.zeros_like(row_ref)
    inv_t = [column(inv_ref[pl.ds(idx * n_chip + chip, 1), :]) for idx in range(2)]
    c_t, s_t = c_ref[own_rows, :], s_ref[own_rows, :]

    def normed(idx, hs):
        d = tok[idx, :, hs].astype(F32)
        return (d * c_t - half_roll(d) * s_t) * gt_ref[idx:idx + 1, hs]

    row_cols = []
    for raw_ref, idx in hats:
        each_peer(lambda p: tok_copy(idx, p, p).wait_recv())
        acc = jnp.zeros((rows, HEAD_DIM), F32)
        for lo in range(0, dim, HEAD_DIM):
            hs = slice(lo, lo + HEAD_DIM)
            acc += normed(idx, hs) * (raw_ref[:, hs] * inv_t[idx])
        row = jnp.sum(acc, axis=1, keepdims=True) / dim
        row_ref[idx:idx + 1, :] = as_row(row)
        row_cols.append(row)

    y_swap.start()
    y_own.start()

    def row_copy(p, owner):
        return pltpu.make_async_remote_copy(src_ref=row_ref, dst_ref=row_all.at[owner], send_sem=rs_sem.at[p], recv_sem=rr_sem.at[owner], device_id=dev(p), device_id_type=MESH)

    for raw_ref, idx in hats:
        for lo in range(0, dim, HEAD_DIM):
            hs = slice(lo, lo + HEAD_DIM)
            tok[idx, :, hs] = (inv_t[idx] * (normed(idx, hs) - raw_ref[:, hs] * inv_t[idx] * row_cols[idx])).astype(BF)
        if idx == 0:
            each_peer(lambda p: row_copy(p, chip).start())
            for step in range(EARLY, n_chip):
                tok_copy(2, flip(chip, step), chip).start()
            row_all[chip] = row_ref[...]

    def merge_v(p, _):
        merge(2, p)
        return 0

    def send_v(i, _):
        send_dw(2, flip(chip, i))
        return 0

    lax.fori_loop(0, n_chip, merge_v, 0)

    def load_w(m, slot):
        return [pltpu.make_async_copy(w.at[pl.ds(pl.multiple_of(m * cols, cols), cols)], wblk.at[slot, i], w_sem.at[slot, i]) for i, w in enumerate((wq_ref, wk_ref, wv_ref))]

    for ld in load_w(0, 0):
        ld.start()
    lax.fori_loop(0, n_chip, send_v, 0)
    each_peer(lambda p: row_copy(p, p).wait_recv())

    dg_ref[...] = jnp.zeros_like(dg_ref)

    def head_step(p, _):
        ts = pl.ds(pl.multiple_of(p * rows, rows), rows)
        for idx, (d_ref, hat_ref) in enumerate(((dq_ref, qh_ref), (dk_ref, kh_ref))):
            inv = column(inv_ref[pl.ds(idx * n_chip + p, 1), :])
            row = column(row_all[p, idx:idx + 1, :])
            for hs in heads:
                d = d_ref[ts, hs].astype(F32)
                rot = d * c_ref[ts, :] - half_roll(d) * s_ref[ts, :]
                hat = hat_ref[ts, hs]
                raw = inv * (rot * g_ref[idx:idx + 1, hs] - hat * row)
                dt_ref[idx, hs, ts] = raw.astype(BF).T
                dg_ref[idx:idx + 1, hs] += jnp.sum(rot * hat, axis=0, keepdims=True)
        return 0

    lax.fori_loop(0, n_chip, head_step, 0)
    dgp[...] = jnp.zeros_like(dgp)
    for u in range(2):
        dgp[u, 0:2, :] = dg_ref[0:2, u * half:(u + 1) * half]

    def lagged(i):
        @pl.when(i > 0)
        def _():
            for w in range(2):
                merge(w, flip(chip, i - 1))

        @pl.when(i > 1)
        def _():
            for w in range(2):
                send_dw(w, flip(chip, i - 2))

    each_h(((0, 0), (1, 1)), lagged)
    for w in range(2):
        send_dw(w, flip(chip, n_chip - 2))
        merge(w, flip(chip, n_chip - 1))
    dwo_copy.wait_recv()
    dwo_out[...] += dwo_in[...]
    for w in range(2):
        send_dw(w, flip(chip, n_chip - 1))
    dg_swap.start()

    each_peer(lambda p: tok_copy(2, p, p).wait_recv())

    def hid_step(m, _):
        slot = lax.rem(m, 2)
        for ld in load_w(m, slot):
            ld.wait()

        @pl.when(m + 1 < n_chip)
        def _():
            for ld in load_w(m + 1, 1 - slot):
                ld.start()
        out = pl.ds(pl.multiple_of(m * cols, cols), cols)
        dhid_ref[:, out] = mm32_nt(tok[0], wblk[slot, 0]) + mm32_nt(tok[1], wblk[slot, 1]) + mm32_nt(tok[2], wblk[slot, 2])
        return 0

    lax.fori_loop(0, n_chip, hid_step, 0)

    blocks = [slice(lo, lo + HEAD_DIM) for lo in range(0, dim, HEAD_DIM)]
    acc = jnp.zeros((rows, HEAD_DIM), F32)
    dot = jnp.zeros((rows, HEAD_DIM), F32)
    for hs in blocks:
        x = x_ref[:, hs].astype(F32)
        acc += x * x
        dot += x * dhid_ref[:, hs] * gt_ref[2:3, hs]
    x_inv = lax.rsqrt(jnp.sum(acc, axis=1, keepdims=True) / dim + NORM_EPS)
    mean = jnp.sum(dot, axis=1, keepdims=True) * x_inv / dim
    gpart[...] = jnp.zeros_like(gpart)
    for i, hs in enumerate(blocks):
        x_hat = x_ref[:, hs].astype(F32) * x_inv
        d = dhid_ref[:, hs]
        gx = (gy_ref[:, hs].astype(F32) + x_inv * (d * gt_ref[2:3, hs] - x_hat * mean)).astype(BF)
        gxs_ref[0, :, hs] = gx[:half]
        gxs_ref[1, :, hs] = gx[half:]
        gpart[i % 2, i // 2, 0:1, :] = jnp.sum(d * x_hat, axis=0, keepdims=True)
    gn_swap.start()
    gx_swap.start()
    gx_own.start()
    dg_swap.wait_recv()
    dg_out[...] = dgp[core] + dgp_in[...]
    gn_swap.wait_recv()
    gsel[...] = gpart[core] + gpair_in[...]

    def gn_copy(p, owner):
        return pltpu.make_async_remote_copy(src_ref=gsel.at[p], dst_ref=gsel_in.at[owner], send_sem=gs_sem.at[p], recv_sem=gr_sem.at[owner], device_id=dev(p), device_id_type=MESH)

    each_peer(lambda p: gn_copy(p, chip).start())
    gsel_in[chip] = gsel[chip]
    each_peer(lambda p: gn_copy(p, p).wait_recv())
    total = gsel_in[0]
    for p in range(1, n_chip):
        total = total + gsel_in[p]
    dgn_out[...] = total
    each_peer(lambda p: gn_copy(p, chip).wait_send())
    for sw in (y_swap, gx_swap):
        sw.wait_recv()
    for sw in (y_swap, gx_swap, dg_swap, gn_swap):
        sw.wait_send()
    y_own.wait()
    gx_own.wait()

    for w in range(3):
        each_peer(lambda p: dw_copy(w, p, p).wait_recv())
        each_peer(lambda p: dw_copy(w, p, chip).wait_send())
        each_peer(lambda p: tok_copy(w, p, chip).wait_send())
        own_copy(w).wait()
        for p in range(n_chip):
            pair_copy(w, p).wait_send()
    each_peer(lambda p: row_copy(p, chip).wait_send())
    each_peer(lambda p: at_copy(p, chip).wait_send())
    dwo_copy.wait_send()


VM = pl.BlockSpec(memory_space=pltpu.VMEM)


def mm32(a, b):
    return jnp.dot(a, b, preferred_element_type=F32)


def mm32_nt(a, b):
    return lax.dot_general(a, b, NT, preferred_element_type=F32)


def front(x, gy, w_query, w_key, w_value, w_out, pos, gains, freq, n_chip):
    loc, dim = x.shape[1:]
    rows = 2 * loc
    cols = dim // n_chip
    n = n_chip * rows
    heads = cols // HEAD_DIM
    any_spec = pl.BlockSpec(memory_space=pl.ANY)
    half = n_chip // 2
    dma, vmem = pltpu.SemaphoreType.DMA, pltpu.VMEM
    outs = [((n_chip, rows, dim), BF), ((n, cols), BF), ((n, cols), BF), ((n, cols), BF), ((n, cols), F32), ((n, cols), F32), ((cols, n), F32), ((heads, n), F32),
            ((n, cols), BF), ((n, cols), BF), ((cols, dim), F32), ((n, HEAD_DIM), F32), ((n, HEAD_DIM), F32), ((2 * n_chip, rows), F32), ((rows, dim), F32), ((rows, dim), F32),
            ((2, loc, dim), BF), ((rows, dim), BF)]
    return pl.pallas_call(
        front_kernel, name='front', out_shape=tuple(jax.ShapeDtypeStruct(s, d) for s, d in outs),
        in_specs=[any_spec] * 6 + [VM] * 5, out_specs=(any_spec,) * 7 + (VM,) + (any_spec,) + (VM,) * 2 + (any_spec,) * 2 + (VM,) + (any_spec,) * 4,
        scratch_shapes=[vmem(*outs[i]) for i in (1, 2, 3, 4, 5, 6, 11, 12, 14, 15, 16)] + [dma((12,)),
            vmem((2, 8, loc), F32), vmem((2, cols), F32), vmem((3, dim), F32), vmem((2, n_chip, rows, dim), BF), vmem((3, dim, cols), BF), vmem((cols, dim), BF), vmem((n, cols), BF), vmem((cols, n), BF),
            vmem((n_chip, 2, 8, loc), F32), vmem((2 * n_chip, rows), F32), vmem((n_chip, 2 * n_chip, rows), F32), vmem((2, dim, cols), BF),
            dma((2,)), dma((6,)), dma((2, 3)), dma((2,)), dma((2, 2, half, CHUNKS)), dma((2, 2, half, CHUNKS)),
            dma((n_chip,)), dma((n_chip,)), dma((n_chip,)), dma((n_chip,))],
        compiler_params=pltpu.CompilerParams(collective_id=0, has_side_effects=True, vmem_limit_bytes=67043328),
        cost_estimate=pl.CostEstimate(flops=400 * n * dim * cols, bytes_accessed=40 * n * dim, transcendentals=n * n * heads // 2),
    )(x, gy, w_query, w_key, w_value, w_out, pos, *gains, freq)


def back(q, k, v, d_att, att_t, lse, gains, inv, hid, qh, kh, cos_a, sin_a, q_raw, k_raw, w_query, w_key, w_value, dwo, w_out, att, x, gy):
    n, cols = q.shape
    rows, dim = q_raw.shape
    n_chip = n // rows
    any_spec = pl.BlockSpec(memory_space=pl.ANY)
    dma = pltpu.SemaphoreType.DMA
    grad = jax.ShapeDtypeStruct((rows // 2, dim), F32)
    seq = jax.ShapeDtypeStruct((2, rows // 2, dim), BF)
    small = jax.ShapeDtypeStruct((8, cols // 2), F32)
    tile = (n_chip, 8, cols // 2)
    vmem = pltpu.VMEM
    return pl.pallas_call(
        back_kernel, name='back', in_specs=[VM] * 10 + [any_spec] * 15, out_specs=(any_spec,) * 5 + (VM,) * 3,
        out_shape=(grad,) * 3 + (seq, seq, grad, small, small),
        scratch_shapes=[
            vmem((n, cols), BF), vmem((n, cols), BF), vmem((n, cols), BF), vmem((n, cols), F32), vmem((n, cols), F32), vmem((cols, n), BF),
            vmem((n, cols), F32), vmem((n, cols), F32), vmem((n, HEAD_DIM), F32), vmem((n, HEAD_DIM), F32), vmem((rows, dim), F32), vmem((rows, dim), F32),
            vmem((3, rows, dim), BF), vmem((3, n_chip, 2, rows // 2, cols), F32), vmem((3, n_chip, rows // 2, cols), F32),
            vmem((2, cols, n), BF), vmem((2, n, cols), BF), vmem((2, 3, cols, dim), BF), vmem((rows // 2, dim), F32),
            vmem((8, rows), F32), vmem((n_chip, 8, rows), F32),
            vmem((2, cols), F32), vmem((3, dim), F32), vmem((rows, dim), F32), vmem((8, cols), F32), vmem((rows, dim), BF), vmem((rows, dim), BF), vmem((rows, dim), BF), vmem((2, rows // 2, dim), BF), vmem((2, rows // 2, dim), BF),
            vmem((2, 8, cols // 2), F32), vmem((8, cols // 2), F32), vmem((2,) + tile, F32), vmem(tile, F32), vmem(tile, F32), vmem(tile, F32),
            dma((n_chip,)), dma((n_chip,)), dma((2, 5)), dma((n_chip,)), dma((n_chip,)), dma((10,)), dma((2,)), dma((2, 3)), dma((6, n_chip)), dma((6, n_chip)), dma((3, n_chip)), dma((3, n_chip)),
            dma((n_chip,)), dma((n_chip,)), dma((3,)), dma((2,))],
        compiler_params=pltpu.CompilerParams(collective_id=1, has_side_effects=True, vmem_limit_bytes=67043328),
        cost_estimate=pl.CostEstimate(flops=400 * n * dim * cols, bytes_accessed=40 * n * dim, transcendentals=n * n),
    )(q, k, v, d_att, att_t, lse, *gains, inv, hid, qh, kh, cos_a, sin_a, q_raw, k_raw, w_query, w_key, w_value, dwo, w_out, att, x, gy)


def copy_kernel(*refs):
    n = len(refs) // 2
    for src, dst in zip(refs[:n], refs[n:]):
        dst[...] = src[...]


def hand_out(arrays, steps=4):
    specs = []
    for a in arrays:
        block = a.shape[:-2] + (a.shape[-2] // steps, a.shape[-1])
        specs.append(pl.BlockSpec(block, (lambda p: (0, p, 0)) if a.ndim == 3 else (lambda p: (p, 0))))
    return pl.pallas_call(copy_kernel, grid=(steps,), name='hand_out', in_specs=specs, out_specs=specs, out_shape=[jax.ShapeDtypeStruct(a.shape, a.dtype) for a in arrays])(*arrays)


def solution(mesh):
    n_chip = mesh.shape['sp'] // 2

    def device_step(x_loc, gy_loc, positions, g_norm, w_query, w_key, w_value, w_out, g_query, g_key):
        loc, dim = x_loc.shape[1], x_loc.shape[2]
        rows = 2 * loc
        gains = (g_query, g_key, g_norm)
        hid_all, q, k, v, qh_hat, kh_hat, att_t, lse, att, d_att, dwo, cos_a, sin_a, inv_all, q_raw, k_raw, x_sw, gy_sw = front(
            x_loc, gy_loc, w_query, w_key, w_value, w_out, positions, gains, rope_rows(), n_chip)
        dwq, dwk, dwv, y, grad_x, dwo, dg, dgn = back(
            q, k, v, d_att, att_t, lse, gains, inv_all, hid_all.reshape(n_chip * rows, dim), qh_hat, kh_hat, cos_a, sin_a,
            q_raw, k_raw, w_query, w_key, w_value, dwo.reshape(2, loc, dim), w_out, att, x_sw.reshape(rows, dim), gy_sw)
        y, grad_x, dwq, dwk, dwv, dwo = hand_out((y, grad_x, dwq, dwk, dwv, dwo))
        return y, grad_x, dgn[0], dwq, dwk, dwv, dwo, dg[0], dg[1]

    seq_spec = P('dp', 'sp', None)
    mat_rep = P(None, None)
    vec_rep = P(None)
    row_spec = P(('dp', 'sp'), None)
    vec_spec = P(('dp', 'sp'))
    return jax.shard_map(device_step, mesh=mesh, in_specs=(seq_spec, seq_spec, P('dp', 'sp'), vec_rep, mat_rep, mat_rep, mat_rep, mat_rep, vec_rep, vec_rep), out_specs=(seq_spec, seq_spec, vec_spec, row_spec, row_spec, row_spec, row_spec, vec_spec, vec_spec), check_vma=False)
```
